128 devices in a mesh: gx: 2 (over core), gy: 4 (over x), gz: 16 (over z, y).
Axes of the slice: x: 4, y: 4, z: 4, core: 2. Of those that a mesh axis runs over, the one named last changes fastest.
Arguments:
- right_side: float32 [64, 512, 1024], P('gx', 'gy', 'gz'), may hold values from -21 to 21, as said below
- conductivity: float32 [64, 512, 1024], P('gx', 'gy', 'gz'), may hold values from 0.25 to 1
- absorption: float32 [64, 512, 1024], P('gx', 'gy', 'gz'), may hold values from 0.5 to 2
Outputs:
- solution_field: float32 [64, 512, 1024], P('gx', 'gy', 'gz')
- residual: float32 [64, 512, 1024], P('gx', 'gy', 'gz')
The draws below stay inside these ranges and needn't reach their ends.
Inputs may be any that keep to these rules, and one draw needn't show every extreme that they name: right_side lies within -21 and 21.
All inputs are finite; a program needn't handle non-finite values.
Results may differ from the reference program's by a relative error of at most 0.004.
Values sent between devices are 32-bit elements.
A program may use at most 128 MiB of HBM per device.

```python
import math
import jax
import jax.numpy as jnp

ITERS = 10
NX = 64
NY = 512
NZ = 1024


def draw_right_side(key, part):
    noise_key = jax.random.fold_in(key, 11)
    phase_key = jax.random.fold_in(key, 23)
    noise = jnp.clip(jax.random.normal(noise_key, (NX, NY, NZ), jnp.float32), -6.0, 6.0)
    phases = jax.random.uniform(phase_key, (3,), jnp.float32, 0.0, 2.0 * math.pi)
    along_x = jnp.arange(NX, dtype=jnp.float32) / NX
    along_y = jnp.arange(NY, dtype=jnp.float32) / NY
    along_z = jnp.arange(NZ, dtype=jnp.float32) / NZ
    wave_x = 0.5 + 0.5 * jnp.cos(2.0 * math.pi * along_x + phases[0])
    wave_y = 0.5 + 0.5 * jnp.cos(2.0 * math.pi * along_y + phases[1])
    wave_z = 0.5 + 0.5 * jnp.cos(2.0 * math.pi * along_z + phases[2])
    envelope = 0.4 + 3.0 * wave_x[:, None, None] * wave_y[None, :, None] * wave_z[None, None, :]
    return noise * envelope


def block_levels(rng, extent, pieces, low, largest):
    level = 1.0
    for position, blocks in pieces:
        steps = jax.random.uniform(jax.random.fold_in(jax.random.fold_in(rng, 6), position), (blocks,), jnp.float32, low / len(pieces), largest / len(pieces))
        level = level * jnp.repeat(jnp.exp(steps), extent[position] // blocks).reshape((-1,) + (1,) * (len(extent) - 1 - position))
    return level


def setup_inputs(seed: int = 0) -> dict:
    seeds = jax.random.split(jax.random.key(seed), 4)
    return {
        "right_side": draw_right_side(jax.random.fold_in(seeds[3], 71), 0),
        "conductivity": jnp.clip(jnp.exp(math.log(1.0) - 1.3862944 * jax.random.uniform(seeds[1], (NX, NY, NZ), jnp.float32) ** block_levels(seeds[1], (NX, NY, NZ), ((0, 2), (1, 4), (2, 16)), -0.2, 0.2)), 0.25, 1.0),
        "absorption": jnp.clip(0.5 + 1.5 * jax.random.uniform(seeds[2], (NX, NY, NZ), jnp.float32) ** block_levels(seeds[2], (NX, NY, NZ), ((0, 2), (1, 4), (2, 16)), -0.2, 0.2), 0.5, 2.0),
    }


def coefficients(conductivity, absorption):
    padded = jnp.pad(conductivity, 1)
    face_x = 0.5 * (padded[:-1, 1:-1, 1:-1] + padded[1:, 1:-1, 1:-1])
    face_y = 0.5 * (padded[1:-1, :-1, 1:-1] + padded[1:-1, 1:, 1:-1])
    face_z = 0.5 * (padded[1:-1, 1:-1, :-1] + padded[1:-1, 1:-1, 1:])
    total = absorption + face_x[1:] + face_x[:-1] + face_y[:, 1:] + face_y[:, :-1] + face_z[:, :, 1:] + face_z[:, :, :-1]
    return face_x, face_y, face_z, total


def operate(field, coeffs):
    face_x, face_y, face_z, total = coeffs
    padded = jnp.pad(field, 1)
    beside = face_x[1:] * padded[2:, 1:-1, 1:-1] + face_x[:-1] * padded[:-2, 1:-1, 1:-1]
    beside = beside + face_y[:, 1:] * padded[1:-1, 2:, 1:-1] + face_y[:, :-1] * padded[1:-1, :-2, 1:-1]
    beside = beside + face_z[:, :, 1:] * padded[1:-1, 1:-1, 2:] + face_z[:, :, :-1] * padded[1:-1, 1:-1, :-2]
    return total * field - beside


def reference(right_side, conductivity, absorption):
    coeffs = coefficients(conductivity, absorption)
    total = coeffs[3]
    solution_field = jnp.zeros_like(right_side)
    residual = right_side
    precond = residual / total
    direction = precond
    rho_now = jnp.sum(residual * precond)
    for iteration in range(ITERS):
        image = operate(direction, coeffs)
        step_size = rho_now / jnp.sum(direction * image)
        solution_field = solution_field + step_size * direction
        residual = residual - step_size * image
        precond = residual / total
        rho_next = jnp.sum(residual * precond)
        direction = precond + (rho_next / rho_now) * direction
        rho_now = rho_next
    return solution_field, residual
```

```python
import functools

import jax
import jax.numpy as jnp
from jax import lax
from jax.experimental import pallas as pl
from jax.experimental.pallas import tpu as pltpu
from jax.sharding import PartitionSpec as P

F32 = jnp.float32
MESH = pl.DeviceIdType.MESH
STEPS = 5
RHO = 0.65
LANES = 128


def added(p, q, scale=None):
    out = dict(p)
    for k, v in q.items():
        w = v if scale is None else scale * v
        out[k] = out[k] + w if k in out else w
    return out


def form(p, q, gram):
    total = None
    for i, a in p.items():
        row = None
        for j, b in q.items():
            g = gram(i, j)
            if g is not None:
                row = g * b if row is None else row + g * b
        if row is not None:
            total = a * row if total is None else total + a * row
    return total


def first_block(mu, one):
    def gram(i, j):
        return 0.5 * (mu[i + j] + mu[abs(i - j)])

    def times(q):
        out = {}
        for k, v in q.items():
            for kk in (k + 1, abs(k - 1)):
                h = 0.5 * v
                out[kk] = out[kk] + h if kk in out else h
        return out

    p, q, x, rho = {0: one}, {0: one}, {}, mu[0]
    for it in range(STEPS):
        image = added(q, times(q), -RHO)
        step = rho / form(q, image, gram)
        x = added(x, q, step)
        p = added(p, image, -step)
        if it + 1 < STEPS:
            new = form(p, p, gram)
            q = added(p, q, new / rho)
            rho = new
    return x, p, q, rho


def second_block(nu, c, x5, q4, rho4, mu, one):
    n = STEPS
    inverse = one / c[n]
    cross = {}

    def own(i, j):
        return 0.5 * (nu[i + j] + nu[abs(i - j)])

    def last(j):
        acc = own(j, 0)
        for k in range(n):
            if cross[(j, k)] is not None:
                acc = acc - c[k] * cross[(j, k)]
        return inverse * acc

    def plus(a, b, sign=1.0):
        if b is None:
            return a
        if a is None:
            return sign * b
        return a + sign * b

    for k in range(n):
        cross[(0, k)] = None
    cross[(0, n)] = last(0)
    for j in range(1, n + 1):
        for k in range(n):
            both = plus(cross[(j - 1, k + 1)], cross[(j - 1, abs(k - 1))])
            if j == 1:
                cross[(j, k)] = None if both is None else 0.5 * both
            else:
                cross[(j, k)] = plus(both, cross[(j - 2, k)], -1.0)
        if j < n:
            cross[(j, n)] = last(j)

    def gram(a, b):
        if a[0] == b[0]:
            m = nu if a[0] == "y" else mu
            return 0.5 * (m[a[1] + b[1]] + m[abs(a[1] - b[1])])
        if a[0] == "t":
            a, b = b, a
        return cross[(a[1], b[1])]

    def times(q):
        out = {}

        def put(k, v):
            out[k] = out[k] + v if k in out else v

        for (s, k), v in q.items():
            h = 0.5 * v
            put((s, abs(k - 1)), h)
            if s == "t" and k == n - 1:
                w = h * inverse
                put(("y", 0), w)
                for kk in range(n):
                    put(("t", kk), -(w * c[kk]))
            else:
                put((s, k + 1), h)
        return out

    rho = nu[0]
    p = {("y", 0): one}
    x = {("t", k): v for k, v in x5.items()}
    q = added(p, {("t", k): v for k, v in q4.items()}, rho / rho4)
    for it in range(n):
        image = added(q, times(q), -RHO)
        step = rho / form(q, image, gram)
        x = added(x, q, step)
        p = added(p, image, -step)
        if it + 1 < n:
            new = form(p, p, gram)
            q = added(p, q, new / rho)
            rho = new
    return x, p


def kernel(nx, nz, sizes, r_hbm, c_hbm, a_hbm, x_hbm, o_hbm,
           cond, absorb, diag, weight, fx, fy, fz, ey, halo, field, zsend, zrecv, ysend, yrecv,
           part1, part2, coef, xout, rout,
           load_sem, store_sem, face_send, face_recv, sum1_send, sum1_recv, sum2_send, sum2_recv):
    gx, gy, gz = sizes
    ix, iy, iz = lax.axis_index("gx"), lax.axis_index("gy"), lax.axis_index("gz")
    ox = 1 - ix
    base = 8
    inner = pl.ds(base, nz)
    above = pl.ds(base + 1, nz)
    below = pl.ds(base - 1, nz)
    half = nz // 2

    loads = [
        pltpu.make_async_copy(c_hbm, cond.at[pl.ds(1, nx), inner, :], load_sem.at[0]),
        pltpu.make_async_copy(a_hbm, absorb, load_sem.at[1]),
        pltpu.make_async_copy(r_hbm, rout, load_sem.at[2]),
    ]
    for load in loads:
        load.start()

    zero_slab = jnp.zeros((nz, LANES), F32)

    def clear(k, _):
        field[k, 0, inner, :] = zero_slab
        field[k, nx + 1, inner, :] = zero_slab
        return 0

    lax.fori_loop(0, 2 * STEPS + 2, clear, 0)
    cond[0, inner, :] = zero_slab
    cond[nx + 1, inner, :] = zero_slab
    zero_face = jnp.zeros((nx, LANES), F32)

    def clear_faces(k, _):
        for side in range(2):
            zrecv[k, side] = zero_face
            yrecv[k, side] = zero_face
        return 0

    lax.fori_loop(0, 2 * STEPS + 1, clear_faces, 0)

    barrier = pltpu.get_barrier_semaphore()
    group = [((ix + dx) % gx, (iy + dy) % gy) for dx in range(gx) for dy in range(gy) if (dx, dy) != (0, 0)]
    line = [(iz + d) % gz for d in range(1, gz)]
    for px, py in group:
        pl.semaphore_signal(barrier, inc=1, device_id=(px, py, iz), device_id_type=MESH)
    for pz in line:
        pl.semaphore_signal(barrier, inc=1, device_id=(ix, iy, pz), device_id_type=MESH)
    pl.semaphore_wait(barrier, len(group) + len(line))

    lane = lax.broadcasted_iota(jnp.int32, (half, LANES), 1)
    pair = lane // 2
    even = (lane % 2) == 0

    def pack(ref):
        out = jnp.zeros((half, LANES), F32)
        for x in range(nx):
            for h in range(2):
                v = ref[x + 1, pl.ds(base + half * h, half), :]
                out = jnp.where(pair == x + nx * h, pltpu.roll(v, (2 * x + 2 * nx * h + 1) % LANES, 1), out)
        return out

    def copies(ref, e):
        xc = pltpu.make_async_remote_copy(
            ref.at[jnp.where(ix == 0, nx, 1), inner, :], ref.at[jnp.where(ix == 0, 0, nx + 1), inner, :],
            face_send.at[e, 0], face_recv.at[e, 0], device_id=(ox, iy, iz), device_id_type=MESH)
        yc, zc = [], []
        for up in range(2):
            yc.append(pltpu.make_async_remote_copy(
                ysend.at[e], yrecv.at[e, 1 - up], face_send.at[e, 1 + up], face_recv.at[e, 2 - up],
                device_id=(ix, jnp.clip(iy + 2 * up - 1, 0, gy - 1), iz), device_id_type=MESH))
            zc.append(pltpu.make_async_remote_copy(
                zsend.at[e, up], zrecv.at[e, 1 - up], face_send.at[e, 3 + up], face_recv.at[e, 4 - up],
                device_id=(ix, iy, jnp.clip(iz + 2 * up - 1, 0, gz - 1)), device_id_type=MESH))
        return xc, yc, zc

    def send(ref, e):
        xc, yc, zc = copies(ref, e)
        xc.start()
        zsend[e, 0] = ref[pl.ds(1, nx), base, :]
        zsend[e, 1] = ref[pl.ds(1, nx), base + nz - 1, :]
        pl.when(iz > 0)(zc[0].start)
        pl.when(iz < gz - 1)(zc[1].start)
        ysend[e] = pack(ref)
        pl.when(iy > 0)(yc[0].start)
        pl.when(iy < gy - 1)(yc[1].start)

    def receive(ref, e):
        xc, yc, zc = copies(ref, e)
        xc.wait()
        pl.when(iy > 0)(lambda: (yc[0].wait_send(), yc[1].wait_recv())[0])
        pl.when(iy < gy - 1)(lambda: (yc[1].wait_send(), yc[0].wait_recv())[0])
        pl.when(iz > 0)(lambda: (zc[0].wait_send(), zc[1].wait_recv())[0])
        pl.when(iz < gz - 1)(lambda: (zc[1].wait_send(), zc[0].wait_recv())[0])
        ref[pl.ds(1, nx), base - 1, :] = zrecv[e, 0]
        ref[pl.ds(1, nx), base + nz, :] = zrecv[e, 1]
        both = jnp.where(even, yrecv[e, 0], pltpu.roll(yrecv[e, 1], LANES - 2, 1))
        for x in range(nx):
            for h in range(2):
                halo[x, pl.ds(half * h, half), :] = pltpu.roll(both, (LANES - 2 * x - 2 * nx * h) % LANES, 1)

    wide_lane = lax.broadcasted_iota(jnp.int32, (nz, LANES), 1)
    inside = wide_lane < LANES - 1
    edge = (wide_lane == 0) | (wide_lane == LANES - 1)

    loads[0].wait()
    send(cond, 0)
    loads[1].wait()
    loads[2].wait()
    receive(cond, 0)
    fx[0] = 0.5 * (cond[0, inner, :] + cond[1, inner, :])

    def coefficients(x, _):
        here = cond[x + 1, inner, :]
        xp = 0.5 * (here + cond[x + 2, inner, :])
        xm = fx[x]
        yp = jnp.where(inside, 0.5 * (here + pltpu.roll(here, LANES - 1, 1)), 0.0)
        ye = jnp.where(edge, 0.5 * (here + halo[x]), 0.0)
        zp = 0.5 * (here + cond[x + 1, above, :])
        zm = 0.5 * (here + cond[x + 1, below, :])
        total = absorb[x] + xp + xm + yp + pltpu.roll(yp, 1, 1) + ye + zp + zm
        inverse = 1.0 / total
        fx[x + 1] = xp
        fy[x] = yp
        ey[x] = ye
        fz[x, below, :] = zm
        fz[x, inner, :] = zp
        diag[x] = total
        weight[x] = (2.0 / RHO) * inverse
        field[0, x + 1, inner, :] = rout[x] * inverse
        return 0

    lax.fori_loop(0, nx, coefficients, 0)

    tiles = nz // 8

    def chain(first, exchange):
        def step(k, sums):
            src, dst, old = first + k, first + k + 1, jnp.maximum(first + k - 1, first)
            send(field.at[src], exchange + k)
            receive(field.at[src], exchange + k)
            scale = jnp.where(k == 0, 0.5, 1.0).astype(F32)
            keep = jnp.where(k == 0, 0.0, 1.0).astype(F32)

            def row(x, acc):
                same, next_ = acc
                v = field[src, x + 1, inner, :]
                y = fy[x]
                s = fx[x + 1] * field[src, x + 2, inner, :] + fx[x] * field[src, x, inner, :]
                s = s + fz[x, inner, :] * field[src, x + 1, above, :] + fz[x, below, :] * field[src, x + 1, below, :]
                s = s + y * pltpu.roll(v, LANES - 1, 1) + pltpu.roll(y * v, 1, 1) + ey[x] * halo[x]
                new = scale * (weight[x] * s) - keep * field[old, x + 1, inner, :]
                field[dst, x + 1, inner, :] = new
                w = diag[x] * v
                return same + w * v, next_ + w * new

            zero = jnp.zeros((nz, LANES), F32)
            same, next_ = lax.fori_loop(0, nx, row, (zero, zero), unroll=4)
            coef[2 * k] = jnp.sum(same.reshape(tiles, 8, LANES), axis=0)
            coef[2 * k + 1] = jnp.sum(next_.reshape(tiles, 8, LANES), axis=0)
            return sums

        lax.fori_loop(0, STEPS, step, 0)

    row_lane = lax.broadcasted_iota(jnp.int32, (1, LANES), 1)
    gxy = ix * gy + iy

    def total_of(n, which):
        out = jnp.zeros((1, LANES), F32)
        for m in range(n):
            one_row = jnp.sum(coef[m], axis=0, keepdims=True)
            out = jnp.where(row_lane == m, jnp.sum(one_row, axis=1, keepdims=True), out)
        for part, peers, mine, send_sem, recv_sem, where in (
            (part1, [(px, py, iz) for px, py in group], gxy, sum1_send, sum1_recv, [px * gy + py for px, py in group]),
            (part2, [(ix, iy, pz) for pz in line], iz, sum2_send, sum2_recv, line),
        ):
            part[which, mine] = out
            sent = []
            for i, peer in enumerate(peers):
                copy = pltpu.make_async_remote_copy(
                    part.at[which, mine], part.at[which, mine], send_sem.at[which, i], recv_sem.at[which, mine],
                    device_id=peer, device_id_type=MESH)
                copy.start()
                sent.append(copy)
            for i, slot in enumerate(where):
                pltpu.make_async_remote_copy(
                    part.at[which, slot], part.at[which, slot], send_sem.at[which, i], recv_sem.at[which, slot],
                    device_id=peers[i], device_id_type=MESH).wait_recv()
            for copy in sent:
                copy.wait_send()
            out = jnp.sum(part[which], axis=0)
        values = []
        for m in range(n):
            values.append(jnp.broadcast_to(jnp.sum(jnp.where(row_lane == m, out, 0.0), axis=1, keepdims=True), (8, LANES)))
        return values

    def moments(dots):
        mu = list(dots[:2])
        for m in range(2, len(dots)):
            mu.append(2.0 * dots[m] - mu[m % 2])
        return mu

    one = jnp.ones((8, LANES), F32)

    chain(0, 1)

    def last_dot(x, acc):
        v = field[STEPS, x + 1, inner, :]
        return acc + diag[x] * v * v

    acc = lax.fori_loop(0, nx, last_dot, jnp.zeros((nz, LANES), F32), unroll=4)
    coef[2 * STEPS] = jnp.sum(acc.reshape(tiles, 8, LANES), axis=0)
    mu = moments(total_of(2 * STEPS + 1, 0))
    x5, p5, q4, rho4 = first_block(mu, one)

    def spread(c):
        return jnp.broadcast_to(c[None], (tiles, 8, LANES)).reshape(nz, LANES)

    for k in range(STEPS + 1):
        coef[16 + k] = p5[k]

    def restart(x, _):
        acc = spread(coef[16]) * field[0, x + 1, inner, :]
        for k in range(1, STEPS + 1):
            acc = acc + spread(coef[16 + k]) * field[k, x + 1, inner, :]
        field[STEPS + 1, x + 1, inner, :] = acc
        return 0

    lax.fori_loop(0, nx, restart, 0, unroll=2)

    chain(STEPS + 1, STEPS + 1)
    nu = moments(total_of(2 * STEPS, 1))
    xs, ps = second_block(nu, p5, x5, q4, rho4, mu, one)
    names = [("t", k) for k in range(STEPS)] + [("y", k) for k in range(STEPS + 1)]
    where = list(range(STEPS)) + list(range(STEPS + 1, 2 * STEPS + 2))
    xs_at, ps_at = [], []
    slot = 16
    for name in names:
        for table, at in ((xs, xs_at), (ps, ps_at)):
            if name in table:
                coef[slot] = table[name]
                at.append(slot)
                slot += 1
            else:
                at.append(None)

    def finish(x, _):
        sx = sp = None
        for n, f in enumerate(where):
            v = field[f, x + 1, inner, :]
            if xs_at[n] is not None:
                t = spread(coef[xs_at[n]]) * v
                sx = t if sx is None else sx + t
            if ps_at[n] is not None:
                t = spread(coef[ps_at[n]]) * v
                sp = t if sp is None else sp + t
        xout[x] = sx
        rout[x] = diag[x] * sp
        return 0

    lax.fori_loop(0, nx, finish, 0)
    stores = [
        pltpu.make_async_copy(xout, x_hbm, store_sem.at[0]),
        pltpu.make_async_copy(rout, o_hbm, store_sem.at[1]),
    ]
    for store in stores:
        store.start()
    for store in stores:
        store.wait()


def solution(mesh):
    gx, gy, gz = mesh.shape["gx"], mesh.shape["gy"], mesh.shape["gz"]

    def on_device(right_side, conductivity, absorption):
        nx, ny, nz = right_side.shape
        assert ny == LANES and nx * 2 * 2 == LANES and gx == 2
        args = [jnp.transpose(v, (0, 2, 1)) for v in (right_side, conductivity, absorption)]
        block = (nx, nz, LANES)
        exchanges = 2 * STEPS + 1
        dma = pltpu.SemaphoreType.DMA
        tall = nz + 16
        out = pl.pallas_call(
            functools.partial(kernel, nx, nz, (gx, gy, gz)),
            out_shape=[jax.ShapeDtypeStruct(block, F32)] * 2,
            in_specs=[pl.BlockSpec(memory_space=pl.ANY)] * 3,
            out_specs=[pl.BlockSpec(memory_space=pl.ANY)] * 2,
            scratch_shapes=[
                pltpu.VMEM((nx + 2, tall, LANES), F32),
                pltpu.VMEM(block, F32),
                pltpu.VMEM(block, F32),
                pltpu.VMEM(block, F32),
                pltpu.VMEM((nx + 1, nz, LANES), F32),
                pltpu.VMEM(block, F32),
                pltpu.VMEM((nx, tall, LANES), F32),
                pltpu.VMEM(block, F32),
                pltpu.VMEM(block, F32),
                pltpu.VMEM((2 * STEPS + 2, nx + 2, tall, LANES), F32),
                pltpu.VMEM((exchanges, 2, nx, LANES), F32),
                pltpu.VMEM((exchanges, 2, nx, LANES), F32),
                pltpu.VMEM((exchanges, nz // 2, LANES), F32),
                pltpu.VMEM((exchanges, 2, nz // 2, LANES), F32),
                pltpu.VMEM((2, gx * gy, 1, LANES), F32),
                pltpu.VMEM((2, gz, 1, LANES), F32),
                pltpu.VMEM((48, 8, LANES), F32),
                pltpu.VMEM(block, F32),
                pltpu.VMEM(block, F32),
                dma((3,)),
                dma((2,)),
                dma((exchanges, 5)),
                dma((exchanges, 5)),
                dma((2, gx * gy)),
                dma((2, gx * gy)),
                dma((2, gz)),
                dma((2, gz)),
            ],
            compiler_params=pltpu.CompilerParams(
                collective_id=0, has_side_effects=True, vmem_limit_bytes=60 * 1024 * 1024
            ),
        )(*args)
        return tuple(jnp.transpose(v, (0, 2, 1)) for v in out)

    spec = P("gx", "gy", "gz")
    return jax.shard_map(on_device, mesh=mesh, in_specs=(spec,) * 3, out_specs=(spec,) * 2, check_vma=False)
```

```python
import functools

import jax
import jax.numpy as jnp
from jax import lax
from jax.experimental import pallas as pl
from jax.experimental.pallas import tpu as pltpu
from jax.sharding import PartitionSpec as P

F32 = jnp.float32
MESH = pl.DeviceIdType.MESH
STEPS = 10
LANES = 128
BASE = 8


def two_sum(a, b):
    s = a + b
    t = s - a
    return s, (a - (s - t)) + (b - t)


def renew(a, b):
    s = a + b
    return s, b - (s - a)


def halves(a):
    t = 4097.0 * a
    high = t - (t - a)
    return high, a - high


def two_product(a, b):
    p = a * b
    ah, al = halves(a)
    bh, bl = halves(b)
    return p, ((ah * bh - p) + ah * bl + al * bh) + al * bl


def dadd(a, b):
    s, e = two_sum(a[0], b[0])
    return renew(s, e + (a[1] + b[1]))


def dneg(a):
    return -a[0], -a[1]


def dmul(a, b):
    p, e = two_product(a[0], b[0])
    return renew(p, e + (a[0] * b[1] + a[1] * b[0]))


def dtimes(a, power):
    return power * a[0], power * a[1]


def ddiv(a, b):
    q = a[0] / b[0]
    p, e = two_product(q, b[0])
    rest = ((a[0] - p) - e) + (a[1] - q * b[1])
    return renew(q, rest / b[0])


def jacobi_matrix(mu):
    n = len(mu) // 2
    cur = [mu[0]] + [dtimes(mu[k], 2.0 ** (1 - k)) for k in range(1, 2 * n)]
    prev = None
    ratio = ddiv(cur[1], cur[0])
    alpha, beta = [ratio], [None]
    for k in range(1, n):
        new = [None] * (2 * n)
        minus_alpha = dneg(alpha[-1])
        minus_beta = None if k == 1 else dneg(beta[-1])
        for l in range(k, 2 * n - k):
            v = dadd(cur[l + 1], dmul(minus_alpha, cur[l]))
            if prev is not None:
                v = dadd(v, dmul(minus_beta, prev[l]))
            new[l] = dadd(v, dtimes(cur[l - 1], 0.5 if l == 1 else 0.25))
        later = ddiv(new[k + 1], new[k])
        alpha.append(dadd(later, dneg(ratio)))
        beta.append(ddiv(new[k], cur[k - 1]))
        prev, cur, ratio = cur, new, later
    return [a[0] for a in alpha], [None if b is None else b[0] for b in beta]


def solution_polynomials(alpha, beta, kappa, one):
    n = len(alpha)
    tau = 0.5 * kappa
    at = [one, tau - alpha[0]]
    for k in range(1, n):
        at.append((tau - alpha[k]) * at[-1] - beta[k] * at[-2])
    before, p = None, [one]
    for k in range(n):
        new = [None] * (k + 2)

        def put(i, v):
            new[i] = v if new[i] is None else new[i] + v

        for i, v in enumerate(p):
            half = 0.5 * v
            put(i + 1, half)
            put(abs(i - 1), half)
        for i, v in enumerate(p):
            put(i, -(alpha[k] * v))
        if before is not None:
            for i, v in enumerate(before):
                put(i, -(beta[k] * v))
        before, p = p, new
    scale = one / at[n]
    residual = [scale * v for v in p]
    rest = [-v for v in residual]
    rest[0] = rest[0] + one
    q = [None] * (n + 2)
    zero = 0.0 * one
    q[n] = q[n + 1] = zero
    for k in range(n, 1, -1):
        q[k - 1] = (q[k] - rest[k]) * kappa - q[k + 1]
    q[0] = (q[1] - rest[1]) * tau - 0.5 * q[2]
    return q[:n], residual


def kernel(nx, nz, sizes, r_hbm, c_hbm, a_hbm, x_out, r_out,
           cond, absorb, diag, weight, fx, fy, fz, ey, turned, wx, wz, field, zsend, zrecv, ysend, yrecv, xrecv,
           part1, part2, dots, table, coef,
           load_sem, face_send, face_recv, sum1_send, sum1_recv, sum2_send, sum2_recv):
    gx, gy, gz = sizes
    ix, iy, iz = lax.axis_index("gx"), lax.axis_index("gy"), lax.axis_index("gz")
    ox = 1 - ix
    base = BASE
    inner = pl.ds(base, nz)
    above = pl.ds(base + 1, nz)
    below = pl.ds(base - 1, nz)
    half = nz // 2
    tiles = nz // 8
    low_x = ix == 0
    border = jnp.where(low_x, nx, 1)

    loads = [
        pltpu.make_async_copy(c_hbm, cond.at[pl.ds(1, nx), inner, :], load_sem.at[0]),
        pltpu.make_async_copy(a_hbm, absorb, load_sem.at[1]),
        pltpu.make_async_copy(r_hbm, r_out, load_sem.at[2]),
    ]
    for load in loads:
        load.start()

    zero_face = jnp.zeros((nx, LANES), F32)
    zero_slab = jnp.zeros((nz, LANES), F32)

    def clear_faces(k, _):
        for side in range(2):
            zrecv[k, side] = zero_face
            yrecv[k, side] = zero_face
        return 0

    lax.fori_loop(0, STEPS + 1, clear_faces, 0)

    barrier = pltpu.get_barrier_semaphore()
    group = [((ix + dx) % gx, (iy + dy) % gy) for dx in range(gx) for dy in range(gy) if (dx, dy) != (0, 0)]
    line = [(iz + d) % gz for d in range(1, gz)]
    for px, py in group:
        pl.semaphore_signal(barrier, inc=1, device_id=(px, py, iz), device_id_type=MESH)
    for pz in line:
        pl.semaphore_signal(barrier, inc=1, device_id=(ix, iy, pz), device_id_type=MESH)

    lane = lax.broadcasted_iota(jnp.int32, (half, LANES), 1)
    pair = lane // 2
    even = (lane % 2) == 0
    row_lane = lax.broadcasted_iota(jnp.int32, (1, LANES), 1)

    def tile_sum(v):
        return jnp.sum(v.reshape(tiles, 8, LANES), axis=0)

    def spread(c, rows=nz):
        return jnp.broadcast_to(c[None], (rows // 8, 8, LANES)).reshape(rows, LANES)

    def turn_of(x, h):
        return 2 * x + 2 * nx * h

    def pack(source):
        out = jnp.zeros((half, LANES), F32)
        for x in range(nx):
            for h in range(2):
                v = source[x + 1, pl.ds(base + half * h, half), :]
                out = jnp.where(pair == x + nx * h, pltpu.roll(v, (turn_of(x, h) + 1) % LANES, 1), out)
        return out

    def copies(source, e):
        xc = pltpu.make_async_remote_copy(
            source.at[border, inner, :], xrecv.at[e],
            face_send.at[e, 0], face_recv.at[e, 0], device_id=(ox, iy, iz), device_id_type=MESH)
        yc, zc = [], []
        for up in range(2):
            yc.append(pltpu.make_async_remote_copy(
                ysend.at[e], yrecv.at[e, 1 - up], face_send.at[e, 1 + up], face_recv.at[e, 2 - up],
                device_id=(ix, jnp.clip(iy + 2 * up - 1, 0, gy - 1), iz), device_id_type=MESH))
            zc.append(pltpu.make_async_remote_copy(
                zsend.at[e, up], zrecv.at[e, 1 - up], face_send.at[e, 3 + up], face_recv.at[e, 4 - up],
                device_id=(ix, iy, jnp.clip(iz + 2 * up - 1, 0, gz - 1)), device_id_type=MESH))
        return xc, yc, zc

    def send(source, e, packed):
        xc, yc, zc = copies(source, e)
        ysend[e] = packed
        zsend[e, 0] = source[pl.ds(1, nx), base, :]
        zsend[e, 1] = source[pl.ds(1, nx), base + nz - 1, :]
        pl.when(iz > 0)(zc[0].start)
        pl.when(iz < gz - 1)(zc[1].start)
        pl.when(iy > 0)(yc[0].start)
        pl.when(iy < gy - 1)(yc[1].start)
        xc.start()

    def receive(source, e):
        xc, yc, zc = copies(source, e)
        xc.wait()
        pl.when(iy > 0)(lambda: (yc[0].wait_send(), yc[1].wait_recv())[0])
        pl.when(iy < gy - 1)(lambda: (yc[1].wait_send(), yc[0].wait_recv())[0])
        pl.when(iz > 0)(lambda: (zc[0].wait_send(), zc[1].wait_recv())[0])
        pl.when(iz < gz - 1)(lambda: (zc[1].wait_send(), zc[0].wait_recv())[0])

    def beside(e):
        return jnp.where(even, yrecv[e, 0], pltpu.roll(yrecv[e, 1], LANES - 2, 1))

    gxy = ix * gy + iy
    first = (part1, [(px, py, iz) for px, py in group], gxy, sum1_send, sum1_recv, [px * gy + py for px, py in group])
    second = (part2, [(ix, iy, pz) for pz in line], iz, sum2_send, sum2_recv, line)

    def spread_out(stage, which):
        part, peers, mine, send_sem, recv_sem, _ = stage
        for i, peer in enumerate(peers):
            pltpu.make_async_remote_copy(
                part.at[which, mine], part.at[which, mine], send_sem.at[which, i], recv_sem.at[which, mine],
                device_id=peer, device_id_type=MESH).start()

    def gather_in(stage, which):
        part, peers, _, send_sem, recv_sem, slots = stage
        for i, slot in enumerate(slots):
            copy = pltpu.make_async_remote_copy(
                part.at[which, slot], part.at[which, slot], send_sem.at[which, i], recv_sem.at[which, slot],
                device_id=peers[i], device_id_type=MESH)
            copy.wait_recv()
            copy.wait_send()
        total, error = part[which, 0], jnp.zeros_like(part[which, 0])
        for i in range(1, part.shape[1]):
            total, e = two_sum(total, part[which, i])
            error = error + e
        return total, error

    def sum_begin(which, row):
        part1[which, gxy] = row
        spread_out(first, which)

    def sum_middle(which):
        high, low = renew(*gather_in(first, which))
        part2[which, iz, pl.ds(0, 1), :] = high
        part2[which, iz, pl.ds(1, 1), :] = low
        spread_out(second, which)

    def sum_end(which):
        total, error = gather_in(second, which)
        return renew(total[0:1], error[0:1] + total[1:2])

    def all_lanes(row, m):
        return jnp.broadcast_to(jnp.sum(jnp.where(row_lane == m, row, 0.0), axis=1, keepdims=True), (8, LANES))

    def one_row(values):
        row = jnp.zeros((1, LANES), F32)
        for m, v in enumerate(values):
            row = jnp.where(row_lane == m, jnp.sum(jnp.sum(v, axis=0, keepdims=True), axis=1, keepdims=True), row)
        return row

    wide_lane = lax.broadcasted_iota(jnp.int32, (nz, LANES), 1)
    inside = wide_lane < LANES - 1
    edge = (wide_lane == 0) | (wide_lane == LANES - 1)
    one = jnp.ones((8, LANES), F32)

    loads[0].wait()
    packed = pack(cond)
    pl.semaphore_wait(barrier, len(group) + len(line))
    send(cond, 0, packed)
    loads[1].wait()

    def means(x, acc):
        return acc[0] + cond[x + 1, inner, :], acc[1] + absorb[x]

    sums = lax.fori_loop(0, nx, means, (zero_slab, zero_slab), unroll=4)
    sum_begin(0, one_row([tile_sum(v) for v in sums]))

    def clear(k, _):
        field[k, 0, inner, :] = zero_slab
        field[k, nx + 1, inner, :] = zero_slab
        field[k, pl.ds(1, nx), base - 1, :] = zero_face
        field[k, pl.ds(1, nx), base + nz, :] = zero_face
        return 0

    lax.fori_loop(0, STEPS, clear, 0)
    table[0, 0] = one
    table[0, 1] = jnp.zeros((8, LANES), F32)
    loads[2].wait()
    receive(cond, 0)
    sum_middle(0)

    cond[jnp.where(low_x, nx + 1, 0), inner, :] = xrecv[0]
    cond[jnp.where(low_x, 0, nx + 1), inner, :] = zero_slab
    cond[pl.ds(1, nx), base - 1, :] = zrecv[0, 0]
    cond[pl.ds(1, nx), base + nz, :] = zrecv[0, 1]
    for_c = beside(0)
    for x in range(nx):
        for h in range(2):
            ey[x, pl.ds(half * h, half), :] = pltpu.roll(for_c, (LANES - turn_of(x, h)) % LANES, 1)
    fx[0] = 0.5 * (cond[0, inner, :] + cond[1, inner, :])

    def coefficients(x, _):
        here = cond[x + 1, inner, :]
        xp = 0.5 * (here + cond[x + 2, inner, :])
        xm = fx[x]
        yp = jnp.where(inside, 0.5 * (here + pltpu.roll(here, LANES - 1, 1)), 0.0)
        ye = jnp.where(edge, 0.5 * (here + ey[x]), 0.0)
        zp = 0.5 * (here + cond[x + 1, above, :])
        zm = 0.5 * (here + cond[x + 1, below, :])
        total = absorb[x] + xp + xm + yp + pltpu.roll(yp, 1, 1) + ye + zp + zm
        inverse = 1.0 / total
        fx[x + 1] = xp
        fy[x] = yp
        ey[x] = ye * inverse
        fz[x, below, :] = zm
        fz[x, inner, :] = zp
        diag[x] = total
        weight[x] = inverse
        field[0, x + 1, inner, :] = r_out[x] * inverse
        return 0

    lax.fori_loop(0, nx, coefficients, 0, unroll=2)
    wx[...] = weight[border - 1] * fx[jnp.where(low_x, nx, 0)]
    wz[0] = weight[pl.ds(0, nx), 0, :] * fz[pl.ds(0, nx), base - 1, :]
    wz[1] = weight[pl.ds(0, nx), nz - 1, :] * fz[pl.ds(0, nx), base + nz - 1, :]

    send(field.at[0], 1, pack(field.at[0]))

    def step(k, _):
        src, dst, old = k, k + 1, jnp.maximum(k - 1, 0)
        e = k + 1

        @pl.when(k == 1)
        def _():
            high, _ = sum_end(0)
            six = 6.0 * all_lanes(high, 0)
            rho = 0.97 * six / (six + all_lanes(high, 1))
            kappa = jnp.floor(64.0 * (2.0 / rho)) * (1.0 / 64.0)
            half_kappa = 0.5 * kappa
            table[1, 0] = kappa * half_kappa
            table[1, 1] = one
            table[2, 0] = kappa
            table[2, 1] = half_kappa
            for j in range(3, STEPS):
                table[j, 0] = kappa
                table[j, 1] = one

        a = table[k, 0]
        a_all, b_all = spread(a), spread(table[k, 1])

        def row(x, acc):
            same, older = acc
            v = field[src, x + 1, inner, :]
            y = fy[x]
            o = field[old, x + 1, inner, :]
            s = fx[x + 1] * field[src, x + 2, inner, :] + fx[x] * field[src, x, inner, :]
            s = s + fz[x, inner, :] * field[src, x + 1, above, :] + fz[x, below, :] * field[src, x + 1, below, :]
            s = s + y * pltpu.roll(v, LANES - 1, 1) + pltpu.roll(y * v, 1, 1)
            field[dst, x + 1, inner, :] = a_all * (weight[x] * s) - b_all * o
            w = diag[x] * v
            return same + w * v, older + w * o

        same, older = lax.fori_loop(0, nx, row, (zero_slab, zero_slab), unroll=4)
        dots[2 * k] = tile_sum(same)
        dots[2 * k + 1] = tile_sum(older)

        receive(field.at[src], e)
        a_half = spread(a, half)
        field[dst, pl.ds(1, nx), base, :] += a_half * wz[0] * zrecv[e, 0]
        field[dst, pl.ds(1, nx), base + nz - 1, :] += a_half * wz[1] * zrecv[e, 1]
        field[dst, border, inner, :] += a_all * wx[...] * xrecv[e]
        sides = a_half * beside(e)
        for x in range(nx):
            for h in range(2):
                turned[x, pl.ds(half * h, half), :] = pltpu.roll(sides, (LANES - turn_of(x, h)) % LANES, 1)

        def add_sides(x, _):
            field[dst, x + 1, inner, :] += ey[x] * turned[x]
            return 0

        lax.fori_loop(0, nx, add_sides, 0, unroll=4)
        packed = pack(field.at[dst])

        @pl.when(k < STEPS - 1)
        def _():
            send(field.at[dst], e + 1, packed)

        return 0

    lax.fori_loop(0, STEPS, step, 0)

    def last_dot(x, acc):
        return acc + diag[x] * field[STEPS, x + 1, inner, :] * field[STEPS - 1, x + 1, inner, :]

    dots[2 * STEPS + 1] = tile_sum(lax.fori_loop(0, nx, last_dot, zero_slab, unroll=4))
    sum_begin(1, one_row([dots[m if m % 2 == 0 else m + 2] for m in range(2 * STEPS)]))
    sum_middle(1)
    high, low = sum_end(1)
    kappa = table[2, 0]
    half_kappa = table[2, 1]
    raw = [(all_lanes(high, m), all_lanes(low, m)) for m in range(2 * STEPS)]
    exact = (half_kappa, jnp.zeros((8, LANES), F32))
    raw[1] = dmul(raw[1], exact)
    raw[2] = dmul(dmul(raw[2], exact), exact)
    raw[3] = dmul(raw[3], exact)
    mu = raw[:2]
    for m in range(2, 2 * STEPS):
        mu.append(dadd(dtimes(raw[m], 2.0), dneg(mu[m % 2])))
    alpha, beta = jacobi_matrix(mu)
    xs, rs = solution_polynomials(alpha, beta, kappa, one)
    xs[1] = xs[1] * half_kappa
    rs[1] = rs[1] * half_kappa
    for k, v in enumerate(xs):
        coef[k] = v
    for k, v in enumerate(rs):
        coef[16 + k] = v

    def finish(x, _):
        v = field[0, x + 1, inner, :]
        sx = spread(coef[0]) * v
        sr = spread(coef[16]) * v
        for k in range(1, STEPS + 1):
            v = field[k, x + 1, inner, :]
            if k < STEPS:
                sx = sx + spread(coef[k]) * v
            sr = sr + spread(coef[16 + k]) * v
        x_out[x] = sx
        r_out[x] = diag[x] * sr
        return 0

    lax.fori_loop(0, nx, finish, 0)


def solution(mesh):
    gx, gy, gz = mesh.shape["gx"], mesh.shape["gy"], mesh.shape["gz"]

    def on_device(right_side, conductivity, absorption):
        nx, ny, nz = right_side.shape
        assert ny == LANES and nx * 2 * 2 == LANES and gx == 2
        args = [jnp.transpose(v, (0, 2, 1)) for v in (right_side, conductivity, absorption)]
        block = (nx, nz, LANES)
        exchanges = STEPS + 1
        dma = pltpu.SemaphoreType.DMA
        tall = nz + 16
        out = pl.pallas_call(
            functools.partial(kernel, nx, nz, (gx, gy, gz)),
            out_shape=[jax.ShapeDtypeStruct(block, F32)] * 2,
            in_specs=[pl.BlockSpec(memory_space=pl.ANY)] * 3,
            out_specs=[pl.BlockSpec(memory_space=pltpu.VMEM)] * 2,
            scratch_shapes=[
                pltpu.VMEM((nx + 2, tall, LANES), F32),
                pltpu.VMEM(block, F32),
                pltpu.VMEM(block, F32),
                pltpu.VMEM(block, F32),
                pltpu.VMEM((nx + 1, nz, LANES), F32),
                pltpu.VMEM(block, F32),
                pltpu.VMEM((nx, tall, LANES), F32),
                pltpu.VMEM(block, F32),
                pltpu.VMEM(block, F32),
                pltpu.VMEM((nz, LANES), F32),
                pltpu.VMEM((2, nx, LANES), F32),
                pltpu.VMEM((STEPS + 1, nx + 2, tall, LANES), F32),
                pltpu.VMEM((exchanges, 2, nx, LANES), F32),
                pltpu.VMEM((exchanges, 2, nx, LANES), F32),
                pltpu.VMEM((exchanges, nz // 2, LANES), F32),
                pltpu.VMEM((exchanges, 2, nz // 2, LANES), F32),
                pltpu.VMEM((exchanges, nz, LANES), F32),
                pltpu.VMEM((2, gx * gy, 1, LANES), F32),
                pltpu.VMEM((2, gz, 2, LANES), F32),
                pltpu.VMEM((2 * STEPS + 2, 8, LANES), F32),
                pltpu.VMEM((STEPS, 2, 8, LANES), F32),
                pltpu.VMEM((32, 8, LANES), F32),
                dma((3,)),
                dma((exchanges, 5)),
                dma((exchanges, 5)),
                dma((2, gx * gy)),
                dma((2, gx * gy)),
                dma((2, gz)),
                dma((2, gz)),
            ],
            compiler_params=pltpu.CompilerParams(
                collective_id=0, has_side_effects=True, vmem_limit_bytes=48 * 1024 * 1024
            ),
        )(*[pltpu.with_memory_space_constraint(v, pltpu.HBM) for v in args])
        return tuple(jnp.transpose(v, (0, 2, 1)) for v in out)

    spec = P("gx", "gy", "gz")
    return jax.shard_map(on_device, mesh=mesh, in_specs=(spec,) * 3, out_specs=(spec,) * 2, check_vma=False)
```

```python
import functools

import jax
import jax.numpy as jnp
from jax import lax
from jax.experimental import pallas as pl
from jax.experimental.pallas import tpu as pltpu
from jax.sharding import PartitionSpec as P

F32 = jnp.float32
MESH = pl.DeviceIdType.MESH
STEPS = 10
LANES = 128
BASE = 8


def two_sum(a, b):
    s = a + b
    t = s - a
    return s, (a - (s - t)) + (b - t)


def renew(a, b):
    s = a + b
    return s, b - (s - a)


def halves(a):
    t = 4097.0 * a
    high = t - (t - a)
    return high, a - high


def two_product(a, b):
    p = a * b
    ah, al = halves(a)
    bh, bl = halves(b)
    return p, ((ah * bh - p) + ah * bl + al * bh) + al * bl


def dadd(a, b):
    s, e = two_sum(a[0], b[0])
    return renew(s, e + (a[1] + b[1]))


def dneg(a):
    return -a[0], -a[1]


def dmul(a, b):
    p, e = two_product(a[0], b[0])
    return renew(p, e + (a[0] * b[1] + a[1] * b[0]))


def dtimes(a, power):
    return power * a[0], power * a[1]


def ddiv(a, b):
    q = a[0] / b[0]
    p, e = two_product(q, b[0])
    rest = ((a[0] - p) - e) + (a[1] - q * b[1])
    return renew(q, rest / b[0])


def jacobi_matrix(mu):
    n = len(mu) // 2
    cur = [mu[0]] + [dtimes(mu[k], 2.0 ** (1 - k)) for k in range(1, 2 * n)]
    prev = None
    ratio = ddiv(cur[1], cur[0])
    alpha, beta = [ratio], [None]
    for k in range(1, n):
        new = [None] * (2 * n)
        minus_alpha = dneg(alpha[-1])
        minus_beta = None if k == 1 else dneg(beta[-1])
        for l in range(k, 2 * n - k):
            v = dadd(cur[l + 1], dmul(minus_alpha, cur[l]))
            if prev is not None:
                v = dadd(v, dmul(minus_beta, prev[l]))
            new[l] = dadd(v, dtimes(cur[l - 1], 0.5 if l == 1 else 0.25))
        later = ddiv(new[k + 1], new[k])
        alpha.append(dadd(later, dneg(ratio)))
        beta.append(ddiv(new[k], cur[k - 1]))
        prev, cur, ratio = cur, new, later
    return [a[0] for a in alpha], [None if b is None else b[0] for b in beta]


def solution_polynomials(alpha, beta, kappa, one):
    n = len(alpha)
    tau = 0.5 * kappa
    at = [one, tau - alpha[0]]
    for k in range(1, n):
        at.append((tau - alpha[k]) * at[-1] - beta[k] * at[-2])
    before, p = None, [one]
    for k in range(n):
        new = [None] * (k + 2)

        def put(i, v):
            new[i] = v if new[i] is None else new[i] + v

        for i, v in enumerate(p):
            half = 0.5 * v
            put(i + 1, half)
            put(abs(i - 1), half)
        for i, v in enumerate(p):
            put(i, -(alpha[k] * v))
        if before is not None:
            for i, v in enumerate(before):
                put(i, -(beta[k] * v))
        before, p = p, new
    scale = one / at[n]
    residual = [scale * v for v in p]
    rest = [-v for v in residual]
    rest[0] = rest[0] + one
    q = [None] * (n + 2)
    zero = 0.0 * one
    q[n] = q[n + 1] = zero
    for k in range(n, 1, -1):
        q[k - 1] = (q[k] - rest[k]) * kappa - q[k + 1]
    q[0] = (q[1] - rest[1]) * tau - 0.5 * q[2]
    return q[:n], residual


def kernel(nx, nz, sizes, r_hbm, c_hbm, a_hbm, x_out, r_out,
           cond, absorb, diag, weight, fx, fy, fz, turned, wx, wy, wz, xadd, yadd, zadd, field, xsend, zsend, zrecv, ysend, yrecv, xrecv,
           part1, part2, dots, table, coef,
           load_sem, face_send, face_recv, sum1_send, sum1_recv, sum2_send, sum2_recv):
    gx, gy, gz = sizes
    ix, iy, iz = lax.axis_index("gx"), lax.axis_index("gy"), lax.axis_index("gz")
    ox = 1 - ix
    base = BASE
    inner = pl.ds(base, nz)
    above = pl.ds(base + 1, nz)
    below = pl.ds(base - 1, nz)
    half = nz // 2
    tiles = nz // 8
    low_x = ix == 0
    border = jnp.where(low_x, nx, 1)

    loads = [
        pltpu.make_async_copy(c_hbm, cond.at[pl.ds(1, nx), inner, :], load_sem.at[0]),
        pltpu.make_async_copy(a_hbm, absorb, load_sem.at[1]),
        pltpu.make_async_copy(r_hbm, r_out, load_sem.at[2]),
    ]
    for load in loads:
        load.start()

    zero_face = jnp.zeros((nx, LANES), F32)
    zero_slab = jnp.zeros((nz, LANES), F32)

    def clear_faces(k, _):
        for side in range(2):
            zrecv[k, side] = zero_face
            yrecv[k, side] = zero_face
        return 0

    lax.fori_loop(0, STEPS + 1, clear_faces, 0)

    barrier = pltpu.get_barrier_semaphore()
    group = [((ix + dx) % gx, (iy + dy) % gy) for dx in range(gx) for dy in range(gy) if (dx, dy) != (0, 0)]
    line = [(iz + d) % gz for d in range(1, gz)]
    for px, py in group:
        pl.semaphore_signal(barrier, inc=1, device_id=(px, py, iz), device_id_type=MESH)
    for pz in line:
        pl.semaphore_signal(barrier, inc=1, device_id=(ix, iy, pz), device_id_type=MESH)

    lane = lax.broadcasted_iota(jnp.int32, (half, LANES), 1)
    pair = lane // 2
    even = (lane % 2) == 0
    row_lane = lax.broadcasted_iota(jnp.int32, (1, LANES), 1)

    def tile_sum(v):
        return jnp.sum(v.reshape(tiles, 8, LANES), axis=0)

    def spread(c, rows=nz):
        return jnp.broadcast_to(c[None], (rows // 8, 8, LANES)).reshape(rows, LANES)

    def turn_of(x, h):
        return 2 * x + 2 * nx * h

    def pack(source):
        out = jnp.zeros((half, LANES), F32)
        for x in range(nx):
            for h in range(2):
                v = source[x + 1, pl.ds(base + half * h, half), :]
                out = jnp.where(pair == x + nx * h, pltpu.roll(v, (turn_of(x, h) + 1) % LANES, 1), out)
        return out

    def copies(e):
        xc = pltpu.make_async_remote_copy(
            xsend.at[e], xrecv.at[e],
            face_send.at[e, 0], face_recv.at[e, 0], device_id=(ox, iy, iz), device_id_type=MESH)
        yc, zc = [], []
        for up in range(2):
            yc.append(pltpu.make_async_remote_copy(
                ysend.at[e], yrecv.at[e, 1 - up], face_send.at[e, 1 + up], face_recv.at[e, 2 - up],
                device_id=(ix, jnp.clip(iy + 2 * up - 1, 0, gy - 1), iz), device_id_type=MESH))
            zc.append(pltpu.make_async_remote_copy(
                zsend.at[e, up], zrecv.at[e, 1 - up], face_send.at[e, 3 + up], face_recv.at[e, 4 - up],
                device_id=(ix, iy, jnp.clip(iz + 2 * up - 1, 0, gz - 1)), device_id_type=MESH))
        return xc, yc, zc

    def send(e):
        xc, yc, zc = copies(e)
        pl.when(iz > 0)(zc[0].start)
        pl.when(iz < gz - 1)(zc[1].start)
        pl.when(iy > 0)(yc[0].start)
        pl.when(iy < gy - 1)(yc[1].start)
        xc.start()

    def send_field(source, e):
        ysend[e] = pack(source)
        zsend[e, 0] = source[pl.ds(1, nx), base, :]
        zsend[e, 1] = source[pl.ds(1, nx), base + nz - 1, :]
        xsend[e] = source[border, inner, :]
        send(e)

    def receive(e):
        xc, yc, zc = copies(e)
        xc.wait()
        pl.when(iy > 0)(lambda: (yc[0].wait_send(), yc[1].wait_recv())[0])
        pl.when(iy < gy - 1)(lambda: (yc[1].wait_send(), yc[0].wait_recv())[0])
        pl.when(iz > 0)(lambda: (zc[0].wait_send(), zc[1].wait_recv())[0])
        pl.when(iz < gz - 1)(lambda: (zc[1].wait_send(), zc[0].wait_recv())[0])

    def beside(e):
        return jnp.where(even, yrecv[e, 0], pltpu.roll(yrecv[e, 1], LANES - 2, 1))

    gxy = ix * gy + iy
    first = (part1, [(px, py, iz) for px, py in group], gxy, sum1_send, sum1_recv, [px * gy + py for px, py in group])
    second = (part2, [(ix, iy, pz) for pz in line], iz, sum2_send, sum2_recv, line)

    def spread_out(stage, which):
        part, peers, mine, send_sem, recv_sem, _ = stage
        for i, peer in enumerate(peers):
            pltpu.make_async_remote_copy(
                part.at[which, mine], part.at[which, mine], send_sem.at[which, i], recv_sem.at[which, mine],
                device_id=peer, device_id_type=MESH).start()

    def gather_in(stage, which):
        part, peers, _, send_sem, recv_sem, slots = stage
        for i, slot in enumerate(slots):
            copy = pltpu.make_async_remote_copy(
                part.at[which, slot], part.at[which, slot], send_sem.at[which, i], recv_sem.at[which, slot],
                device_id=peers[i], device_id_type=MESH)
            copy.wait_recv()
            copy.wait_send()
        total, error = part[which, 0], jnp.zeros_like(part[which, 0])
        for i in range(1, part.shape[1]):
            total, e = two_sum(total, part[which, i])
            error = error + e
        return total, error

    def sum_begin(which, row):
        part1[which, gxy] = row
        spread_out(first, which)

    def sum_middle(which):
        high, low = renew(*gather_in(first, which))
        part2[which, iz, pl.ds(0, 1), :] = high
        part2[which, iz, pl.ds(1, 1), :] = low
        spread_out(second, which)

    def sum_end(which):
        total, error = gather_in(second, which)
        return renew(total[0:1], error[0:1] + total[1:2])

    def all_lanes(row, m):
        return jnp.broadcast_to(jnp.sum(jnp.where(row_lane == m, row, 0.0), axis=1, keepdims=True), (8, LANES))

    def one_row(values):
        row = jnp.zeros((1, LANES), F32)
        for m, v in enumerate(values):
            row = jnp.where(row_lane == m, jnp.sum(jnp.sum(v, axis=0, keepdims=True), axis=1, keepdims=True), row)
        return row

    wide_lane = lax.broadcasted_iota(jnp.int32, (nz, LANES), 1)
    inside = wide_lane < LANES - 1
    edge = (wide_lane == 0) | (wide_lane == LANES - 1)
    one = jnp.ones((8, LANES), F32)

    loads[0].wait()
    pl.semaphore_wait(barrier, len(group) + len(line))
    send_field(cond, 0)
    loads[1].wait()

    def means(x, acc):
        return acc[0] + cond[x + 1, inner, :], acc[1] + absorb[x]

    sums = lax.fori_loop(0, nx, means, (zero_slab, zero_slab), unroll=4)
    sum_begin(0, one_row([tile_sum(v) for v in sums]))

    def clear(k, _):
        field[k, 0, inner, :] = zero_slab
        field[k, nx + 1, inner, :] = zero_slab
        field[k, pl.ds(1, nx), base - 1, :] = zero_face
        field[k, pl.ds(1, nx), base + nz, :] = zero_face
        return 0

    lax.fori_loop(0, STEPS, clear, 0)
    table[0, 0] = one
    table[0, 1] = jnp.zeros((8, LANES), F32)
    loads[2].wait()
    receive(0)
    sum_middle(0)

    cond[jnp.where(low_x, nx + 1, 0), inner, :] = xrecv[0]
    cond[jnp.where(low_x, 0, nx + 1), inner, :] = zero_slab
    cond[pl.ds(1, nx), base - 1, :] = zrecv[0, 0]
    cond[pl.ds(1, nx), base + nz, :] = zrecv[0, 1]
    for_c = beside(0)
    for x in range(nx):
        for h in range(2):
            turned[x, pl.ds(half * h, half), :] = pltpu.roll(for_c, (LANES - turn_of(x, h)) % LANES, 1)
    fx[0] = 0.5 * (cond[0, inner, :] + cond[1, inner, :])

    def coefficients(x, _):
        here = cond[x + 1, inner, :]
        xp = 0.5 * (here + cond[x + 2, inner, :])
        xm = fx[x]
        yp = jnp.where(inside, 0.5 * (here + pltpu.roll(here, LANES - 1, 1)), 0.0)
        ye = jnp.where(edge, 0.5 * (here + turned[x]), 0.0)
        zp = 0.5 * (here + cond[x + 1, above, :])
        zm = 0.5 * (here + cond[x + 1, below, :])
        total = absorb[x] + xp + xm + yp + pltpu.roll(yp, 1, 1) + ye + zp + zm
        inverse = 1.0 / total
        fx[x + 1] = xp
        fy[x] = yp
        turned[x] = ye * inverse
        fz[x, below, :] = zm
        fz[x, inner, :] = zp
        diag[x] = total
        weight[x] = inverse
        field[0, x + 1, inner, :] = r_out[x] * inverse
        return 0

    lax.fori_loop(0, nx, coefficients, 0, unroll=2)
    wx[...] = weight[border - 1] * fx[jnp.where(low_x, nx, 0)]
    wz[0] = weight[pl.ds(0, nx), 0, :] * fz[pl.ds(0, nx), base - 1, :]
    wz[1] = weight[pl.ds(0, nx), nz - 1, :] * fz[pl.ds(0, nx), base + nz - 1, :]

    send_field(field.at[0], 1)
    packed = jnp.zeros((half, LANES), F32)
    for x in range(nx):
        for h in range(2):
            v = turned[x, pl.ds(half * h, half), :]
            packed = jnp.where(pair == x + nx * h, pltpu.roll(v, (turn_of(x, h) + 1) % LANES, 1), packed)
    wy[...] = packed
    zadd[0] = zero_face
    zadd[1] = zero_face
    xadd[...] = zero_slab
    yadd[...] = jnp.zeros((half, LANES), F32)

    face_row = lax.broadcasted_iota(jnp.int32, (nx, LANES), 0)
    face_lane = lax.broadcasted_iota(jnp.int32, (nx, LANES), 1)
    half_row = lax.broadcasted_iota(jnp.int32, (half, LANES), 0)
    slab_row = lax.broadcasted_iota(jnp.int32, (nz, LANES), 0)

    def correct(k):
        field[k, pl.ds(1, nx), base, :] += zadd[0]
        field[k, pl.ds(1, nx), base + nz - 1, :] += zadd[1]
        field[k, border, inner, :] += xadd[...]
        terms = yadd[...]
        for x in range(nx):
            for h in range(2):
                turned[x, pl.ds(half * h, half), :] = pltpu.roll(terms, (LANES - turn_of(x, h) - 1) % LANES, 1)

        def add_sides(x, _):
            field[k, x + 1, inner, :] += jnp.where(edge, turned[x], 0.0)
            return 0

        lax.fori_loop(0, nx, add_sides, 0, unroll=4)

    def step(k, _):
        src, dst, old = k, k + 1, jnp.maximum(k - 1, 0)
        e = k + 1

        @pl.when(k == 1)
        def _():
            high, _ = sum_end(0)
            six = 6.0 * all_lanes(high, 0)
            rho = 0.97 * six / (six + all_lanes(high, 1))
            kappa = jnp.floor(64.0 * (2.0 / rho)) * (1.0 / 64.0)
            half_kappa = 0.5 * kappa
            table[1, 0] = kappa * half_kappa
            table[1, 1] = one
            table[2, 0] = kappa
            table[2, 1] = half_kappa
            for j in range(3, STEPS):
                table[j, 0] = kappa
                table[j, 1] = one

        correct(k)
        a = table[k, 0]
        a_all, b_all = spread(a), spread(table[k, 1])

        def row(x, acc):
            same, older = acc
            v = field[src, x + 1, inner, :]
            y = fy[x]
            o = field[old, x + 1, inner, :]
            s = fx[x + 1] * field[src, x + 2, inner, :] + fx[x] * field[src, x, inner, :]
            s = s + fz[x, inner, :] * field[src, x + 1, above, :] + fz[x, below, :] * field[src, x + 1, below, :]
            s = s + y * pltpu.roll(v, LANES - 1, 1) + pltpu.roll(y * v, 1, 1)
            field[dst, x + 1, inner, :] = a_all * (weight[x] * s) - b_all * o
            w = diag[x] * v
            return same + w * v, older + w * o

        same, older = lax.fori_loop(0, nx, row, (zero_slab, zero_slab), unroll=4)
        dots[2 * k] = tile_sum(same)
        dots[2 * k + 1] = tile_sum(older)

        ypart = pack(field.at[dst])
        zpart = [field[dst, pl.ds(1, nx), base + row_, :] for row_ in (0, nz - 1)]
        xpart = field[dst, border, inner, :]

        receive(e)
        a_half = spread(a, half)
        sides = jnp.where(even, pltpu.roll(yrecv[e, 1], LANES - 1, 1), pltpu.roll(yrecv[e, 0], 1, 1))
        ya = a_half * wy[...] * sides
        za = [a_half * wz[i] * zrecv[e, i] for i in range(2)]
        xa = a_all * wx[...] * xrecv[e]
        yadd[...] = ya
        zadd[0] = za[0]
        zadd[1] = za[1]
        xadd[...] = xa

        @pl.when(k < STEPS - 1)
        def _():
            yface, xface = ypart + ya, xpart + xa
            xlanes = []
            for h in range(2):
                here = 2 * nx * h + 1
                at = half_row == (nz - 1 - half) * h
                moved = jnp.where(face_lane // 2 == face_row + nx * h, pltpu.roll(za[h], here, 1, stride=2, stride_axis=0), 0.0)
                yface = yface + jnp.where(at, jnp.sum(moved, axis=0, keepdims=True), 0.0)
                xa_half = xa[half * h:half * (h + 1)]
                turns = [(2 * (nx - 1) + here) % LANES, here]
                moved = jnp.where(low_x, pltpu.roll(xa_half, turns[0], 1), pltpu.roll(xa_half, turns[1], 1))
                yface = yface + jnp.where(pair == border - 1 + nx * h, moved, 0.0)
                moved = jnp.where(low_x, pltpu.roll(ya, (LANES - turns[0]) % LANES, 1), pltpu.roll(ya, LANES - turns[1], 1))
                xlanes.append(moved)
                line_ = jnp.sum(jnp.where(at, ya, 0.0), axis=0, keepdims=True)
                zface = zpart[h] + za[h]
                for at_lane, shift in ((LANES - 1, 0), (0, 1)):
                    one_lane = jnp.where(face_lane == 2 * face_row + 2 * nx * h + shift, line_, 0.0)
                    zface = zface + jnp.where(face_lane == at_lane, jnp.sum(one_lane, axis=1, keepdims=True), 0.0)
                z_at = slab_row == (nz - 1) * h
                zface = zface + jnp.where(face_row == border - 1, jnp.sum(jnp.where(z_at, xa, 0.0), axis=0, keepdims=True), 0.0)
                zsend[e + 1, h] = zface
                xface = xface + jnp.where(z_at, jnp.sum(jnp.where(face_row == border - 1, za[h], 0.0), axis=0, keepdims=True), 0.0)
            xsend[e + 1] = xface + jnp.where(edge, jnp.concatenate(xlanes, axis=0), 0.0)
            ysend[e + 1] = yface
            send(e + 1)

        return 0

    lax.fori_loop(0, STEPS, step, 0)
    correct(STEPS)

    def last_dot(x, acc):
        return acc + diag[x] * field[STEPS, x + 1, inner, :] * field[STEPS - 1, x + 1, inner, :]

    dots[2 * STEPS + 1] = tile_sum(lax.fori_loop(0, nx, last_dot, zero_slab, unroll=4))
    sum_begin(1, one_row([dots[m if m % 2 == 0 else m + 2] for m in range(2 * STEPS)]))
    sum_middle(1)
    high, low = sum_end(1)
    kappa = table[2, 0]
    half_kappa = table[2, 1]
    raw = [(all_lanes(high, m), all_lanes(low, m)) for m in range(2 * STEPS)]
    exact = (half_kappa, jnp.zeros((8, LANES), F32))
    raw[1] = dmul(raw[1], exact)
    raw[2] = dmul(dmul(raw[2], exact), exact)
    raw[3] = dmul(raw[3], exact)
    mu = raw[:2]
    for m in range(2, 2 * STEPS):
        mu.append(dadd(dtimes(raw[m], 2.0), dneg(mu[m % 2])))
    alpha, beta = jacobi_matrix(mu)
    xs, rs = solution_polynomials(alpha, beta, kappa, one)
    xs[1] = xs[1] * half_kappa
    rs[1] = rs[1] * half_kappa
    for k, v in enumerate(xs):
        coef[k] = v
    for k, v in enumerate(rs):
        coef[16 + k] = v

    def finish(x, _):
        v = field[0, x + 1, inner, :]
        sx = spread(coef[0]) * v
        sr = spread(coef[16]) * v
        for k in range(1, STEPS + 1):
            v = field[k, x + 1, inner, :]
            if k < STEPS:
                sx = sx + spread(coef[k]) * v
            sr = sr + spread(coef[16 + k]) * v
        x_out[x] = sx
        r_out[x] = diag[x] * sr
        return 0

    lax.fori_loop(0, nx, finish, 0)


def solution(mesh):
    gx, gy, gz = mesh.shape["gx"], mesh.shape["gy"], mesh.shape["gz"]

    def on_device(right_side, conductivity, absorption):
        nx, ny, nz = right_side.shape
        assert ny == LANES and nx * 2 * 2 == LANES and gx == 2
        args = [jnp.transpose(v, (0, 2, 1)) for v in (right_side, conductivity, absorption)]
        block = (nx, nz, LANES)
        exchanges = STEPS + 1
        dma = pltpu.SemaphoreType.DMA
        tall = nz + 16
        out = pl.pallas_call(
            functools.partial(kernel, nx, nz, (gx, gy, gz)),
            out_shape=[jax.ShapeDtypeStruct(block, F32)] * 2,
            in_specs=[pl.BlockSpec(memory_space=pl.ANY)] * 3,
            out_specs=[pl.BlockSpec(memory_space=pltpu.VMEM)] * 2,
            scratch_shapes=[
                pltpu.VMEM((nx + 2, tall, LANES), F32),
                pltpu.VMEM(block, F32),
                pltpu.VMEM(block, F32),
                pltpu.VMEM(block, F32),
                pltpu.VMEM((nx + 1, nz, LANES), F32),
                pltpu.VMEM(block, F32),
                pltpu.VMEM((nx, tall, LANES), F32),
                pltpu.VMEM(block, F32),
                pltpu.VMEM((nz, LANES), F32),
                pltpu.VMEM((nz // 2, LANES), F32),
                pltpu.VMEM((2, nx, LANES), F32),
                pltpu.VMEM((nz, LANES), F32),
                pltpu.VMEM((nz // 2, LANES), F32),
                pltpu.VMEM((2, nx, LANES), F32),
                pltpu.VMEM((STEPS + 1, nx + 2, tall, LANES), F32),
                pltpu.VMEM((exchanges, nz, LANES), F32),
                pltpu.VMEM((exchanges, 2, nx, LANES), F32),
                pltpu.VMEM((exchanges, 2, nx, LANES), F32),
                pltpu.VMEM((exchanges, nz // 2, LANES), F32),
                pltpu.VMEM((exchanges, 2, nz // 2, LANES), F32),
                pltpu.VMEM((exchanges, nz, LANES), F32),
                pltpu.VMEM((2, gx * gy, 1, LANES), F32),
                pltpu.VMEM((2, gz, 2, LANES), F32),
                pltpu.VMEM((2 * STEPS + 2, 8, LANES), F32),
                pltpu.VMEM((STEPS, 2, 8, LANES), F32),
                pltpu.VMEM((32, 8, LANES), F32),
                dma((3,)),
                dma((exchanges, 5)),
                dma((exchanges, 5)),
                dma((2, gx * gy)),
                dma((2, gx * gy)),
                dma((2, gz)),
                dma((2, gz)),
            ],
            compiler_params=pltpu.CompilerParams(
                collective_id=0, has_side_effects=True, vmem_limit_bytes=48 * 1024 * 1024
            ),
        )(*[pltpu.with_memory_space_constraint(v, pltpu.HBM) for v in args])
        return tuple(jnp.transpose(v, (0, 2, 1)) for v in out)

    spec = P("gx", "gy", "gz")
    return jax.shard_map(on_device, mesh=mesh, in_specs=(spec,) * 3, out_specs=(spec,) * 2, check_vma=False)
```

```python
import functools

import jax
import jax.numpy as jnp
from jax import lax
from jax.experimental import pallas as pl
from jax.experimental.pallas import tpu as pltpu
from jax.sharding import PartitionSpec as P

F32 = jnp.float32
MESH = pl.DeviceIdType.MESH
STEPS = 10
LANES = 128
BASE = 8


def two_sum(a, b):
    s = a + b
    t = s - a
    return s, (a - (s - t)) + (b - t)


def renew(a, b):
    s = a + b
    return s, b - (s - a)


def halves(a):
    t = 4097.0 * a
    high = t - (t - a)
    return high, a - high


def two_product(a, b):
    p = a * b
    ah, al = halves(a)
    bh, bl = halves(b)
    return p, ((ah * bh - p) + ah * bl + al * bh) + al * bl


def dadd(a, b):
    s, e = two_sum(a[0], b[0])
    return renew(s, e + (a[1] + b[1]))


def dneg(a):
    return -a[0], -a[1]


def dmul(a, b):
    p, e = two_product(a[0], b[0])
    return renew(p, e + (a[0] * b[1] + a[1] * b[0]))


def dtimes(a, power):
    return power * a[0], power * a[1]


def ddiv(a, b):
    q = a[0] / b[0]
    p, e = two_product(q, b[0])
    rest = ((a[0] - p) - e) + (a[1] - q * b[1])
    return renew(q, rest / b[0])


def jacobi_matrix(mu):
    n = (len(mu) + 1) // 2
    zero = (0.0 * mu[0][0], 0.0 * mu[0][0])
    cur = [mu[0]] + [dtimes(mu[k], 2.0 ** (1 - k)) for k in range(1, 2 * n - 1)] + [zero]
    prev = None
    ratio = ddiv(cur[1], cur[0])
    alpha, beta = [ratio], [None]
    for k in range(1, n):
        new = [None] * (2 * n)
        minus_alpha = dneg(alpha[-1])
        minus_beta = None if k == 1 else dneg(beta[-1])
        for l in range(k, 2 * n - k):
            v = dadd(cur[l + 1], dmul(minus_alpha, cur[l]))
            if prev is not None:
                v = dadd(v, dmul(minus_beta, prev[l]))
            new[l] = dadd(v, dtimes(cur[l - 1], 0.5 if l == 1 else 0.25))
        beta.append(ddiv(new[k], cur[k - 1]))
        prev, cur = cur, new
        if k < n - 1:
            later = ddiv(new[k + 1], new[k])
            alpha.append(dadd(later, dneg(ratio)))
            ratio = later
    high = [a[0] for a in alpha], [None if b is None else b[0] for b in beta]
    return high[0], high[1], cur[n], cur[n - 1], ratio


def without_pole(p, kappa):
    n = len(p) - 1
    q = [None] * (n + 2)
    q[n] = q[n + 1] = 0.0 * kappa
    for k in range(n, 1, -1):
        q[k - 1] = (q[k] + p[k]) * kappa - q[k + 1]
    q[0] = (q[1] + p[1]) * (0.5 * kappa) - 0.5 * q[2]
    return q[:n]


def solution_polynomials(alpha, beta, kappa, one):
    n = len(beta)
    tau = 0.5 * kappa
    at = [one, tau - alpha[0]]
    for k in range(1, n - 1):
        at.append((tau - alpha[k]) * at[-1] - beta[k] * at[-2])
    before, p = None, [one]
    for k in range(n):
        new = [None] * (k + 2)

        def put(i, v):
            new[i] = v if new[i] is None else new[i] + v

        for i, v in enumerate(p):
            half = 0.5 * v
            put(i + 1, half)
            put(abs(i - 1), half)
        if k < n - 1:
            for i, v in enumerate(p):
                put(i, -(alpha[k] * v))
        if before is not None:
            for i, v in enumerate(before):
                put(i, -(beta[k] * v))
        before, p = p, new
    v = before + [0.0 * one]
    at_u = tau * at[-1] - beta[n - 1] * at[-2]
    return p, v, without_pole(p, kappa), without_pole(v, kappa), at_u, at[-1]


def kernel(nx, nz, sizes, r_hbm, c_hbm, a_hbm, x_out, r_out,
           cond, absorb, diag, weight, fx, fy, fz, turned, wx, wy, dy, wz, xadd, yadd, zadd, field, xsend, zsend, zrecv, ysend, yrecv, xrecv,
           part1, part2, dots, table, coef,
           load_sem, face_send, face_recv, sum1_send, sum1_recv, sum2_send, sum2_recv):
    gx, gy, gz = sizes
    ix, iy, iz = lax.axis_index("gx"), lax.axis_index("gy"), lax.axis_index("gz")
    ox = 1 - ix
    base = BASE
    inner = pl.ds(base, nz)
    above = pl.ds(base + 1, nz)
    below = pl.ds(base - 1, nz)
    half = nz // 2
    tiles = nz // 8
    low_x = ix == 0
    border = jnp.where(low_x, nx, 1)

    loads = [
        pltpu.make_async_copy(c_hbm, cond.at[pl.ds(1, nx), inner, :], load_sem.at[0]),
        pltpu.make_async_copy(a_hbm, absorb, load_sem.at[1]),
        pltpu.make_async_copy(r_hbm, r_out, load_sem.at[2]),
    ]
    for load in loads:
        load.start()

    zero_face = jnp.zeros((nx, LANES), F32)
    zero_slab = jnp.zeros((nz, LANES), F32)

    def clear_faces(k, _):
        for side in range(2):
            zrecv[k, side] = zero_face
            yrecv[k, side] = zero_face
        return 0

    lax.fori_loop(0, STEPS + 1, clear_faces, 0)

    barrier = pltpu.get_barrier_semaphore()
    group = [((ix + dx) % gx, (iy + dy) % gy) for dx in range(gx) for dy in range(gy) if (dx, dy) != (0, 0)]
    line = [(iz + d) % gz for d in range(1, gz)]
    for px, py in group:
        pl.semaphore_signal(barrier, inc=1, device_id=(px, py, iz), device_id_type=MESH)
    for pz in line:
        pl.semaphore_signal(barrier, inc=1, device_id=(ix, iy, pz), device_id_type=MESH)

    lane = lax.broadcasted_iota(jnp.int32, (half, LANES), 1)
    pair = lane // 2
    even = (lane % 2) == 0
    row_lane = lax.broadcasted_iota(jnp.int32, (1, LANES), 1)

    def tile_sum(v):
        return jnp.sum(v.reshape(tiles, 8, LANES), axis=0)

    def spread(c, rows=nz):
        return jnp.broadcast_to(c[None], (rows // 8, 8, LANES)).reshape(rows, LANES)

    def turn_of(x, h):
        return 2 * x + 2 * nx * h

    def pack(source, skip=1, start=base):
        out = jnp.zeros((half, LANES), F32)
        for x in range(nx):
            for h in range(2):
                v = source[x + skip, pl.ds(start + half * h, half), :]
                out = jnp.where(pair == x + nx * h, pltpu.roll(v, (turn_of(x, h) + 1) % LANES, 1), out)
        return out

    def copies(e):
        xc = pltpu.make_async_remote_copy(
            xsend.at[e], xrecv.at[e],
            face_send.at[e, 0], face_recv.at[e, 0], device_id=(ox, iy, iz), device_id_type=MESH)
        yc, zc = [], []
        for up in range(2):
            yc.append(pltpu.make_async_remote_copy(
                ysend.at[e], yrecv.at[e, 1 - up], face_send.at[e, 1 + up], face_recv.at[e, 2 - up],
                device_id=(ix, jnp.clip(iy + 2 * up - 1, 0, gy - 1), iz), device_id_type=MESH))
            zc.append(pltpu.make_async_remote_copy(
                zsend.at[e, up], zrecv.at[e, 1 - up], face_send.at[e, 3 + up], face_recv.at[e, 4 - up],
                device_id=(ix, iy, jnp.clip(iz + 2 * up - 1, 0, gz - 1)), device_id_type=MESH))
        return xc, yc, zc

    def send_z(e):
        _, _, zc = copies(e)
        pl.when(iz > 0)(zc[0].start)
        pl.when(iz < gz - 1)(zc[1].start)

    def send_xy(e):
        xc, yc, _ = copies(e)
        pl.when(iy > 0)(yc[0].start)
        pl.when(iy < gy - 1)(yc[1].start)
        xc.start()

    def send_field(source, e):
        zsend[e, 0] = source[pl.ds(1, nx), base, :]
        zsend[e, 1] = source[pl.ds(1, nx), base + nz - 1, :]
        send_z(e)
        ysend[e] = pack(source)
        xsend[e] = source[border, inner, :]
        send_xy(e)

    def receive(e):
        xc, yc, zc = copies(e)
        xc.wait()
        pl.when(iy > 0)(lambda: (yc[0].wait_send(), yc[1].wait_recv())[0])
        pl.when(iy < gy - 1)(lambda: (yc[1].wait_send(), yc[0].wait_recv())[0])
        pl.when(iz > 0)(lambda: (zc[0].wait_send(), zc[1].wait_recv())[0])
        pl.when(iz < gz - 1)(lambda: (zc[1].wait_send(), zc[0].wait_recv())[0])

    def beside(e):
        return jnp.where(even, yrecv[e, 0], pltpu.roll(yrecv[e, 1], LANES - 2, 1))

    gxy = ix * gy + iy
    first = (part1, [(px, py, iz) for px, py in group], gxy, sum1_send, sum1_recv, [px * gy + py for px, py in group])
    second = (part2, [(ix, iy, pz) for pz in line], iz, sum2_send, sum2_recv, line)

    def spread_out(stage, which):
        part, peers, mine, send_sem, recv_sem, _ = stage
        for i, peer in enumerate(peers):
            pltpu.make_async_remote_copy(
                part.at[which, mine], part.at[which, mine], send_sem.at[which, i], recv_sem.at[which, mine],
                device_id=peer, device_id_type=MESH).start()

    def gather_in(stage, which):
        part, peers, _, send_sem, recv_sem, slots = stage
        for i, slot in enumerate(slots):
            copy = pltpu.make_async_remote_copy(
                part.at[which, slot], part.at[which, slot], send_sem.at[which, i], recv_sem.at[which, slot],
                device_id=peers[i], device_id_type=MESH)
            copy.wait_recv()
            copy.wait_send()
        total, error = part[which, 0], jnp.zeros_like(part[which, 0])
        for i in range(1, part.shape[1]):
            total, e = two_sum(total, part[which, i])
            error = error + e
        return total, error

    def sum_begin(which, row):
        part1[which, gxy] = row
        spread_out(first, which)

    def sum_middle(which):
        high, low = renew(*gather_in(first, which))
        part2[which, iz, pl.ds(0, 1), :] = high
        part2[which, iz, pl.ds(1, 1), :] = low
        spread_out(second, which)

    def sum_end(which):
        total, error = gather_in(second, which)
        return renew(total[0:1], error[0:1] + total[1:2])

    def all_lanes(row, m):
        return jnp.broadcast_to(jnp.sum(jnp.where(row_lane == m, row, 0.0), axis=1, keepdims=True), (8, LANES))

    def one_row(values):
        row = jnp.zeros((1, LANES), F32)
        for m, v in enumerate(values):
            row = jnp.where(row_lane == m, jnp.sum(jnp.sum(v, axis=0, keepdims=True), axis=1, keepdims=True), row)
        return row

    wide_lane = lax.broadcasted_iota(jnp.int32, (nz, LANES), 1)
    inside = wide_lane < LANES - 1
    edge = (wide_lane == 0) | (wide_lane == LANES - 1)
    one = jnp.ones((8, LANES), F32)

    loads[0].wait()
    pl.semaphore_wait(barrier, len(group) + len(line))
    send_field(cond, 0)
    loads[1].wait()

    def means(x, acc):
        return acc[0] + cond[x + 1, inner, :], acc[1] + absorb[x]

    sums = lax.fori_loop(0, nx, means, (zero_slab, zero_slab), unroll=4)
    sum_begin(0, one_row([tile_sum(v) for v in sums]))

    def clear(k, _):
        field[k, 0, inner, :] = zero_slab
        field[k, nx + 1, inner, :] = zero_slab
        field[k, pl.ds(1, nx), base - 1, :] = zero_face
        field[k, pl.ds(1, nx), base + nz, :] = zero_face
        return 0

    lax.fori_loop(0, STEPS, clear, 0)
    table[0, 0] = one
    table[0, 1] = jnp.zeros((8, LANES), F32)
    loads[2].wait()
    receive(0)
    sum_middle(0)

    cond[jnp.where(low_x, nx + 1, 0), inner, :] = xrecv[0]
    cond[jnp.where(low_x, 0, nx + 1), inner, :] = zero_slab
    cond[pl.ds(1, nx), base - 1, :] = zrecv[0, 0]
    cond[pl.ds(1, nx), base + nz, :] = zrecv[0, 1]
    for_c = beside(0)
    for x in range(nx):
        for h in range(2):
            turned[x, pl.ds(half * h, half), :] = pltpu.roll(for_c, (LANES - turn_of(x, h)) % LANES, 1)
    fx[0] = 0.5 * (cond[0, inner, :] + cond[1, inner, :])

    def coefficients(x, _):
        here = cond[x + 1, inner, :]
        xp = 0.5 * (here + cond[x + 2, inner, :])
        xm = fx[x]
        yp = jnp.where(inside, 0.5 * (here + pltpu.roll(here, LANES - 1, 1)), 0.0)
        ye = jnp.where(edge, 0.5 * (here + turned[x]), 0.0)
        zp = 0.5 * (here + cond[x + 1, above, :])
        zm = 0.5 * (here + cond[x + 1, below, :])
        total = absorb[x] + xp + xm + yp + pltpu.roll(yp, 1, 1) + ye + zp + zm
        inverse = 1.0 / total
        fx[x + 1] = xp
        fy[x] = yp
        turned[x] = ye * inverse
        fz[x, below, :] = zm
        fz[x, inner, :] = zp
        diag[x] = total
        weight[x] = inverse
        field[0, x + 1, inner, :] = r_out[x] * inverse
        return 0

    lax.fori_loop(0, nx, coefficients, 0, unroll=2)
    wx[...] = weight[border - 1] * fx[jnp.where(low_x, nx, 0)]
    wz[0] = weight[pl.ds(0, nx), 0, :] * fz[pl.ds(0, nx), base - 1, :]
    wz[1] = weight[pl.ds(0, nx), nz - 1, :] * fz[pl.ds(0, nx), base + nz - 1, :]

    send_field(field.at[0], 1)
    packed = pack(turned, 0, 0)
    wy[0] = jnp.where(even, pltpu.roll(packed, LANES - 1, 1), 0.0)
    wy[1] = jnp.where(even, 0.0, pltpu.roll(packed, 1, 1))
    dy[...] = pack(diag, 0, 0)
    zadd[0] = zero_face
    zadd[1] = zero_face
    xadd[...] = zero_slab
    yadd[...] = jnp.zeros((half, LANES), F32)

    face_row = lax.broadcasted_iota(jnp.int32, (nx, LANES), 0)
    face_lane = lax.broadcasted_iota(jnp.int32, (nx, LANES), 1)
    half_row = lax.broadcasted_iota(jnp.int32, (half, LANES), 0)
    slab_row = lax.broadcasted_iota(jnp.int32, (nz, LANES), 0)

    def correct(k):
        field[k, pl.ds(1, nx), base, :] += zadd[0]
        field[k, pl.ds(1, nx), base + nz - 1, :] += zadd[1]
        field[k, border, inner, :] += xadd[...]
        terms = yadd[...]
        for x in range(nx):
            for h in range(2):
                turned[x, pl.ds(half * h, half), :] = pltpu.roll(terms, (LANES - turn_of(x, h) - 1) % LANES, 1)

        def add_sides(x, _):
            field[k, x + 1, inner, :] += jnp.where(edge, turned[x], 0.0)
            return 0

        lax.fori_loop(0, nx, add_sides, 0, unroll=4)

    def step(k, _):
        src, dst, old = k, k + 1, jnp.maximum(k - 1, 0)
        e = k + 1

        @pl.when(k == 1)
        def _():
            high, _ = sum_end(0)
            six = 6.0 * all_lanes(high, 0)
            rho = 0.97 * six / (six + all_lanes(high, 1))
            kappa = jnp.floor(64.0 * (2.0 / rho)) * (1.0 / 64.0)
            half_kappa = 0.5 * kappa
            table[1, 0] = kappa * half_kappa
            table[1, 1] = one
            table[2, 0] = kappa
            table[2, 1] = half_kappa
            for j in range(3, STEPS):
                table[j, 0] = kappa
                table[j, 1] = one

        correct(k)
        a = table[k, 0]
        a_all, b_all = spread(a), spread(table[k, 1])

        def row(x, acc):
            same, older, ahead = acc
            v = field[src, x + 1, inner, :]
            y = fy[x]
            o = field[old, x + 1, inner, :]
            s = fx[x + 1] * field[src, x + 2, inner, :] + fx[x] * field[src, x, inner, :]
            s = s + fz[x, inner, :] * field[src, x + 1, above, :] + fz[x, below, :] * field[src, x + 1, below, :]
            s = s + y * pltpu.roll(v, LANES - 1, 1) + pltpu.roll(y * v, 1, 1)
            new = a_all * (weight[x] * s) - b_all * o
            field[dst, x + 1, inner, :] = new
            w = diag[x] * v
            return same + w * v, older + w * o, ahead + w * new

        same, older, ahead = lax.fori_loop(0, nx, row, (zero_slab, zero_slab, zero_slab), unroll=4)
        dots[2 * k] = tile_sum(same)
        dots[2 * k + 1] = tile_sum(older)
        dots[2 * STEPS] = tile_sum(ahead)

        @pl.when(k == STEPS - 1)
        def _():
            sum_begin(1, one_row([dots[m if m % 2 == 0 else m + 2] for m in range(2 * STEPS - 1)]))


        ypart = pack(field.at[dst])
        zpart = [field[dst, pl.ds(1, nx), base + row_, :] for row_ in (0, nz - 1)]
        xpart = field[dst, border, inner, :]

        receive(e)
        a_half = spread(a, half)
        low_side = a_half * wy[0] * yrecv[e, 0]
        high_side = a_half * wy[1] * yrecv[e, 1]
        za = [a_half * wz[i] * zrecv[e, i] for i in range(2)]
        xa = a_all * wx[...] * xrecv[e]

        @pl.when(k < STEPS - 1)
        def _():
            for h in range(2):
                at = (half - 1) * h
                zface = zpart[h] + za[h]
                for at_lane, side, shift in ((0, low_side, 0), (LANES - 1, high_side, 1)):
                    one_lane = jnp.where(face_lane == 2 * face_row + 2 * nx * h + shift, side[at:at + 1], 0.0)
                    zface = zface + jnp.where(face_lane == at_lane, jnp.sum(one_lane, axis=1, keepdims=True), 0.0)
                at = (nz - 1) * h
                zsend[e + 1, h] = zface + jnp.where(face_row == border - 1, xa[at:at + 1], 0.0)
            send_z(e + 1)

        ya = jnp.where(even, pltpu.roll(high_side, LANES - 1, 1), pltpu.roll(low_side, 1, 1))
        yadd[...] = ya
        zadd[0] = za[0]
        zadd[1] = za[1]
        xadd[...] = xa

        @pl.when(k < STEPS - 1)
        def _():
            yface, xface = ypart + ya, xpart + xa
            xlanes = []
            for h in range(2):
                here = 2 * nx * h + 1
                at = half_row == (half - 1) * h
                moved = jnp.where(face_lane // 2 == face_row + nx * h, pltpu.roll(za[h], here, 1, stride=2, stride_axis=0), 0.0)
                yface = yface + jnp.where(at, jnp.sum(moved, axis=0, keepdims=True), 0.0)
                xa_half = xa[half * h:half * (h + 1)]
                turns = [(2 * (nx - 1) + here) % LANES, here]
                moved = jnp.where(low_x, pltpu.roll(xa_half, turns[0], 1), pltpu.roll(xa_half, turns[1], 1))
                yface = yface + jnp.where(pair == border - 1 + nx * h, moved, 0.0)
                moved = jnp.where(low_x, pltpu.roll(ya, (LANES - turns[0]) % LANES, 1), pltpu.roll(ya, LANES - turns[1], 1))
                xlanes.append(moved)
                z_at = slab_row == (nz - 1) * h
                xface = xface + jnp.where(z_at, jnp.sum(jnp.where(face_row == border - 1, za[h], 0.0), axis=0, keepdims=True), 0.0)
            xsend[e + 1] = xface + jnp.where(edge, jnp.concatenate(xlanes, axis=0), 0.0)
            ysend[e + 1] = yface
            send_xy(e + 1)

        return 0

    lax.fori_loop(0, STEPS, step, 0)
    last = dots[2 * STEPS] + tile_sum(xadd[...] * diag[border - 1] * xsend[STEPS])
    faces = yadd[...] * dy[...] * ysend[STEPS]
    for i in range(2):
        faces = faces + zadd[i] * diag[pl.ds(0, nx), (nz - 1) * i, :] * zsend[STEPS, i]
    sum_begin(2, one_row([last + jnp.sum(faces.reshape(half // 8, 8, LANES), axis=0)]))
    correct(STEPS)
    sum_middle(1)
    sum_middle(2)
    high, low = sum_end(1)
    kappa = table[2, 0]
    half_kappa = table[2, 1]
    raw = [(all_lanes(high, m), all_lanes(low, m)) for m in range(2 * STEPS - 1)]
    exact = (half_kappa, jnp.zeros((8, LANES), F32))
    raw[1] = dmul(raw[1], exact)
    raw[2] = dmul(dmul(raw[2], exact), exact)
    raw[3] = dmul(raw[3], exact)
    mu = raw[:2]
    for m in range(2, 2 * STEPS - 1):
        mu.append(dadd(dtimes(raw[m], 2.0), dneg(mu[m % 2])))
    alpha, beta, end, pivot, ratio = jacobi_matrix(mu)
    u, v, xu, xv, at_u, at_v = solution_polynomials(alpha, beta, kappa, one)
    for p in (u, v, xu, xv):
        p[1] = p[1] * half_kappa
    end = dadd(end, dtimes(mu[1], -(2.0 ** (2 - 2 * STEPS))))
    high, low = sum_end(2)
    end = dadd(end, dtimes((all_lanes(high, 0), all_lanes(low, 0)), 2.0 ** (3 - 2 * STEPS)))
    end = dadd(ddiv(end, pivot), dneg(ratio))[0]
    scale = one / (at_u - end * at_v)
    xs = [scale * (p - end * q) for p, q in zip(xu, xv)]
    rs = [scale * (p - end * q) for p, q in zip(u, v)]
    for k, v in enumerate(xs):
        coef[k] = v
    for k, v in enumerate(rs):
        coef[16 + k] = v

    def finish(x, _):
        v = field[0, x + 1, inner, :]
        sx = spread(coef[0]) * v
        sr = spread(coef[16]) * v
        for k in range(1, STEPS + 1):
            v = field[k, x + 1, inner, :]
            if k < STEPS:
                sx = sx + spread(coef[k]) * v
            sr = sr + spread(coef[16 + k]) * v
        x_out[x] = sx
        r_out[x] = diag[x] * sr
        return 0

    lax.fori_loop(0, nx, finish, 0)


def solution(mesh):
    gx, gy, gz = mesh.shape["gx"], mesh.shape["gy"], mesh.shape["gz"]

    def on_device(right_side, conductivity, absorption):
        nx, ny, nz = right_side.shape
        assert ny == LANES and nx * 2 * 2 == LANES and gx == 2
        args = [jnp.transpose(v, (0, 2, 1)) for v in (right_side, conductivity, absorption)]
        block = (nx, nz, LANES)
        exchanges = STEPS + 1
        dma = pltpu.SemaphoreType.DMA
        tall = nz + 16
        out = pl.pallas_call(
            functools.partial(kernel, nx, nz, (gx, gy, gz)),
            out_shape=[jax.ShapeDtypeStruct(block, F32)] * 2,
            in_specs=[pl.BlockSpec(memory_space=pl.ANY)] * 3,
            out_specs=[pl.BlockSpec(memory_space=pltpu.VMEM)] * 2,
            scratch_shapes=[
                pltpu.VMEM((nx + 2, tall, LANES), F32),
                pltpu.VMEM(block, F32),
                pltpu.VMEM(block, F32),
                pltpu.VMEM(block, F32),
                pltpu.VMEM((nx + 1, nz, LANES), F32),
                pltpu.VMEM(block, F32),
                pltpu.VMEM((nx, tall, LANES), F32),
                pltpu.VMEM(block, F32),
                pltpu.VMEM((nz, LANES), F32),
                pltpu.VMEM((2, nz // 2, LANES), F32),
                pltpu.VMEM((nz // 2, LANES), F32),
                pltpu.VMEM((2, nx, LANES), F32),
                pltpu.VMEM((nz, LANES), F32),
                pltpu.VMEM((nz // 2, LANES), F32),
                pltpu.VMEM((2, nx, LANES), F32),
                pltpu.VMEM((STEPS + 1, nx + 2, tall, LANES), F32),
                pltpu.VMEM((exchanges, nz, LANES), F32),
                pltpu.VMEM((exchanges, 2, nx, LANES), F32),
                pltpu.VMEM((exchanges, 2, nx, LANES), F32),
                pltpu.VMEM((exchanges, nz // 2, LANES), F32),
                pltpu.VMEM((exchanges, 2, nz // 2, LANES), F32),
                pltpu.VMEM((exchanges, nz, LANES), F32),
                pltpu.VMEM((3, gx * gy, 1, LANES), F32),
                pltpu.VMEM((3, gz, 2, LANES), F32),
                pltpu.VMEM((2 * STEPS + 2, 8, LANES), F32),
                pltpu.VMEM((STEPS, 2, 8, LANES), F32),
                pltpu.VMEM((32, 8, LANES), F32),
                dma((3,)),
                dma((exchanges, 5)),
                dma((exchanges, 5)),
                dma((3, gx * gy)),
                dma((3, gx * gy)),
                dma((3, gz)),
                dma((3, gz)),
            ],
            compiler_params=pltpu.CompilerParams(
                collective_id=0, has_side_effects=True, vmem_limit_bytes=48 * 1024 * 1024
            ),
        )(*[pltpu.with_memory_space_constraint(v, pltpu.HBM) for v in args])
        return tuple(jnp.transpose(v, (0, 2, 1)) for v in out)

    spec = P("gx", "gy", "gz")
    return jax.shard_map(on_device, mesh=mesh, in_specs=(spec,) * 3, out_specs=(spec,) * 2, check_vma=False)
```

```python
import functools

import jax
import jax.numpy as jnp
from jax import lax
from jax.experimental import pallas as pl
from jax.experimental.pallas import tpu as pltpu
from jax.sharding import PartitionSpec as P

F32 = jnp.float32
MESH = pl.DeviceIdType.MESH
STEPS = 10
LANES = 128
BASE = 8


def two_sum(a, b):
    s = a + b
    t = s - a
    return s, (a - (s - t)) + (b - t)


def renew(a, b):
    s = a + b
    return s, b - (s - a)


def halves(a):
    t = 4097.0 * a
    high = t - (t - a)
    return high, a - high


def two_product(a, b):
    p = a * b
    ah, al = halves(a)
    bh, bl = halves(b)
    return p, ((ah * bh - p) + ah * bl + al * bh) + al * bl


def dadd(a, b):
    s, e = two_sum(a[0], b[0])
    return renew(s, e + (a[1] + b[1]))


def dneg(a):
    return -a[0], -a[1]


def dmul(a, b):
    p, e = two_product(a[0], b[0])
    return renew(p, e + (a[0] * b[1] + a[1] * b[0]))


def dtimes(a, power):
    return power * a[0], power * a[1]


def ddiv(a, b):
    q = a[0] / b[0]
    p, e = two_product(q, b[0])
    rest = ((a[0] - p) - e) + (a[1] - q * b[1])
    return renew(q, rest / b[0])


def jacobi_matrix(mu):
    n = (len(mu) + 1) // 2
    zero = (0.0 * mu[0][0], 0.0 * mu[0][0])
    cur = [mu[0]] + [dtimes(mu[k], 2.0 ** (1 - k)) for k in range(1, 2 * n - 1)] + [zero]
    prev = None
    ratio = ddiv(cur[1], cur[0])
    alpha, beta = [ratio], [None]
    for k in range(1, n):
        new = [None] * (2 * n)
        minus_alpha = dneg(alpha[-1])
        minus_beta = None if k == 1 else dneg(beta[-1])
        for l in range(k, 2 * n - k):
            v = dadd(cur[l + 1], dmul(minus_alpha, cur[l]))
            if prev is not None:
                v = dadd(v, dmul(minus_beta, prev[l]))
            new[l] = dadd(v, dtimes(cur[l - 1], 0.5 if l == 1 else 0.25))
        beta.append(ddiv(new[k], cur[k - 1]))
        prev, cur = cur, new
        if k < n - 1:
            later = ddiv(new[k + 1], new[k])
            alpha.append(dadd(later, dneg(ratio)))
            ratio = later
    high = [a[0] for a in alpha], [None if b is None else b[0] for b in beta]
    return high[0], high[1], cur[n], cur[n - 1], ratio


def without_pole(p, kappa):
    n = len(p) - 1
    q = [None] * (n + 2)
    q[n] = q[n + 1] = 0.0 * kappa
    for k in range(n, 1, -1):
        q[k - 1] = (q[k] + p[k]) * kappa - q[k + 1]
    q[0] = (q[1] + p[1]) * (0.5 * kappa) - 0.5 * q[2]
    return q[:n]


def solution_polynomials(alpha, beta, kappa, one):
    n = len(beta)
    tau = 0.5 * kappa
    at = [one, tau - alpha[0]]
    for k in range(1, n - 1):
        at.append((tau - alpha[k]) * at[-1] - beta[k] * at[-2])
    before, p = None, [one]
    for k in range(n):
        new = [None] * (k + 2)

        def put(i, v):
            new[i] = v if new[i] is None else new[i] + v

        for i, v in enumerate(p):
            half = 0.5 * v
            put(i + 1, half)
            put(abs(i - 1), half)
        if k < n - 1:
            for i, v in enumerate(p):
                put(i, -(alpha[k] * v))
        if before is not None:
            for i, v in enumerate(before):
                put(i, -(beta[k] * v))
        before, p = p, new
    v = before + [0.0 * one]
    at_u = tau * at[-1] - beta[n - 1] * at[-2]
    return p, v, without_pole(p, kappa), without_pole(v, kappa), at_u, at[-1]


def kernel(nx, nz, sizes, r_hbm, c_hbm, a_hbm, field, diag, coef,
           cond, absorb, weight, fx, fy, fz, turned, wx, wy, dy, wz, xadd, yadd, zadd, xsend, zsend, zrecv, ysend, yrecv, xrecv,
           part1, part2, dots, table,
           load_sem, face_send, face_recv, sum1_send, sum1_recv, sum2_send, sum2_recv):
    gx, gy, gz = sizes
    ix, iy, iz = lax.axis_index("gx"), lax.axis_index("gy"), lax.axis_index("gz")
    ox = 1 - ix
    base = BASE
    inner = pl.ds(base, nz)
    above = pl.ds(base + 1, nz)
    below = pl.ds(base - 1, nz)
    half = nz // 2
    tiles = nz // 8
    low_x = ix == 0
    border = jnp.where(low_x, nx, 1)

    loads = [
        pltpu.make_async_copy(c_hbm, cond.at[pl.ds(1, nx), inner, :], load_sem.at[0]),
        pltpu.make_async_copy(a_hbm, absorb, load_sem.at[1]),
        pltpu.make_async_copy(r_hbm, weight, load_sem.at[2]),
    ]
    for load in loads:
        load.start()

    zero_face = jnp.zeros((nx, LANES), F32)
    zero_slab = jnp.zeros((nz, LANES), F32)

    def clear_faces(k, _):
        for side in range(2):
            zrecv[k, side] = zero_face
            yrecv[k, side] = zero_face
        return 0

    lax.fori_loop(0, STEPS + 1, clear_faces, 0)

    barrier = pltpu.get_barrier_semaphore()
    group = [((ix + dx) % gx, (iy + dy) % gy) for dx in range(gx) for dy in range(gy) if (dx, dy) != (0, 0)]
    line = [(iz + d) % gz for d in range(1, gz)]
    for px, py in group:
        pl.semaphore_signal(barrier, inc=1, device_id=(px, py, iz), device_id_type=MESH)
    for pz in line:
        pl.semaphore_signal(barrier, inc=1, device_id=(ix, iy, pz), device_id_type=MESH)

    lane = lax.broadcasted_iota(jnp.int32, (half, LANES), 1)
    pair = lane // 2
    even = (lane % 2) == 0
    row_lane = lax.broadcasted_iota(jnp.int32, (1, LANES), 1)

    def tile_sum(v):
        return jnp.sum(v.reshape(tiles, 8, LANES), axis=0)

    def spread(c, rows=nz):
        return jnp.broadcast_to(c[None], (rows // 8, 8, LANES)).reshape(rows, LANES)

    def turn_of(x, h):
        return 2 * x + 2 * nx * h

    def pack(source, skip=1, start=base):
        out = jnp.zeros((half, LANES), F32)
        for x in range(nx):
            for h in range(2):
                v = source[x + skip, pl.ds(start + half * h, half), :]
                out = jnp.where(pair == x + nx * h, pltpu.roll(v, (turn_of(x, h) + 1) % LANES, 1), out)
        return out

    def copies(e):
        xc = pltpu.make_async_remote_copy(
            xsend.at[e], xrecv.at[e],
            face_send.at[e, 0], face_recv.at[e, 0], device_id=(ox, iy, iz), device_id_type=MESH)
        yc, zc = [], []
        for up in range(2):
            yc.append(pltpu.make_async_remote_copy(
                ysend.at[e], yrecv.at[e, 1 - up], face_send.at[e, 1 + up], face_recv.at[e, 2 - up],
                device_id=(ix, jnp.clip(iy + 2 * up - 1, 0, gy - 1), iz), device_id_type=MESH))
            zc.append(pltpu.make_async_remote_copy(
                zsend.at[e, up], zrecv.at[e, 1 - up], face_send.at[e, 3 + up], face_recv.at[e, 4 - up],
                device_id=(ix, iy, jnp.clip(iz + 2 * up - 1, 0, gz - 1)), device_id_type=MESH))
        return xc, yc, zc

    def send_z(e):
        _, _, zc = copies(e)
        pl.when(iz > 0)(zc[0].start)
        pl.when(iz < gz - 1)(zc[1].start)

    def send_xy(e):
        xc, yc, _ = copies(e)
        pl.when(iy > 0)(yc[0].start)
        pl.when(iy < gy - 1)(yc[1].start)
        xc.start()

    def fill_z(source, e):
        zsend[e, 0] = source[pl.ds(1, nx), base, :]
        zsend[e, 1] = source[pl.ds(1, nx), base + nz - 1, :]

    def fill_xy(source, e):
        ysend[e] = pack(source)
        xsend[e] = source[border, inner, :]

    def receive(e):
        xc, yc, zc = copies(e)
        xc.wait()
        pl.when(iy > 0)(lambda: (yc[0].wait_send(), yc[1].wait_recv())[0])
        pl.when(iy < gy - 1)(lambda: (yc[1].wait_send(), yc[0].wait_recv())[0])
        pl.when(iz > 0)(lambda: (zc[0].wait_send(), zc[1].wait_recv())[0])
        pl.when(iz < gz - 1)(lambda: (zc[1].wait_send(), zc[0].wait_recv())[0])

    def beside(e):
        return jnp.where(even, yrecv[e, 0], pltpu.roll(yrecv[e, 1], LANES - 2, 1))

    gxy = ix * gy + iy
    first = (part1, [(px, py, iz) for px, py in group], gxy, sum1_send, sum1_recv, [px * gy + py for px, py in group])
    second = (part2, [(ix, iy, pz) for pz in line], iz, sum2_send, sum2_recv, line)

    def spread_out(stage, which):
        part, peers, mine, send_sem, recv_sem, _ = stage
        for i, peer in enumerate(peers):
            pltpu.make_async_remote_copy(
                part.at[which, mine], part.at[which, mine], send_sem.at[which, i], recv_sem.at[which, mine],
                device_id=peer, device_id_type=MESH).start()

    def arrivals(stage, which):
        part, peers, _, send_sem, recv_sem, slots = stage
        return [
            pltpu.make_async_remote_copy(
                part.at[which, slot], part.at[which, slot], send_sem.at[which, i], recv_sem.at[which, slot],
                device_id=peers[i], device_id_type=MESH)
            for i, slot in enumerate(slots)
        ]

    def gather_in(stage, which):
        part = stage[0]
        for copy in arrivals(stage, which):
            copy.wait_recv()
        total, error = part[which, 0], jnp.zeros_like(part[which, 0])
        for i in range(1, part.shape[1]):
            total, e = two_sum(total, part[which, i])
            error = error + e
        return total, error

    def sum_begin(which, row):
        part1[which, gxy] = row
        spread_out(first, which)

    def sum_middle(which):
        high, low = renew(*gather_in(first, which))
        part2[which, iz, pl.ds(0, 1), :] = high
        part2[which, iz, pl.ds(1, 1), :] = low
        spread_out(second, which)

    def sum_end(which):
        total, error = gather_in(second, which)
        return renew(total[0:1], error[0:1] + total[1:2])

    def all_lanes(row, m):
        return jnp.broadcast_to(jnp.sum(jnp.where(row_lane == m, row, 0.0), axis=1, keepdims=True), (8, LANES))

    def one_row(values):
        row = jnp.zeros((1, LANES), F32)
        for m, v in enumerate(values):
            row = jnp.where(row_lane == m, jnp.sum(jnp.sum(v, axis=0, keepdims=True), axis=1, keepdims=True), row)
        return row

    wide_lane = lax.broadcasted_iota(jnp.int32, (nz, LANES), 1)
    inside = wide_lane < LANES - 1
    after = wide_lane > 0
    edge = (wide_lane == 0) | (wide_lane == LANES - 1)
    one = jnp.ones((8, LANES), F32)

    loads[0].wait()
    pl.semaphore_wait(barrier, len(group) + len(line))
    fill_z(cond, 0)
    send_z(0)
    fill_xy(cond, 0)
    send_xy(0)
    loads[1].wait()

    def means(x, acc):
        return acc[0] + cond[x + 1, inner, :], acc[1] + absorb[x]

    sums = lax.fori_loop(0, nx, means, (zero_slab, zero_slab), unroll=4)
    sum_begin(0, one_row([tile_sum(v) for v in sums]))

    def clear(k, _):
        field[k, 0, inner, :] = zero_slab
        field[k, nx + 1, inner, :] = zero_slab
        field[k, pl.ds(1, nx), base - 1, :] = zero_face
        field[k, pl.ds(1, nx), base + nz, :] = zero_face
        return 0

    lax.fori_loop(0, STEPS, clear, 0)
    table[0, 0] = one
    table[0, 1] = jnp.zeros((8, LANES), F32)
    loads[2].wait()
    receive(0)
    sum_middle(0)

    cond[jnp.where(low_x, nx + 1, 0), inner, :] = xrecv[0]
    cond[jnp.where(low_x, 0, nx + 1), inner, :] = zero_slab
    cond[pl.ds(1, nx), base - 1, :] = zrecv[0, 0]
    cond[pl.ds(1, nx), base + nz, :] = zrecv[0, 1]
    for_c = beside(0)
    for x in range(nx):
        for h in range(2):
            turned[x, pl.ds(half * h, half), :] = pltpu.roll(for_c, (LANES - turn_of(x, h)) % LANES, 1)
    fx[0] = 0.5 * (cond[0, inner, :] + cond[1, inner, :])

    def coefficients(x, _):
        here = cond[x + 1, inner, :]
        xp = 0.5 * (here + cond[x + 2, inner, :])
        xm = fx[x]
        yp = jnp.where(inside, 0.5 * (here + pltpu.roll(here, LANES - 1, 1)), 0.0)
        ym = jnp.where(after, 0.5 * (here + pltpu.roll(here, 1, 1)), 0.0)
        ye = jnp.where(edge, 0.5 * (here + turned[x]), 0.0)
        zp = 0.5 * (here + cond[x + 1, above, :])
        zm = 0.5 * (here + cond[x + 1, below, :])
        total = absorb[x] + xp + xm + yp + ym + ye + zp + zm
        inverse = 1.0 / total
        fx[x + 1] = xp
        fy[x] = yp
        turned[x] = ye * inverse
        fz[x, below, :] = zm
        fz[x, inner, :] = zp
        diag[x] = total
        field[0, x + 1, inner, :] = weight[x] * inverse
        weight[x] = inverse
        return 0

    lax.fori_loop(0, nx, coefficients, 0, unroll=8)
    wx[...] = weight[border - 1] * fx[jnp.where(low_x, nx, 0)]
    wz[0] = weight[pl.ds(0, nx), 0, :] * fz[pl.ds(0, nx), base - 1, :]
    wz[1] = weight[pl.ds(0, nx), nz - 1, :] * fz[pl.ds(0, nx), base + nz - 1, :]

    fill_z(field.at[0], 1)
    send_z(1)
    fill_xy(field.at[0], 1)
    send_xy(1)
    packed = pack(turned, 0, 0)
    wy[0] = jnp.where(even, pltpu.roll(packed, LANES - 1, 1), 0.0)
    wy[1] = jnp.where(even, 0.0, pltpu.roll(packed, 1, 1))
    dy[...] = pack(diag, 0, 0)
    zadd[0] = zero_face
    zadd[1] = zero_face
    xadd[...] = zero_slab
    yadd[...] = jnp.zeros((half, LANES), F32)

    face_row = lax.broadcasted_iota(jnp.int32, (nx, LANES), 0)
    face_lane = lax.broadcasted_iota(jnp.int32, (nx, LANES), 1)
    half_row = lax.broadcasted_iota(jnp.int32, (half, LANES), 0)
    slab_row = lax.broadcasted_iota(jnp.int32, (nz, LANES), 0)

    def correct(k):
        field[k, pl.ds(1, nx), base, :] += zadd[0]
        field[k, pl.ds(1, nx), base + nz - 1, :] += zadd[1]
        field[k, border, inner, :] += xadd[...]
        terms = yadd[...]
        for x in range(nx):
            for h in range(2):
                turned[x, pl.ds(half * h, half), :] = pltpu.roll(terms, (LANES - turn_of(x, h) - 1) % LANES, 1)

        def add_sides(x, _):
            field[k, x + 1, inner, :] += jnp.where(edge, turned[x], 0.0)
            return 0

        lax.fori_loop(0, nx, add_sides, 0, unroll=4)

    def step(k, _):
        src, dst, old = k, k + 1, jnp.maximum(k - 1, 0)
        e = k + 1

        @pl.when(k == 1)
        def _():
            high, _ = sum_end(0)
            six = 6.0 * all_lanes(high, 0)
            rho = 0.97 * six / (six + all_lanes(high, 1))
            kappa = jnp.floor(64.0 * (2.0 / rho)) * (1.0 / 64.0)
            half_kappa = 0.5 * kappa
            table[1, 0] = kappa * half_kappa
            table[1, 1] = one
            table[2, 0] = kappa
            table[2, 1] = half_kappa
            for j in range(3, STEPS):
                table[j, 0] = kappa
                table[j, 1] = one

        correct(k)
        a = table[k, 0]
        a_all, b_all = spread(a), spread(table[k, 1])

        def row(x, acc):
            same, older, ahead = acc
            v = field[src, x + 1, inner, :]
            y = fy[x]
            o = field[old, x + 1, inner, :]
            s = fx[x + 1] * field[src, x + 2, inner, :] + fx[x] * field[src, x, inner, :]
            s = s + fz[x, inner, :] * field[src, x + 1, above, :] + fz[x, below, :] * field[src, x + 1, below, :]
            s = s + y * pltpu.roll(v, LANES - 1, 1) + pltpu.roll(y * v, 1, 1)
            new = a_all * (weight[x] * s) - b_all * o
            field[dst, x + 1, inner, :] = new
            w = diag[x] * v
            return same + w * v, older + w * o, ahead + w * new

        same, older, ahead = lax.fori_loop(0, nx, row, (zero_slab, zero_slab, zero_slab), unroll=4)
        dots[2 * k] = tile_sum(same)
        dots[2 * k + 1] = tile_sum(older)
        dots[2 * STEPS] = tile_sum(ahead)

        @pl.when(k == STEPS - 1)
        def _():
            sum_begin(1, one_row([dots[m if m % 2 == 0 else m + 2] for m in range(2 * STEPS - 1)]))


        ypart = pack(field.at[dst])
        zpart = [field[dst, pl.ds(1, nx), base + row_, :] for row_ in (0, nz - 1)]
        xpart = field[dst, border, inner, :]

        receive(e)
        a_half = spread(a, half)
        low_side = a_half * wy[0] * yrecv[e, 0]
        high_side = a_half * wy[1] * yrecv[e, 1]
        za = [a_half * wz[i] * zrecv[e, i] for i in range(2)]
        xa = a_all * wx[...] * xrecv[e]

        @pl.when(k < STEPS - 1)
        def _():
            for h in range(2):
                at = (half - 1) * h
                zface = zpart[h] + za[h]
                for at_lane, side, shift in ((0, low_side, 0), (LANES - 1, high_side, 1)):
                    one_lane = jnp.where(face_lane == 2 * face_row + 2 * nx * h + shift, side[at:at + 1], 0.0)
                    zface = zface + jnp.where(face_lane == at_lane, jnp.sum(one_lane, axis=1, keepdims=True), 0.0)
                at = (nz - 1) * h
                zsend[e + 1, h] = zface + jnp.where(face_row == border - 1, xa[at:at + 1], 0.0)
            send_z(e + 1)

        ya = jnp.where(even, pltpu.roll(high_side, LANES - 1, 1), pltpu.roll(low_side, 1, 1))
        yadd[...] = ya
        zadd[0] = za[0]
        zadd[1] = za[1]
        xadd[...] = xa

        @pl.when(k < STEPS - 1)
        def _():
            yface, xface = ypart + ya, xpart + xa
            xlanes = []
            for h in range(2):
                here = 2 * nx * h + 1
                at = half_row == (half - 1) * h
                moved = jnp.where(face_lane // 2 == face_row + nx * h, pltpu.roll(za[h], here, 1, stride=2, stride_axis=0), 0.0)
                yface = yface + jnp.where(at, jnp.sum(moved, axis=0, keepdims=True), 0.0)
                xa_half = xa[half * h:half * (h + 1)]
                turns = [(2 * (nx - 1) + here) % LANES, here]
                moved = jnp.where(low_x, pltpu.roll(xa_half, turns[0], 1), pltpu.roll(xa_half, turns[1], 1))
                yface = yface + jnp.where(pair == border - 1 + nx * h, moved, 0.0)
                moved = jnp.where(low_x, pltpu.roll(ya, (LANES - turns[0]) % LANES, 1), pltpu.roll(ya, LANES - turns[1], 1))
                xlanes.append(moved)
                z_at = slab_row == (nz - 1) * h
                xface = xface + jnp.where(z_at, jnp.sum(jnp.where(face_row == border - 1, za[h], 0.0), axis=0, keepdims=True), 0.0)
            xsend[e + 1] = xface + jnp.where(edge, jnp.concatenate(xlanes, axis=0), 0.0)
            ysend[e + 1] = yface
            send_xy(e + 1)

        return 0

    lax.fori_loop(0, STEPS, step, 0)
    last = dots[2 * STEPS] + tile_sum(xadd[...] * diag[border - 1] * xsend[STEPS])
    faces = yadd[...] * dy[...] * ysend[STEPS]
    for i in range(2):
        faces = faces + zadd[i] * diag[pl.ds(0, nx), (nz - 1) * i, :] * zsend[STEPS, i]
    sum_begin(2, one_row([last + jnp.sum(faces.reshape(half // 8, 8, LANES), axis=0)]))
    correct(STEPS)
    sum_middle(1)
    sum_middle(2)
    high, low = sum_end(1)
    kappa = table[2, 0]
    half_kappa = table[2, 1]
    raw = [(all_lanes(high, m), all_lanes(low, m)) for m in range(2 * STEPS - 1)]
    exact = (half_kappa, jnp.zeros((8, LANES), F32))
    raw[1] = dmul(raw[1], exact)
    raw[2] = dmul(dmul(raw[2], exact), exact)
    raw[3] = dmul(raw[3], exact)
    mu = raw[:2]
    for m in range(2, 2 * STEPS - 1):
        mu.append(dadd(dtimes(raw[m], 2.0), dneg(mu[m % 2])))
    alpha, beta, end, pivot, ratio = jacobi_matrix(mu)
    u, v, xu, xv, at_u, at_v = solution_polynomials(alpha, beta, kappa, one)
    for p in (u, v, xu, xv):
        p[1] = p[1] * half_kappa
    end = dadd(end, dtimes(mu[1], -(2.0 ** (2 - 2 * STEPS))))
    high, low = sum_end(2)
    end = dadd(end, dtimes((all_lanes(high, 0), all_lanes(low, 0)), 2.0 ** (3 - 2 * STEPS)))
    end = dadd(ddiv(end, pivot), dneg(ratio))[0]
    scale = one / (at_u - end * at_v)
    xs = [scale * (p - end * q) for p, q in zip(xu, xv)]
    rs = [scale * (p - end * q) for p, q in zip(u, v)]
    for k, v in enumerate(xs):
        coef[k] = v
    for k, v in enumerate(rs):
        coef[16 + k] = v
    for which in range(3):
        for stage in (first, second):
            for copy in arrivals(stage, which):
                copy.wait_send()


def finish(nx, nz, groups, field, diag, coef, x_hbm, r_hbm, xs, rs, sems):
    inner = pl.ds(BASE, nz)
    size = nx // groups

    def spread(c):
        return jnp.broadcast_to(c[None], (nz // 8, 8, LANES)).reshape(nz, LANES)

    def slab(x, _):
        v = field[0, x + 1, inner, :]
        sx = spread(coef[0]) * v
        sr = spread(coef[16]) * v
        for k in range(1, STEPS + 1):
            v = field[k, x + 1, inner, :]
            if k < STEPS:
                sx = sx + spread(coef[k]) * v
            sr = sr + spread(coef[16 + k]) * v
        xs[x] = sx
        rs[x] = diag[x] * sr
        return 0

    copies = []
    for g in range(groups):
        lax.fori_loop(g * size, (g + 1) * size, slab, 0, unroll=2)
        part = pl.ds(g * size, size)
        for n, (src, dst) in enumerate(((xs, x_hbm), (rs, r_hbm))):
            copy = pltpu.make_async_copy(src.at[part], dst.at[part], sems.at[n, g])
            copy.start()
            copies.append(copy)
    for copy in copies:
        copy.wait()


def solution(mesh):
    gx, gy, gz = mesh.shape["gx"], mesh.shape["gy"], mesh.shape["gz"]

    def on_device(right_side, conductivity, absorption):
        nx, ny, nz = right_side.shape
        assert ny == LANES and nx * 2 * 2 == LANES and gx == 2
        args = [jnp.transpose(v, (0, 2, 1)) for v in (right_side, conductivity, absorption)]
        block = (nx, nz, LANES)
        exchanges = STEPS + 1
        dma = pltpu.SemaphoreType.DMA
        tall = nz + 16
        field = (STEPS + 1, nx + 2, tall, LANES)
        vmem = pl.BlockSpec(memory_space=pltpu.VMEM)
        kept = pl.pallas_call(
            functools.partial(kernel, nx, nz, (gx, gy, gz)),
            out_shape=[pltpu.VMEM(field, F32), pltpu.VMEM(block, F32), pltpu.VMEM((32, 8, LANES), F32)],
            in_specs=[pl.BlockSpec(memory_space=pl.ANY)] * 3,
            out_specs=[vmem] * 3,
            scratch_shapes=[
                pltpu.VMEM((nx + 2, tall, LANES), F32),
                pltpu.VMEM(block, F32),
                pltpu.VMEM(block, F32),
                pltpu.VMEM((nx + 1, nz, LANES), F32),
                pltpu.VMEM(block, F32),
                pltpu.VMEM((nx, tall, LANES), F32),
                pltpu.VMEM(block, F32),
                pltpu.VMEM((nz, LANES), F32),
                pltpu.VMEM((2, nz // 2, LANES), F32),
                pltpu.VMEM((nz // 2, LANES), F32),
                pltpu.VMEM((2, nx, LANES), F32),
                pltpu.VMEM((nz, LANES), F32),
                pltpu.VMEM((nz // 2, LANES), F32),
                pltpu.VMEM((2, nx, LANES), F32),
                pltpu.VMEM((exchanges, nz, LANES), F32),
                pltpu.VMEM((exchanges, 2, nx, LANES), F32),
                pltpu.VMEM((exchanges, 2, nx, LANES), F32),
                pltpu.VMEM((exchanges, nz // 2, LANES), F32),
                pltpu.VMEM((exchanges, 2, nz // 2, LANES), F32),
                pltpu.VMEM((exchanges, nz, LANES), F32),
                pltpu.VMEM((3, gx * gy, 1, LANES), F32),
                pltpu.VMEM((3, gz, 2, LANES), F32),
                pltpu.VMEM((2 * STEPS + 2, 8, LANES), F32),
                pltpu.VMEM((STEPS, 2, 8, LANES), F32),
                dma((3,)),
                dma((exchanges, 5)),
                dma((exchanges, 5)),
                dma((3, gx * gy)),
                dma((3, gx * gy)),
                dma((3, gz)),
                dma((3, gz)),
            ],
            compiler_params=pltpu.CompilerParams(
                collective_id=0, has_side_effects=True, vmem_limit_bytes=40 * 1024 * 1024
            ),
        )(*[pltpu.with_memory_space_constraint(v, pltpu.HBM) for v in args])
        groups = 4
        out = pl.pallas_call(
            functools.partial(finish, nx, nz, groups),
            out_shape=[jax.ShapeDtypeStruct(block, F32)] * 2,
            in_specs=[vmem] * 3,
            out_specs=[pl.BlockSpec(memory_space=pltpu.HBM)] * 2,
            scratch_shapes=[pltpu.VMEM(block, F32), pltpu.VMEM(block, F32), dma((2, groups))],
            compiler_params=pltpu.CompilerParams(vmem_limit_bytes=20 * 1024 * 1024),
        )(*kept)
        return tuple(jnp.transpose(v, (0, 2, 1)) for v in out)

    spec = P("gx", "gy", "gz")
    return jax.shard_map(on_device, mesh=mesh, in_specs=(spec,) * 3, out_specs=(spec,) * 2, check_vma=False)
```

```python
import functools

import jax
import jax.numpy as jnp
from jax import lax
from jax.experimental import pallas as pl
from jax.experimental.pallas import tpu as pltpu
from jax.sharding import PartitionSpec as P

F32 = jnp.float32
MESH = pl.DeviceIdType.MESH
STEPS = 10
LANES = 128
BASE = 8


def two_sum(a, b):
    s = a + b
    t = s - a
    return s, (a - (s - t)) + (b - t)


def renew(a, b):
    s = a + b
    return s, b - (s - a)


def halves(a):
    t = 4097.0 * a
    high = t - (t - a)
    return high, a - high


def two_product(a, b):
    p = a * b
    ah, al = halves(a)
    bh, bl = halves(b)
    return p, ((ah * bh - p) + ah * bl + al * bh) + al * bl


def dadd(a, b):
    s, e = two_sum(a[0], b[0])
    return renew(s, e + (a[1] + b[1]))


def dneg(a):
    return -a[0], -a[1]


def dmul(a, b):
    p, e = two_product(a[0], b[0])
    return renew(p, e + (a[0] * b[1] + a[1] * b[0]))


def dtimes(a, power):
    return power * a[0], power * a[1]


def ddiv(a, b):
    q = a[0] / b[0]
    p, e = two_product(q, b[0])
    rest = ((a[0] - p) - e) + (a[1] - q * b[1])
    return renew(q, rest / b[0])


def jacobi_matrix(mu):
    n = (len(mu) + 1) // 2
    zero = (0.0 * mu[0][0], 0.0 * mu[0][0])
    cur = [mu[0]] + [dtimes(mu[k], 2.0 ** (1 - k)) for k in range(1, 2 * n - 1)] + [zero]
    prev = None
    ratio = ddiv(cur[1], cur[0])
    alpha, beta = [ratio], [None]
    for k in range(1, n):
        new = [None] * (2 * n)
        minus_alpha = dneg(alpha[-1])
        minus_beta = None if k == 1 else dneg(beta[-1])
        for l in range(k, 2 * n - k):
            v = dadd(cur[l + 1], dmul(minus_alpha, cur[l]))
            if prev is not None:
                v = dadd(v, dmul(minus_beta, prev[l]))
            new[l] = dadd(v, dtimes(cur[l - 1], 0.5 if l == 1 else 0.25))
        beta.append(ddiv(new[k], cur[k - 1]))
        prev, cur = cur, new
        if k < n - 1:
            later = ddiv(new[k + 1], new[k])
            alpha.append(dadd(later, dneg(ratio)))
            ratio = later
    high = [a[0] for a in alpha], [None if b is None else b[0] for b in beta]
    return high[0], high[1], cur[n], cur[n - 1], ratio


def without_pole(p, kappa):
    n = len(p) - 1
    q = [None] * (n + 2)
    q[n] = q[n + 1] = 0.0 * kappa
    for k in range(n, 1, -1):
        q[k - 1] = (q[k] + p[k]) * kappa - q[k + 1]
    q[0] = (q[1] + p[1]) * (0.5 * kappa) - 0.5 * q[2]
    return q[:n]


def solution_polynomials(alpha, beta, kappa, one):
    n = len(beta)
    tau = 0.5 * kappa
    at = [one, tau - alpha[0]]
    for k in range(1, n - 1):
        at.append((tau - alpha[k]) * at[-1] - beta[k] * at[-2])
    before, p = None, [one]
    for k in range(n):
        new = [None] * (k + 2)

        def put(i, v):
            new[i] = v if new[i] is None else new[i] + v

        for i, v in enumerate(p):
            half = 0.5 * v
            put(i + 1, half)
            put(abs(i - 1), half)
        if k < n - 1:
            for i, v in enumerate(p):
                put(i, -(alpha[k] * v))
        if before is not None:
            for i, v in enumerate(before):
                put(i, -(beta[k] * v))
        before, p = p, new
    v = before + [0.0 * one]
    at_u = tau * at[-1] - beta[n - 1] * at[-2]
    return p, v, without_pole(p, kappa), without_pole(v, kappa), at_u, at[-1]


def kernel(nx, nz, sizes, r_hbm, c_hbm, a_hbm, field, diag, coef,
           cond, absorb, weight, fx, fy, fz, turned, wx, wy, dy, wz, xadd, yadd, zadd, xsend, zsend, zrecv, ysend, yrecv, xrecv,
           part1, part2, dots, table,
           load_sem, face_send, face_recv, sum1_send, sum1_recv, sum2_send, sum2_recv):
    gx, gy, gz = sizes
    ix, iy, iz = lax.axis_index("gx"), lax.axis_index("gy"), lax.axis_index("gz")
    ox = 1 - ix
    base = BASE
    inner = pl.ds(base, nz)
    above = pl.ds(base + 1, nz)
    below = pl.ds(base - 1, nz)
    half = nz // 2
    tiles = nz // 8
    low_x = ix == 0
    border = jnp.where(low_x, nx, 1)

    loads = [
        pltpu.make_async_copy(c_hbm, cond.at[pl.ds(1, nx), inner, :], load_sem.at[0]),
        pltpu.make_async_copy(a_hbm, absorb, load_sem.at[1]),
        pltpu.make_async_copy(r_hbm, weight, load_sem.at[2]),
    ]
    for load in loads:
        load.start()

    zero_face = jnp.zeros((nx, LANES), F32)
    zero_slab = jnp.zeros((nz, LANES), F32)

    def clear_faces(k, _):
        for side in range(2):
            zrecv[k, side] = zero_face
            yrecv[k, side] = zero_face
        return 0

    lax.fori_loop(0, STEPS + 1, clear_faces, 0)

    barrier = pltpu.get_barrier_semaphore()
    group = [((ix + dx) % gx, (iy + dy) % gy) for dx in range(gx) for dy in range(gy) if (dx, dy) != (0, 0)]
    line = [(iz + d) % gz for d in range(1, gz)]
    for px, py in group:
        pl.semaphore_signal(barrier, inc=1, device_id=(px, py, iz), device_id_type=MESH)
    for pz in line:
        pl.semaphore_signal(barrier, inc=1, device_id=(ix, iy, pz), device_id_type=MESH)

    lane = lax.broadcasted_iota(jnp.int32, (half, LANES), 1)
    pair = lane // 2
    even = (lane % 2) == 0
    row_lane = lax.broadcasted_iota(jnp.int32, (1, LANES), 1)

    def tile_sum(v):
        return jnp.sum(v.reshape(tiles, 8, LANES), axis=0)

    def spread(c, rows=nz):
        return jnp.broadcast_to(c[None], (rows // 8, 8, LANES)).reshape(rows, LANES)

    def turn_of(x, h):
        return 2 * x + 2 * nx * h

    def pack(source, skip=1, start=base):
        out = jnp.zeros((half, LANES), F32)
        for x in range(nx):
            for h in range(2):
                v = source[x + skip, pl.ds(start + half * h, half), :]
                out = jnp.where(pair == x + nx * h, pltpu.roll(v, (turn_of(x, h) + 1) % LANES, 1), out)
        return out

    def copies(e):
        xc = pltpu.make_async_remote_copy(
            xsend.at[e], xrecv.at[e],
            face_send.at[e, 0], face_recv.at[e, 0], device_id=(ox, iy, iz), device_id_type=MESH)
        yc, zc = [], []
        for up in range(2):
            yc.append(pltpu.make_async_remote_copy(
                ysend.at[e], yrecv.at[e, 1 - up], face_send.at[e, 1 + up], face_recv.at[e, 2 - up],
                device_id=(ix, jnp.clip(iy + 2 * up - 1, 0, gy - 1), iz), device_id_type=MESH))
            zc.append(pltpu.make_async_remote_copy(
                zsend.at[e, up], zrecv.at[e, 1 - up], face_send.at[e, 3 + up], face_recv.at[e, 4 - up],
                device_id=(ix, iy, jnp.clip(iz + 2 * up - 1, 0, gz - 1)), device_id_type=MESH))
        return xc, yc, zc

    def send_z(e):
        _, _, zc = copies(e)
        pl.when(iz > 0)(zc[0].start)
        pl.when(iz < gz - 1)(zc[1].start)

    def send_xy(e):
        xc, yc, _ = copies(e)
        pl.when(iy > 0)(yc[0].start)
        pl.when(iy < gy - 1)(yc[1].start)
        xc.start()

    def fill_z(source, e):
        zsend[e, 0] = source[pl.ds(1, nx), base, :]
        zsend[e, 1] = source[pl.ds(1, nx), base + nz - 1, :]

    def fill_xy(source, e):
        ysend[e] = pack(source)
        xsend[e] = source[border, inner, :]

    def receive(e):
        xc, yc, zc = copies(e)
        xc.wait()
        pl.when(iy > 0)(lambda: (yc[0].wait_send(), yc[1].wait_recv())[0])
        pl.when(iy < gy - 1)(lambda: (yc[1].wait_send(), yc[0].wait_recv())[0])
        pl.when(iz > 0)(lambda: (zc[0].wait_send(), zc[1].wait_recv())[0])
        pl.when(iz < gz - 1)(lambda: (zc[1].wait_send(), zc[0].wait_recv())[0])

    gxy = ix * gy + iy
    first = (part1, [(px, py, iz) for px, py in group], gxy, sum1_send, sum1_recv, [px * gy + py for px, py in group])
    second = (part2, [(ix, iy, pz) for pz in line], iz, sum2_send, sum2_recv, line)

    def spread_out(stage, which):
        part, peers, mine, send_sem, recv_sem, _ = stage
        for i, peer in enumerate(peers):
            pltpu.make_async_remote_copy(
                part.at[which, mine], part.at[which, mine], send_sem.at[which, i], recv_sem.at[which, mine],
                device_id=peer, device_id_type=MESH).start()

    def arrivals(stage, which):
        part, peers, _, send_sem, recv_sem, slots = stage
        return [
            pltpu.make_async_remote_copy(
                part.at[which, slot], part.at[which, slot], send_sem.at[which, i], recv_sem.at[which, slot],
                device_id=peers[i], device_id_type=MESH)
            for i, slot in enumerate(slots)
        ]

    def gather_in(stage, which):
        part = stage[0]
        for copy in arrivals(stage, which):
            copy.wait_recv()
        total, error = part[which, 0], jnp.zeros_like(part[which, 0])
        for i in range(1, part.shape[1]):
            total, e = two_sum(total, part[which, i])
            error = error + e
        return total, error

    def sum_begin(which, row):
        part1[which, gxy] = row
        spread_out(first, which)

    def sum_middle(which):
        high, low = renew(*gather_in(first, which))
        part2[which, iz, pl.ds(0, 1), :] = high
        part2[which, iz, pl.ds(1, 1), :] = low
        spread_out(second, which)

    def sum_end(which):
        total, error = gather_in(second, which)
        return renew(total[0:1], error[0:1] + total[1:2])

    def all_lanes(row, m):
        return jnp.broadcast_to(jnp.sum(jnp.where(row_lane == m, row, 0.0), axis=1, keepdims=True), (8, LANES))

    def one_row(values):
        row = jnp.zeros((1, LANES), F32)
        for m, v in enumerate(values):
            row = jnp.where(row_lane == m, jnp.sum(jnp.sum(v, axis=0, keepdims=True), axis=1, keepdims=True), row)
        return row

    wide_lane = lax.broadcasted_iota(jnp.int32, (nz, LANES), 1)
    inside = wide_lane < LANES - 1
    after = wide_lane > 0
    edge = (wide_lane == 0) | (wide_lane == LANES - 1)
    one = jnp.ones((8, LANES), F32)

    face_row = lax.broadcasted_iota(jnp.int32, (nx, LANES), 0)
    face_lane = lax.broadcasted_iota(jnp.int32, (nx, LANES), 1)
    half_row = lax.broadcasted_iota(jnp.int32, (half, LANES), 0)
    slab_row = lax.broadcasted_iota(jnp.int32, (nz, LANES), 0)

    def z_faces(zpart, za, low_side, high_side, xa):
        faces = []
        for h in range(2):
            at = (half - 1) * h
            face = zpart[h] + za[h]
            for at_lane, side, shift in ((0, low_side, 0), (LANES - 1, high_side, 1)):
                one_lane = jnp.where(face_lane == 2 * face_row + 2 * nx * h + shift, side[at:at + 1], 0.0)
                face = face + jnp.where(face_lane == at_lane, jnp.sum(one_lane, axis=1, keepdims=True), 0.0)
            at = (nz - 1) * h
            faces.append(face + jnp.where(face_row == border - 1, xa[at:at + 1], 0.0))
        return faces

    def joined(low_side, high_side):
        return jnp.where(even, pltpu.roll(high_side, LANES - 1, 1), pltpu.roll(low_side, 1, 1))

    def xy_faces(xpart, ypart, za, ya, xa):
        yface, xface = ypart + ya, xpart + xa
        xlanes = []
        for h in range(2):
            here = 2 * nx * h + 1
            at = half_row == (half - 1) * h
            moved = jnp.where(face_lane // 2 == face_row + nx * h, pltpu.roll(za[h], here, 1, stride=2, stride_axis=0), 0.0)
            yface = yface + jnp.where(at, jnp.sum(moved, axis=0, keepdims=True), 0.0)
            xa_half = xa[half * h:half * (h + 1)]
            turns = [(2 * (nx - 1) + here) % LANES, here]
            moved = jnp.where(low_x, pltpu.roll(xa_half, turns[0], 1), pltpu.roll(xa_half, turns[1], 1))
            yface = yface + jnp.where(pair == border - 1 + nx * h, moved, 0.0)
            moved = jnp.where(low_x, pltpu.roll(ya, (LANES - turns[0]) % LANES, 1), pltpu.roll(ya, LANES - turns[1], 1))
            xlanes.append(moved)
            z_at = slab_row == (nz - 1) * h
            xface = xface + jnp.where(z_at, jnp.sum(jnp.where(face_row == border - 1, za[h], 0.0), axis=0, keepdims=True), 0.0)
        return xface + jnp.where(edge, jnp.concatenate(xlanes, axis=0), 0.0), yface

    def keep(za, ya, xa):
        yadd[...] = ya
        zadd[0] = za[0]
        zadd[1] = za[1]
        xadd[...] = xa

    def correct(ref, skip=1, start=base):
        ref[pl.ds(skip, nx), start, :] += zadd[0]
        ref[pl.ds(skip, nx), start + nz - 1, :] += zadd[1]
        ref[border - 1 + skip, pl.ds(start, nz), :] += xadd[...]
        terms = yadd[...]
        for x in range(nx):
            for h in range(2):
                turned[x, pl.ds(half * h, half), :] = pltpu.roll(terms, (LANES - turn_of(x, h) - 1) % LANES, 1)

        def add_sides(x, _):
            ref[x + skip, pl.ds(start, nz), :] += jnp.where(edge, turned[x], 0.0)
            return 0

        lax.fori_loop(0, nx, add_sides, 0, unroll=4)

    loads[0].wait()
    pl.semaphore_wait(barrier, len(group) + len(line))
    fill_z(cond, 0)
    send_z(0)
    fill_xy(cond, 0)
    send_xy(0)
    loads[1].wait()

    def means(x, acc):
        return acc[0] + cond[x + 1, inner, :], acc[1] + absorb[x]

    sums = lax.fori_loop(0, nx, means, (zero_slab, zero_slab), unroll=4)
    sum_begin(0, one_row([tile_sum(v) for v in sums]))

    def clear(k, _):
        field[k, 0, inner, :] = zero_slab
        field[k, nx + 1, inner, :] = zero_slab
        field[k, pl.ds(1, nx), base - 1, :] = zero_face
        field[k, pl.ds(1, nx), base + nz, :] = zero_face
        return 0

    lax.fori_loop(0, STEPS, clear, 0)
    table[0, 0] = one
    table[0, 1] = jnp.zeros((8, LANES), F32)
    cond[0, inner, :] = zero_slab
    cond[nx + 1, inner, :] = zero_slab
    cond[pl.ds(1, nx), base - 1, :] = zero_face
    cond[pl.ds(1, nx), base + nz, :] = zero_face
    fx[0] = 0.5 * cond[1, inner, :]

    def coefficients(x, _):
        here = cond[x + 1, inner, :]
        xp = 0.5 * (here + cond[x + 2, inner, :])
        xm = fx[x]
        yp = 0.5 * (here + jnp.where(inside, pltpu.roll(here, LANES - 1, 1), 0.0))
        ym = 0.5 * (here + jnp.where(after, pltpu.roll(here, 1, 1), 0.0))
        zp = 0.5 * (here + cond[x + 1, above, :])
        zm = 0.5 * (here + cond[x + 1, below, :])
        fx[x + 1] = xp
        fy[x] = jnp.where(inside, yp, 0.0)
        fz[x, below, :] = zm
        fz[x, inner, :] = zp
        diag[x] = absorb[x] + xp + xm + yp + ym + zp + zm
        return 0

    lax.fori_loop(0, nx, coefficients, 0, unroll=8)
    loads[2].wait()
    ypart, yright = pack(diag, 0, 0), pack(weight, 0, 0)
    receive(0)
    low_side, high_side = 0.5 * yrecv[0, 0], 0.5 * yrecv[0, 1]
    za = [0.5 * zrecv[0, i] for i in range(2)]
    xa = 0.5 * xrecv[0]
    zdiag = z_faces([diag[pl.ds(0, nx), (nz - 1) * i, :] for i in range(2)], za, low_side, high_side, xa)
    for i in range(2):
        zsend[1, i] = weight[pl.ds(0, nx), (nz - 1) * i, :] / zdiag[i]
    send_z(1)
    ya = joined(low_side, high_side)
    xdiag, ydiag = xy_faces(diag[border - 1], ypart, za, ya, xa)
    xsend[1] = weight[border - 1] / xdiag
    ysend[1] = yright / ydiag
    send_xy(1)
    sum_middle(0)
    for i in range(2):
        wz[i] = (0.5 * zsend[0, i] + za[i]) / zdiag[i]
    wx[...] = (0.5 * xsend[0] + xa) / xdiag
    sides = (0.5 * ysend[0] + ya) / ydiag
    wy[0] = jnp.where(even, pltpu.roll(sides, LANES - 1, 1), 0.0)
    wy[1] = jnp.where(even, 0.0, pltpu.roll(sides, 1, 1))
    dy[...] = ydiag
    keep(za, ya, xa)
    correct(diag, 0, 0)

    def begin(x, _):
        inverse = 1.0 / diag[x]
        field[0, x + 1, inner, :] = weight[x] * inverse
        weight[x] = inverse
        return 0

    lax.fori_loop(0, nx, begin, 0, unroll=4)
    keep([zero_face, zero_face], jnp.zeros((half, LANES), F32), zero_slab)

    def step(k, _):
        src, dst, old = k, k + 1, jnp.maximum(k - 1, 0)
        e = k + 1

        @pl.when(k == 1)
        def _():
            high, _ = sum_end(0)
            six = 6.0 * all_lanes(high, 0)
            rho = 0.97 * six / (six + all_lanes(high, 1))
            kappa = jnp.floor(64.0 * (2.0 / rho)) * (1.0 / 64.0)
            half_kappa = 0.5 * kappa
            table[1, 0] = kappa * half_kappa
            table[1, 1] = one
            table[2, 0] = kappa
            table[2, 1] = half_kappa
            for j in range(3, STEPS):
                table[j, 0] = kappa
                table[j, 1] = one

        correct(field.at[k])
        a = table[k, 0]
        a_all, b_all = spread(a), spread(table[k, 1])

        def row(x, acc):
            same, older, ahead = acc
            v = field[src, x + 1, inner, :]
            y = fy[x]
            o = field[old, x + 1, inner, :]
            s = fx[x + 1] * field[src, x + 2, inner, :] + fx[x] * field[src, x, inner, :]
            s = s + fz[x, inner, :] * field[src, x + 1, above, :] + fz[x, below, :] * field[src, x + 1, below, :]
            s = s + y * pltpu.roll(v, LANES - 1, 1) + pltpu.roll(y * v, 1, 1)
            new = a_all * (weight[x] * s) - b_all * o
            field[dst, x + 1, inner, :] = new
            w = diag[x] * v
            return same + w * v, older + w * o, ahead + w * new

        same, older, ahead = lax.fori_loop(0, nx, row, (zero_slab, zero_slab, zero_slab), unroll=4)
        dots[2 * k] = tile_sum(same)
        dots[2 * k + 1] = tile_sum(older)
        dots[2 * STEPS] = tile_sum(ahead)

        @pl.when(k == STEPS - 1)
        def _():
            sum_begin(1, one_row([dots[m if m % 2 == 0 else m + 2] for m in range(2 * STEPS - 1)]))


        ypart = pack(field.at[dst])
        zpart = [field[dst, pl.ds(1, nx), base + row_, :] for row_ in (0, nz - 1)]
        xpart = field[dst, border, inner, :]

        receive(e)
        a_half = spread(a, half)
        low_side = a_half * wy[0] * yrecv[e, 0]
        high_side = a_half * wy[1] * yrecv[e, 1]
        za = [a_half * wz[i] * zrecv[e, i] for i in range(2)]
        xa = a_all * wx[...] * xrecv[e]

        @pl.when(k < STEPS - 1)
        def _():
            for i, face in enumerate(z_faces(zpart, za, low_side, high_side, xa)):
                zsend[e + 1, i] = face
            send_z(e + 1)

        ya = joined(low_side, high_side)
        keep(za, ya, xa)

        @pl.when(k < STEPS - 1)
        def _():
            xsend[e + 1], ysend[e + 1] = xy_faces(xpart, ypart, za, ya, xa)
            send_xy(e + 1)

        return 0

    lax.fori_loop(0, STEPS, step, 0)
    last = dots[2 * STEPS] + tile_sum(xadd[...] * diag[border - 1] * xsend[STEPS])
    faces = yadd[...] * dy[...] * ysend[STEPS]
    for i in range(2):
        faces = faces + zadd[i] * diag[pl.ds(0, nx), (nz - 1) * i, :] * zsend[STEPS, i]
    sum_begin(2, one_row([last + jnp.sum(faces.reshape(half // 8, 8, LANES), axis=0)]))
    correct(field.at[STEPS])
    sum_middle(1)
    sum_middle(2)
    high, low = sum_end(1)
    kappa = table[2, 0]
    half_kappa = table[2, 1]
    raw = [(all_lanes(high, m), all_lanes(low, m)) for m in range(2 * STEPS - 1)]
    exact = (half_kappa, jnp.zeros((8, LANES), F32))
    raw[1] = dmul(raw[1], exact)
    raw[2] = dmul(dmul(raw[2], exact), exact)
    raw[3] = dmul(raw[3], exact)
    mu = raw[:2]
    for m in range(2, 2 * STEPS - 1):
        mu.append(dadd(dtimes(raw[m], 2.0), dneg(mu[m % 2])))
    alpha, beta, end, pivot, ratio = jacobi_matrix(mu)
    u, v, xu, xv, at_u, at_v = solution_polynomials(alpha, beta, kappa, one)
    for p in (u, v, xu, xv):
        p[1] = p[1] * half_kappa
    end = dadd(end, dtimes(mu[1], -(2.0 ** (2 - 2 * STEPS))))
    high, low = sum_end(2)
    end = dadd(end, dtimes((all_lanes(high, 0), all_lanes(low, 0)), 2.0 ** (3 - 2 * STEPS)))
    end = dadd(ddiv(end, pivot), dneg(ratio))[0]
    scale = one / (at_u - end * at_v)
    xs = [scale * (p - end * q) for p, q in zip(xu, xv)]
    rs = [scale * (p - end * q) for p, q in zip(u, v)]
    for k, v in enumerate(xs):
        coef[k] = v
    for k, v in enumerate(rs):
        coef[16 + k] = v
    for which in range(3):
        for stage in (first, second):
            for copy in arrivals(stage, which):
                copy.wait_send()


def finish(nx, nz, groups, field, diag, coef, x_hbm, r_hbm, xs, rs, sems):
    inner = pl.ds(BASE, nz)
    size = nx // groups

    def spread(c):
        return jnp.broadcast_to(c[None], (nz // 8, 8, LANES)).reshape(nz, LANES)

    def slab(x, _):
        v = field[0, x + 1, inner, :]
        sx = spread(coef[0]) * v
        sr = spread(coef[16]) * v
        for k in range(1, STEPS + 1):
            v = field[k, x + 1, inner, :]
            if k < STEPS:
                sx = sx + spread(coef[k]) * v
            sr = sr + spread(coef[16 + k]) * v
        xs[x] = sx
        rs[x] = diag[x] * sr
        return 0

    copies = []
    for g in range(groups):
        lax.fori_loop(g * size, (g + 1) * size, slab, 0, unroll=2)
        part = pl.ds(g * size, size)
        for n, (src, dst) in enumerate(((xs, x_hbm), (rs, r_hbm))):
            copy = pltpu.make_async_copy(src.at[part], dst.at[part], sems.at[n, g])
            copy.start()
            copies.append(copy)
    for copy in copies:
        copy.wait()


def solution(mesh):
    gx, gy, gz = mesh.shape["gx"], mesh.shape["gy"], mesh.shape["gz"]

    def on_device(right_side, conductivity, absorption):
        nx, ny, nz = right_side.shape
        assert ny == LANES and nx * 2 * 2 == LANES and gx == 2
        args = [jnp.transpose(v, (0, 2, 1)) for v in (right_side, conductivity, absorption)]
        block = (nx, nz, LANES)
        exchanges = STEPS + 1
        dma = pltpu.SemaphoreType.DMA
        tall = nz + 16
        field = (STEPS + 1, nx + 2, tall, LANES)
        vmem = pl.BlockSpec(memory_space=pltpu.VMEM)
        kept = pl.pallas_call(
            functools.partial(kernel, nx, nz, (gx, gy, gz)),
            out_shape=[pltpu.VMEM(field, F32), pltpu.VMEM(block, F32), pltpu.VMEM((32, 8, LANES), F32)],
            in_specs=[pl.BlockSpec(memory_space=pl.ANY)] * 3,
            out_specs=[vmem] * 3,
            scratch_shapes=[
                pltpu.VMEM((nx + 2, tall, LANES), F32),
                pltpu.VMEM(block, F32),
                pltpu.VMEM(block, F32),
                pltpu.VMEM((nx + 1, nz, LANES), F32),
                pltpu.VMEM(block, F32),
                pltpu.VMEM((nx, tall, LANES), F32),
                pltpu.VMEM(block, F32),
                pltpu.VMEM((nz, LANES), F32),
                pltpu.VMEM((2, nz // 2, LANES), F32),
                pltpu.VMEM((nz // 2, LANES), F32),
                pltpu.VMEM((2, nx, LANES), F32),
                pltpu.VMEM((nz, LANES), F32),
                pltpu.VMEM((nz // 2, LANES), F32),
                pltpu.VMEM((2, nx, LANES), F32),
                pltpu.VMEM((exchanges, nz, LANES), F32),
                pltpu.VMEM((exchanges, 2, nx, LANES), F32),
                pltpu.VMEM((exchanges, 2, nx, LANES), F32),
                pltpu.VMEM((exchanges, nz // 2, LANES), F32),
                pltpu.VMEM((exchanges, 2, nz // 2, LANES), F32),
                pltpu.VMEM((exchanges, nz, LANES), F32),
                pltpu.VMEM((3, gx * gy, 1, LANES), F32),
                pltpu.VMEM((3, gz, 2, LANES), F32),
                pltpu.VMEM((2 * STEPS + 2, 8, LANES), F32),
                pltpu.VMEM((STEPS, 2, 8, LANES), F32),
                dma((3,)),
                dma((exchanges, 5)),
                dma((exchanges, 5)),
                dma((3, gx * gy)),
                dma((3, gx * gy)),
                dma((3, gz)),
                dma((3, gz)),
            ],
            compiler_params=pltpu.CompilerParams(
                collective_id=0, has_side_effects=True, vmem_limit_bytes=40 * 1024 * 1024
            ),
        )(*[pltpu.with_memory_space_constraint(v, pltpu.HBM) for v in args])
        groups = 4
        out = pl.pallas_call(
            functools.partial(finish, nx, nz, groups),
            out_shape=[jax.ShapeDtypeStruct(block, F32)] * 2,
            in_specs=[vmem] * 3,
            out_specs=[pl.BlockSpec(memory_space=pltpu.HBM)] * 2,
            scratch_shapes=[pltpu.VMEM(block, F32), pltpu.VMEM(block, F32), dma((2, groups))],
            compiler_params=pltpu.CompilerParams(vmem_limit_bytes=20 * 1024 * 1024),
        )(*kept)
        return tuple(jnp.transpose(v, (0, 2, 1)) for v in out)

    spec = P("gx", "gy", "gz")
    return jax.shard_map(on_device, mesh=mesh, in_specs=(spec,) * 3, out_specs=(spec,) * 2, check_vma=False)
```

```python
import functools

import jax
import jax.numpy as jnp
from jax import lax
from jax.experimental import pallas as pl
from jax.experimental.pallas import tpu as pltpu
from jax.sharding import PartitionSpec as P

F32 = jnp.float32
MESH = pl.DeviceIdType.MESH
STEPS = 10
LANES = 128
BASE = 8


def two_sum(a, b):
    s = a + b
    t = s - a
    return s, (a - (s - t)) + (b - t)


def renew(a, b):
    s = a + b
    return s, b - (s - a)


def halves(a):
    t = 4097.0 * a
    high = t - (t - a)
    return high, a - high


def two_product(a, b):
    p = a * b
    ah, al = halves(a)
    bh, bl = halves(b)
    return p, ((ah * bh - p) + ah * bl + al * bh) + al * bl


def dadd(a, b):
    s, e = two_sum(a[0], b[0])
    return renew(s, e + (a[1] + b[1]))


def dneg(a):
    return -a[0], -a[1]


def dmul(a, b):
    p, e = two_product(a[0], b[0])
    return renew(p, e + (a[0] * b[1] + a[1] * b[0]))


def dtimes(a, power):
    return power * a[0], power * a[1]


def ddiv(a, b):
    q = a[0] / b[0]
    p, e = two_product(q, b[0])
    rest = ((a[0] - p) - e) + (a[1] - q * b[1])
    return renew(q, rest / b[0])


def jacobi_matrix(mu):
    n = (len(mu) + 1) // 2
    zero = (0.0 * mu[0][0], 0.0 * mu[0][0])
    cur = [mu[0]] + [dtimes(mu[k], 2.0 ** (1 - k)) for k in range(1, 2 * n - 1)] + [zero]
    prev = None
    ratio = ddiv(cur[1], cur[0])
    alpha, beta = [ratio], [None]
    for k in range(1, n):
        new = [None] * (2 * n)
        minus_alpha = dneg(alpha[-1])
        minus_beta = None if k == 1 else dneg(beta[-1])
        for l in range(k, 2 * n - k):
            v = dadd(cur[l + 1], dmul(minus_alpha, cur[l]))
            if prev is not None:
                v = dadd(v, dmul(minus_beta, prev[l]))
            new[l] = dadd(v, dtimes(cur[l - 1], 0.5 if l == 1 else 0.25))
        beta.append(ddiv(new[k], cur[k - 1]))
        prev, cur = cur, new
        if k < n - 1:
            later = ddiv(new[k + 1], new[k])
            alpha.append(dadd(later, dneg(ratio)))
            ratio = later
    high = [a[0] for a in alpha], [None if b is None else b[0] for b in beta]
    return high[0], high[1], cur[n], cur[n - 1], ratio


def without_pole(p, kappa):
    n = len(p) - 1
    q = [None] * (n + 2)
    q[n] = q[n + 1] = 0.0 * kappa
    for k in range(n, 1, -1):
        q[k - 1] = (q[k] + p[k]) * kappa - q[k + 1]
    q[0] = (q[1] + p[1]) * (0.5 * kappa) - 0.5 * q[2]
    return q[:n]


def solution_polynomials(alpha, beta, kappa, one):
    n = len(beta)
    tau = 0.5 * kappa
    at = [one, tau - alpha[0]]
    for k in range(1, n - 1):
        at.append((tau - alpha[k]) * at[-1] - beta[k] * at[-2])
    before, p = None, [one]
    for k in range(n):
        new = [None] * (k + 2)

        def put(i, v):
            new[i] = v if new[i] is None else new[i] + v

        for i, v in enumerate(p):
            half = 0.5 * v
            put(i + 1, half)
            put(abs(i - 1), half)
        if k < n - 1:
            for i, v in enumerate(p):
                put(i, -(alpha[k] * v))
        if before is not None:
            for i, v in enumerate(before):
                put(i, -(beta[k] * v))
        before, p = p, new
    v = before + [0.0 * one]
    at_u = tau * at[-1] - beta[n - 1] * at[-2]
    return p, v, without_pole(p, kappa), without_pole(v, kappa), at_u, at[-1]


def kernel(nx, nz, sizes, r_hbm, c_hbm, a_hbm, field, diag, coef,
           cond, absorb, weight, fx, fy, fz, turned, wx, wy, dy, wz, xadd, yadd, zadd, xsend, zsend, zrecv, ysend, yrecv, xrecv,
           part1, part2, dots, table,
           load_sem, face_send, face_recv, sum1_send, sum1_recv, sum2_send, sum2_recv):
    gx, gy, gz = sizes
    ix, iy, iz = lax.axis_index("gx"), lax.axis_index("gy"), lax.axis_index("gz")
    ox = 1 - ix
    base = BASE
    inner = pl.ds(base, nz)
    above = pl.ds(base + 1, nz)
    below = pl.ds(base - 1, nz)
    half = nz // 2
    tiles = nz // 8
    low_x = ix == 0
    border = jnp.where(low_x, nx, 1)

    loads = [
        pltpu.make_async_copy(c_hbm, cond.at[pl.ds(1, nx), inner, :], load_sem.at[0]),
        pltpu.make_async_copy(a_hbm, absorb, load_sem.at[1]),
        pltpu.make_async_copy(r_hbm, weight, load_sem.at[2]),
    ]
    loads[0].start()

    zero_face = jnp.zeros((nx, LANES), F32)
    zero_slab = jnp.zeros((nz, LANES), F32)

    barrier = pltpu.get_barrier_semaphore()
    group = [((ix + dx) % gx, (iy + dy) % gy) for dx in range(gx) for dy in range(gy) if (dx, dy) != (0, 0)]
    line = [(iz + d) % gz for d in range(1, gz)]
    for px, py in group:
        pl.semaphore_signal(barrier, inc=1, device_id=(px, py, iz), device_id_type=MESH)
    for pz in line:
        pl.semaphore_signal(barrier, inc=1, device_id=(ix, iy, pz), device_id_type=MESH)

    for ref, side, alone in ((zrecv, 0, iz == 0), (zrecv, 1, iz == gz - 1), (yrecv, 0, iy == 0), (yrecv, 1, iy == gy - 1)):

        @pl.when(alone)
        def _(ref=ref, side=side):
            def clear_faces(k, _):
                ref[k, side] = zero_face
                return 0

            lax.fori_loop(0, STEPS + 1, clear_faces, 0)

    lane = lax.broadcasted_iota(jnp.int32, (half, LANES), 1)
    pair = lane // 2
    even = (lane % 2) == 0
    row_lane = lax.broadcasted_iota(jnp.int32, (1, LANES), 1)

    def tile_sum(v):
        return jnp.sum(v.reshape(tiles, 8, LANES), axis=0)

    def spread(c, rows=nz):
        return jnp.broadcast_to(c[None], (rows // 8, 8, LANES)).reshape(rows, LANES)

    def turn_of(x, h):
        return 2 * x + 2 * nx * h

    def pack(source, skip=1, start=base):
        out = jnp.zeros((half, LANES), F32)
        for x in range(nx):
            for h in range(2):
                v = source[x + skip, pl.ds(start + half * h, half), :]
                out = jnp.where(pair == x + nx * h, pltpu.roll(v, (turn_of(x, h) + 1) % LANES, 1), out)
        return out

    def copies(e):
        xc = pltpu.make_async_remote_copy(
            xsend.at[e], xrecv.at[e],
            face_send.at[e, 0], face_recv.at[e, 0], device_id=(ox, iy, iz), device_id_type=MESH)
        yc, zc = [], []
        for up in range(2):
            yc.append(pltpu.make_async_remote_copy(
                ysend.at[e], yrecv.at[e, 1 - up], face_send.at[e, 1 + up], face_recv.at[e, 2 - up],
                device_id=(ix, jnp.clip(iy + 2 * up - 1, 0, gy - 1), iz), device_id_type=MESH))
            zc.append(pltpu.make_async_remote_copy(
                zsend.at[e, up], zrecv.at[e, 1 - up], face_send.at[e, 3 + up], face_recv.at[e, 4 - up],
                device_id=(ix, iy, jnp.clip(iz + 2 * up - 1, 0, gz - 1)), device_id_type=MESH))
        return xc, yc, zc

    def send_z(e):
        _, _, zc = copies(e)
        pl.when(iz > 0)(zc[0].start)
        pl.when(iz < gz - 1)(zc[1].start)

    def send_xy(e):
        xc, yc, _ = copies(e)
        pl.when(iy > 0)(yc[0].start)
        pl.when(iy < gy - 1)(yc[1].start)
        xc.start()

    def fill_z(source, e):
        zsend[e, 0] = source[pl.ds(1, nx), base, :]
        zsend[e, 1] = source[pl.ds(1, nx), base + nz - 1, :]

    def fill_xy(source, e):
        ysend[e] = pack(source)
        xsend[e] = source[border, inner, :]

    def receive_xy(e):
        xc, yc, _ = copies(e)
        xc.wait()
        pl.when(iy > 0)(lambda: (yc[0].wait_send(), yc[1].wait_recv())[0])
        pl.when(iy < gy - 1)(lambda: (yc[1].wait_send(), yc[0].wait_recv())[0])

    def receive_z(e):
        _, _, zc = copies(e)
        pl.when(iz > 0)(lambda: (zc[0].wait_send(), zc[1].wait_recv())[0])
        pl.when(iz < gz - 1)(lambda: (zc[1].wait_send(), zc[0].wait_recv())[0])

    gxy = ix * gy + iy
    first = (part1, [(px, py, iz) for px, py in group], gxy, sum1_send, sum1_recv, [px * gy + py for px, py in group])
    second = (part2, [(ix, iy, pz) for pz in line], iz, sum2_send, sum2_recv, line)

    def spread_out(stage, which):
        part, peers, mine, send_sem, recv_sem, _ = stage
        for i, peer in enumerate(peers):
            pltpu.make_async_remote_copy(
                part.at[which, mine], part.at[which, mine], send_sem.at[which, i], recv_sem.at[which, mine],
                device_id=peer, device_id_type=MESH).start()

    def arrivals(stage, which):
        part, peers, _, send_sem, recv_sem, slots = stage
        return [
            pltpu.make_async_remote_copy(
                part.at[which, slot], part.at[which, slot], send_sem.at[which, i], recv_sem.at[which, slot],
                device_id=peers[i], device_id_type=MESH)
            for i, slot in enumerate(slots)
        ]

    def gather_in(stage, which):
        part = stage[0]
        for copy in arrivals(stage, which):
            copy.wait_recv()
        total, error = part[which, 0], jnp.zeros_like(part[which, 0])
        for i in range(1, part.shape[1]):
            total, e = two_sum(total, part[which, i])
            error = error + e
        return total, error

    def sum_begin(which, row):
        part1[which, gxy] = row
        spread_out(first, which)

    def sum_middle(which):
        high, low = renew(*gather_in(first, which))
        part2[which, iz, pl.ds(0, 1), :] = high
        part2[which, iz, pl.ds(1, 1), :] = low
        spread_out(second, which)

    def sum_end(which):
        total, error = gather_in(second, which)
        return renew(total[0:1], error[0:1] + total[1:2])

    def all_lanes(row, m):
        return jnp.broadcast_to(jnp.sum(jnp.where(row_lane == m, row, 0.0), axis=1, keepdims=True), (8, LANES))

    def one_row(values):
        row = jnp.zeros((1, LANES), F32)
        for m, v in enumerate(values):
            row = jnp.where(row_lane == m, jnp.sum(jnp.sum(v, axis=0, keepdims=True), axis=1, keepdims=True), row)
        return row

    wide_lane = lax.broadcasted_iota(jnp.int32, (nz, LANES), 1)
    inside = wide_lane < LANES - 1
    after = wide_lane > 0
    edge = (wide_lane == 0) | (wide_lane == LANES - 1)
    one = jnp.ones((8, LANES), F32)

    face_row = lax.broadcasted_iota(jnp.int32, (nx, LANES), 0)
    face_lane = lax.broadcasted_iota(jnp.int32, (nx, LANES), 1)
    half_row = lax.broadcasted_iota(jnp.int32, (half, LANES), 0)
    slab_row = lax.broadcasted_iota(jnp.int32, (nz, LANES), 0)

    def z_edges(zpart, low_side, high_side, xa):
        faces = []
        for h in range(2):
            at = (half - 1) * h
            face = zpart[h]
            for at_lane, side, shift in ((0, low_side, 0), (LANES - 1, high_side, 1)):
                one_lane = jnp.where(face_lane == 2 * face_row + 2 * nx * h + shift, side[at:at + 1], 0.0)
                face = face + jnp.where(face_lane == at_lane, jnp.sum(one_lane, axis=1, keepdims=True), 0.0)
            at = (nz - 1) * h
            faces.append(face + jnp.where(face_row == border - 1, xa[at:at + 1], 0.0))
        return faces

    def joined(low_side, high_side):
        return jnp.where(even, pltpu.roll(high_side, LANES - 1, 1), pltpu.roll(low_side, 1, 1))

    def xy_faces(xpart, ypart, za, ya, xa):
        yface, xface = ypart + ya, xpart + xa
        xlanes = []
        for h in range(2):
            here = 2 * nx * h + 1
            at = half_row == (half - 1) * h
            moved = jnp.where(face_lane // 2 == face_row + nx * h, pltpu.roll(za[h], here, 1, stride=2, stride_axis=0), 0.0)
            yface = yface + jnp.where(at, jnp.sum(moved, axis=0, keepdims=True), 0.0)
            xa_half = xa[half * h:half * (h + 1)]
            turns = [(2 * (nx - 1) + here) % LANES, here]
            moved = jnp.where(low_x, pltpu.roll(xa_half, turns[0], 1), pltpu.roll(xa_half, turns[1], 1))
            yface = yface + jnp.where(pair == border - 1 + nx * h, moved, 0.0)
            moved = jnp.where(low_x, pltpu.roll(ya, (LANES - turns[0]) % LANES, 1), pltpu.roll(ya, LANES - turns[1], 1))
            xlanes.append(moved)
            z_at = slab_row == (nz - 1) * h
            xface = xface + jnp.where(z_at, jnp.sum(jnp.where(face_row == border - 1, za[h], 0.0), axis=0, keepdims=True), 0.0)
        return xface + jnp.where(edge, jnp.concatenate(xlanes, axis=0), 0.0), yface

    def keep(za, ya, xa):
        yadd[...] = ya
        zadd[0] = za[0]
        zadd[1] = za[1]
        xadd[...] = xa

    def correct(ref, skip=1, start=base):
        ref[pl.ds(skip, nx), start, :] += zadd[0]
        ref[pl.ds(skip, nx), start + nz - 1, :] += zadd[1]
        ref[border - 1 + skip, pl.ds(start, nz), :] += xadd[...]
        terms = yadd[...]
        for x in range(nx):
            for h in range(2):
                turned[x, pl.ds(half * h, half), :] = pltpu.roll(terms, (LANES - turn_of(x, h) - 1) % LANES, 1)

        def add_sides(x, _):
            ref[x + skip, pl.ds(start, nz), :] += jnp.where(edge, turned[x], 0.0)
            return 0

        lax.fori_loop(0, nx, add_sides, 0, unroll=4)

    loads[0].wait()
    loads[1].start()
    loads[2].start()
    pl.semaphore_wait(barrier, len(group) + len(line))
    fill_z(cond, 0)
    send_z(0)
    fill_xy(cond, 0)
    send_xy(0)
    loads[1].wait()

    def means(x, acc):
        return acc[0] + cond[x + 1, inner, :], acc[1] + absorb[x]

    sums = lax.fori_loop(0, nx, means, (zero_slab, zero_slab), unroll=4)
    sum_begin(0, one_row([tile_sum(v) for v in sums]))

    def clear(k, _):
        field[k, 0, inner, :] = zero_slab
        field[k, nx + 1, inner, :] = zero_slab
        field[k, pl.ds(1, nx), base - 1, :] = zero_face
        field[k, pl.ds(1, nx), base + nz, :] = zero_face
        return 0

    lax.fori_loop(0, STEPS, clear, 0)
    table[0, 0] = one
    table[0, 1] = jnp.zeros((8, LANES), F32)
    cond[0, inner, :] = zero_slab
    cond[nx + 1, inner, :] = zero_slab
    cond[pl.ds(1, nx), base - 1, :] = zero_face
    cond[pl.ds(1, nx), base + nz, :] = zero_face
    fx[0] = 0.5 * cond[1, inner, :]

    def coefficients(x, _):
        here = cond[x + 1, inner, :]
        xp = 0.5 * (here + cond[x + 2, inner, :])
        xm = fx[x]
        yp = 0.5 * (here + jnp.where(inside, pltpu.roll(here, LANES - 1, 1), 0.0))
        ym = 0.5 * (here + jnp.where(after, pltpu.roll(here, 1, 1), 0.0))
        zp = 0.5 * (here + cond[x + 1, above, :])
        zm = 0.5 * (here + cond[x + 1, below, :])
        fx[x + 1] = xp
        fy[x] = jnp.where(inside, yp, 0.0)
        fz[x, below, :] = zm
        fz[x, inner, :] = zp
        diag[x] = absorb[x] + xp + xm + yp + ym + zp + zm
        return 0

    lax.fori_loop(0, nx, coefficients, 0, unroll=8)
    loads[2].wait()
    ypart, yright = pack(diag, 0, 0), pack(weight, 0, 0)
    zpart = [diag[pl.ds(0, nx), (nz - 1) * i, :] for i in range(2)]
    zright = [weight[pl.ds(0, nx), (nz - 1) * i, :] for i in range(2)]
    receive_xy(0)
    low_side, high_side = 0.5 * yrecv[0, 0], 0.5 * yrecv[0, 1]
    xa = 0.5 * xrecv[0]
    zpart = z_edges(zpart, low_side, high_side, xa)
    receive_z(0)
    za = [0.5 * zrecv[0, i] for i in range(2)]
    zdiag = [zpart[i] + za[i] for i in range(2)]
    for i in range(2):
        zsend[1, i] = zright[i] / zdiag[i]
    send_z(1)
    ya = joined(low_side, high_side)
    xdiag, ydiag = xy_faces(diag[border - 1], ypart, za, ya, xa)
    xsend[1] = weight[border - 1] / xdiag
    ysend[1] = yright / ydiag
    send_xy(1)
    sum_middle(0)
    for i in range(2):
        wz[i] = (0.5 * zsend[0, i] + za[i]) / zdiag[i]
    wx[...] = (0.5 * xsend[0] + xa) / xdiag
    sides = (0.5 * ysend[0] + ya) / ydiag
    wy[0] = jnp.where(even, pltpu.roll(sides, LANES - 1, 1), 0.0)
    wy[1] = jnp.where(even, 0.0, pltpu.roll(sides, 1, 1))
    dy[...] = ydiag
    keep(za, ya, xa)
    correct(diag, 0, 0)

    def begin(x, _):
        inverse = 1.0 / diag[x]
        field[0, x + 1, inner, :] = weight[x] * inverse
        weight[x] = inverse
        return 0

    lax.fori_loop(0, nx, begin, 0, unroll=4)
    keep([zero_face, zero_face], jnp.zeros((half, LANES), F32), zero_slab)

    def step(k, _):
        src, dst, old = k, k + 1, jnp.maximum(k - 1, 0)
        e = k + 1

        @pl.when(k == 1)
        def _():
            high, _ = sum_end(0)
            six = 6.0 * all_lanes(high, 0)
            rho = 0.97 * six / (six + all_lanes(high, 1))
            kappa = jnp.floor(64.0 * (2.0 / rho)) * (1.0 / 64.0)
            half_kappa = 0.5 * kappa
            table[1, 0] = kappa * half_kappa
            table[1, 1] = one
            table[2, 0] = kappa
            table[2, 1] = half_kappa
            for j in range(3, STEPS):
                table[j, 0] = kappa
                table[j, 1] = one

        correct(field.at[k])
        a = table[k, 0]
        a_all, b_all = spread(a), spread(table[k, 1])

        def row(x, acc):
            same, older, ahead = acc
            v = field[src, x + 1, inner, :]
            y = fy[x]
            o = field[old, x + 1, inner, :]
            s = fx[x + 1] * field[src, x + 2, inner, :] + fx[x] * field[src, x, inner, :]
            s = s + fz[x, inner, :] * field[src, x + 1, above, :] + fz[x, below, :] * field[src, x + 1, below, :]
            s = s + y * pltpu.roll(v, LANES - 1, 1) + pltpu.roll(y * v, 1, 1)
            new = a_all * (weight[x] * s) - b_all * o
            field[dst, x + 1, inner, :] = new
            w = diag[x] * v
            return same + w * v, older + w * o, ahead + w * new

        same, older, ahead = lax.fori_loop(0, nx, row, (zero_slab, zero_slab, zero_slab), unroll=4)
        dots[2 * k] = tile_sum(same)
        dots[2 * k + 1] = tile_sum(older)
        dots[2 * STEPS] = tile_sum(ahead)

        @pl.when(k == STEPS - 1)
        def _():
            sum_begin(1, one_row([dots[m if m % 2 == 0 else m + 2] for m in range(2 * STEPS - 1)]))


        ypart = pack(field.at[dst])
        zpart = [field[dst, pl.ds(1, nx), base + row_, :] for row_ in (0, nz - 1)]
        xpart = field[dst, border, inner, :]

        a_half = spread(a, half)
        receive_xy(e)
        low_side = a_half * wy[0] * yrecv[e, 0]
        high_side = a_half * wy[1] * yrecv[e, 1]
        xa = a_all * wx[...] * xrecv[e]
        zpart = z_edges(zpart, low_side, high_side, xa)
        zscale = [a_half * wz[i] for i in range(2)]
        receive_z(e)
        za = [zscale[i] * zrecv[e, i] for i in range(2)]

        @pl.when(k < STEPS - 1)
        def _():
            for i in range(2):
                zsend[e + 1, i] = zpart[i] + za[i]
            send_z(e + 1)

        ya = joined(low_side, high_side)
        keep(za, ya, xa)

        @pl.when(k < STEPS - 1)
        def _():
            xsend[e + 1], ysend[e + 1] = xy_faces(xpart, ypart, za, ya, xa)
            send_xy(e + 1)

        return 0

    lax.fori_loop(0, STEPS, step, 0)
    last = dots[2 * STEPS] + tile_sum(xadd[...] * diag[border - 1] * xsend[STEPS])
    faces = yadd[...] * dy[...] * ysend[STEPS]
    for i in range(2):
        faces = faces + zadd[i] * diag[pl.ds(0, nx), (nz - 1) * i, :] * zsend[STEPS, i]
    sum_begin(2, one_row([last + jnp.sum(faces.reshape(half // 8, 8, LANES), axis=0)]))
    correct(field.at[STEPS])
    sum_middle(1)
    sum_middle(2)
    high, low = sum_end(1)
    kappa = table[2, 0]
    half_kappa = table[2, 1]
    raw = [(all_lanes(high, m), all_lanes(low, m)) for m in range(2 * STEPS - 1)]
    exact = (half_kappa, jnp.zeros((8, LANES), F32))
    raw[1] = dmul(raw[1], exact)
    raw[2] = dmul(dmul(raw[2], exact), exact)
    raw[3] = dmul(raw[3], exact)
    mu = raw[:2]
    for m in range(2, 2 * STEPS - 1):
        mu.append(dadd(dtimes(raw[m], 2.0), dneg(mu[m % 2])))
    alpha, beta, end, pivot, ratio = jacobi_matrix(mu)
    u, v, xu, xv, at_u, at_v = solution_polynomials(alpha, beta, kappa, one)
    for p in (u, v, xu, xv):
        p[1] = p[1] * half_kappa
    end = dadd(end, dtimes(mu[1], -(2.0 ** (2 - 2 * STEPS))))
    high, low = sum_end(2)
    end = dadd(end, dtimes((all_lanes(high, 0), all_lanes(low, 0)), 2.0 ** (3 - 2 * STEPS)))
    end = dadd(ddiv(end, pivot), dneg(ratio))[0]
    scale = one / (at_u - end * at_v)
    xs = [scale * (p - end * q) for p, q in zip(xu, xv)]
    rs = [scale * (p - end * q) for p, q in zip(u, v)]
    for k, v in enumerate(xs):
        coef[k] = v
    for k, v in enumerate(rs):
        coef[16 + k] = v
    for which in range(3):
        for stage in (first, second):
            for copy in arrivals(stage, which):
                copy.wait_send()


def finish(nx, nz, groups, field, diag, coef, x_hbm, r_hbm, xs, rs, sems):
    inner = pl.ds(BASE, nz)
    size = nx // groups

    def spread(c):
        return jnp.broadcast_to(c[None], (nz // 8, 8, LANES)).reshape(nz, LANES)

    def slab(x, _):
        v = field[0, x + 1, inner, :]
        sx = spread(coef[0]) * v
        sr = spread(coef[16]) * v
        for k in range(1, STEPS + 1):
            v = field[k, x + 1, inner, :]
            if k < STEPS:
                sx = sx + spread(coef[k]) * v
            sr = sr + spread(coef[16 + k]) * v
        xs[x] = sx
        rs[x] = diag[x] * sr
        return 0

    copies = []
    for g in range(groups):
        lax.fori_loop(g * size, (g + 1) * size, slab, 0, unroll=2)
        part = pl.ds(g * size, size)
        for n, (src, dst) in enumerate(((xs, x_hbm), (rs, r_hbm))):
            copy = pltpu.make_async_copy(src.at[part], dst.at[part], sems.at[n, g])
            copy.start()
            copies.append(copy)
    for copy in copies:
        copy.wait()


def solution(mesh):
    gx, gy, gz = mesh.shape["gx"], mesh.shape["gy"], mesh.shape["gz"]

    def on_device(right_side, conductivity, absorption):
        nx, ny, nz = right_side.shape
        assert ny == LANES and nx * 2 * 2 == LANES and gx == 2
        args = [jnp.transpose(v, (0, 2, 1)) for v in (right_side, conductivity, absorption)]
        block = (nx, nz, LANES)
        exchanges = STEPS + 1
        dma = pltpu.SemaphoreType.DMA
        tall = nz + 16
        field = (STEPS + 1, nx + 2, tall, LANES)
        vmem = pl.BlockSpec(memory_space=pltpu.VMEM)
        kept = pl.pallas_call(
            functools.partial(kernel, nx, nz, (gx, gy, gz)),
            out_shape=[pltpu.VMEM(field, F32), pltpu.VMEM(block, F32), pltpu.VMEM((32, 8, LANES), F32)],
            in_specs=[pl.BlockSpec(memory_space=pl.ANY)] * 3,
            out_specs=[vmem] * 3,
            scratch_shapes=[
                pltpu.VMEM((nx + 2, tall, LANES), F32),
                pltpu.VMEM(block, F32),
                pltpu.VMEM(block, F32),
                pltpu.VMEM((nx + 1, nz, LANES), F32),
                pltpu.VMEM(block, F32),
                pltpu.VMEM((nx, tall, LANES), F32),
                pltpu.VMEM(block, F32),
                pltpu.VMEM((nz, LANES), F32),
                pltpu.VMEM((2, nz // 2, LANES), F32),
                pltpu.VMEM((nz // 2, LANES), F32),
                pltpu.VMEM((2, nx, LANES), F32),
                pltpu.VMEM((nz, LANES), F32),
                pltpu.VMEM((nz // 2, LANES), F32),
                pltpu.VMEM((2, nx, LANES), F32),
                pltpu.VMEM((exchanges, nz, LANES), F32),
                pltpu.VMEM((exchanges, 2, nx, LANES), F32),
                pltpu.VMEM((exchanges, 2, nx, LANES), F32),
                pltpu.VMEM((exchanges, nz // 2, LANES), F32),
                pltpu.VMEM((exchanges, 2, nz // 2, LANES), F32),
                pltpu.VMEM((exchanges, nz, LANES), F32),
                pltpu.VMEM((3, gx * gy, 1, LANES), F32),
                pltpu.VMEM((3, gz, 2, LANES), F32),
                pltpu.VMEM((2 * STEPS + 2, 8, LANES), F32),
                pltpu.VMEM((STEPS, 2, 8, LANES), F32),
                dma((3,)),
                dma((exchanges, 5)),
                dma((exchanges, 5)),
                dma((3, gx * gy)),
                dma((3, gx * gy)),
                dma((3, gz)),
                dma((3, gz)),
            ],
            compiler_params=pltpu.CompilerParams(
                collective_id=0, has_side_effects=True, vmem_limit_bytes=40 * 1024 * 1024
            ),
        )(*[pltpu.with_memory_space_constraint(v, pltpu.HBM) for v in args])
        groups = 4
        out = pl.pallas_call(
            functools.partial(finish, nx, nz, groups),
            out_shape=[jax.ShapeDtypeStruct(block, F32)] * 2,
            in_specs=[vmem] * 3,
            out_specs=[pl.BlockSpec(memory_space=pltpu.HBM)] * 2,
            scratch_shapes=[pltpu.VMEM(block, F32), pltpu.VMEM(block, F32), dma((2, groups))],
            compiler_params=pltpu.CompilerParams(vmem_limit_bytes=20 * 1024 * 1024),
        )(*kept)
        return tuple(jnp.transpose(v, (0, 2, 1)) for v in out)

    spec = P("gx", "gy", "gz")
    return jax.shard_map(on_device, mesh=mesh, in_specs=(spec,) * 3, out_specs=(spec,) * 2, check_vma=False)
```

```python
import functools

import jax
import jax.numpy as jnp
from jax import lax
from jax.experimental import pallas as pl
from jax.experimental.pallas import tpu as pltpu
from jax.sharding import PartitionSpec as P

F32 = jnp.float32
MESH = pl.DeviceIdType.MESH
STEPS = 10
LANES = 128
BASE = 8


def two_sum(a, b):
    s = a + b
    t = s - a
    return s, (a - (s - t)) + (b - t)


def joined_sum(a, b):
    s, e = two_sum(a[0], b[0])
    return s, e if a[1] is None else e + (a[1] + b[1])


def renew(a, b):
    s = a + b
    return s, b - (s - a)


def halves(a):
    t = 4097.0 * a
    high = t - (t - a)
    return high, a - high


def two_product(a, b):
    p = a * b
    ah, al = halves(a)
    bh, bl = halves(b)
    return p, ((ah * bh - p) + ah * bl + al * bh) + al * bl


def dadd(a, b):
    s, e = two_sum(a[0], b[0])
    return renew(s, e + (a[1] + b[1]))


def dneg(a):
    return -a[0], -a[1]


def dmul(a, b):
    p, e = two_product(a[0], b[0])
    return renew(p, e + (a[0] * b[1] + a[1] * b[0]))


def dtimes(a, power):
    return power * a[0], power * a[1]


def ddiv(a, b):
    q = a[0] / b[0]
    p, e = two_product(q, b[0])
    rest = ((a[0] - p) - e) + (a[1] - q * b[1])
    return renew(q, rest / b[0])


def jacobi_matrix(mu):
    n = (len(mu) + 1) // 2
    zero = (0.0 * mu[0][0], 0.0 * mu[0][0])
    cur = [mu[0]] + [dtimes(mu[k], 2.0 ** (1 - k)) for k in range(1, 2 * n - 1)] + [zero]
    prev = None
    ratio = ddiv(cur[1], cur[0])
    alpha, beta = [ratio], [None]
    for k in range(1, n):
        new = [None] * (2 * n)
        minus_alpha = dneg(alpha[-1])
        minus_beta = None if k == 1 else dneg(beta[-1])
        for l in range(k, 2 * n - k):
            v = dadd(cur[l + 1], dmul(minus_alpha, cur[l]))
            if prev is not None:
                v = dadd(v, dmul(minus_beta, prev[l]))
            new[l] = dadd(v, dtimes(cur[l - 1], 0.5 if l == 1 else 0.25))
        beta.append(ddiv(new[k], cur[k - 1]))
        prev, cur = cur, new
        if k < n - 1:
            later = ddiv(new[k + 1], new[k])
            alpha.append(dadd(later, dneg(ratio)))
            ratio = later
    high = [a[0] for a in alpha], [None if b is None else b[0] for b in beta]
    return high[0], high[1], cur[n], cur[n - 1], ratio


def without_pole(p, kappa):
    n = len(p) - 1
    q = [None] * (n + 2)
    q[n] = q[n + 1] = 0.0 * kappa
    for k in range(n, 1, -1):
        q[k - 1] = (q[k] + p[k]) * kappa - q[k + 1]
    q[0] = (q[1] + p[1]) * (0.5 * kappa) - 0.5 * q[2]
    return q[:n]


def solution_polynomials(alpha, beta, kappa, one):
    n = len(beta)
    tau = 0.5 * kappa
    at = [one, tau - alpha[0]]
    for k in range(1, n - 1):
        at.append((tau - alpha[k]) * at[-1] - beta[k] * at[-2])
    before, p = None, [one]
    for k in range(n):
        new = [None] * (k + 2)

        def put(i, v):
            new[i] = v if new[i] is None else new[i] + v

        for i, v in enumerate(p):
            half = 0.5 * v
            put(i + 1, half)
            put(abs(i - 1), half)
        if k < n - 1:
            for i, v in enumerate(p):
                put(i, -(alpha[k] * v))
        if before is not None:
            for i, v in enumerate(before):
                put(i, -(beta[k] * v))
        before, p = p, new
    v = before + [0.0 * one]
    at_u = tau * at[-1] - beta[n - 1] * at[-2]
    return p, v, without_pole(p, kappa), without_pole(v, kappa), at_u, at[-1]


def kernel(nx, nz, sizes, r_hbm, c_hbm, a_hbm, field, diag, coef,
           cond, absorb, weight, fx, fy, fz, turned, wx, wy, dy, wz, wzn, zterm, zown, xadd, yadd, zadd, xsend, zsend, zrecv, ysend, yrecv, xrecv,
           part1, part2, dots, table,
           load_sem, face_send, face_recv, wz_send, wz_recv, sum1_send, sum1_recv, sum2_send, sum2_recv):
    gx, gy, gz = sizes
    ix, iy, iz = lax.axis_index("gx"), lax.axis_index("gy"), lax.axis_index("gz")
    ox = 1 - ix
    base = BASE
    inner = pl.ds(base, nz)
    above = pl.ds(base + 1, nz)
    below = pl.ds(base - 1, nz)
    half = nz // 2
    tiles = nz // 8
    low_x = ix == 0
    border = jnp.where(low_x, nx, 1)

    loads = [
        pltpu.make_async_copy(c_hbm, cond.at[pl.ds(1, nx), inner, :], load_sem.at[0]),
        pltpu.make_async_copy(a_hbm, absorb, load_sem.at[1]),
        pltpu.make_async_copy(r_hbm, weight, load_sem.at[2]),
    ]
    loads[0].start()
    loads[1].start()

    zero_face = jnp.zeros((nx, LANES), F32)
    zero_slab = jnp.zeros((nz, LANES), F32)

    barrier = pltpu.get_barrier_semaphore()
    group = [((ix + dx) % gx, (iy + dy) % gy) for dx in range(gx) for dy in range(gy) if (dx, dy) != (0, 0)]
    line = [(iz + d) % gz for d in range(1, gz)]
    for px, py in group:
        pl.semaphore_signal(barrier, inc=1, device_id=(px, py, iz), device_id_type=MESH)
    for pz in line:
        pl.semaphore_signal(barrier, inc=1, device_id=(ix, iy, pz), device_id_type=MESH)

    for ref, side, alone in ((zrecv, 0, iz == 0), (zrecv, 1, iz == gz - 1), (yrecv, 0, iy == 0), (yrecv, 1, iy == gy - 1)):

        @pl.when(alone)
        def _(ref=ref, side=side):
            def clear_faces(k, _):
                ref[k, side] = zero_face
                return 0

            lax.fori_loop(0, STEPS + 1, clear_faces, 0)
            if ref is zrecv:
                wzn[side] = zero_face

    lane = lax.broadcasted_iota(jnp.int32, (half, LANES), 1)
    pair = lane // 2
    even = (lane % 2) == 0
    row_lane = lax.broadcasted_iota(jnp.int32, (1, LANES), 1)

    def tile_sum(v):
        return jnp.sum(v.reshape(tiles, 8, LANES), axis=0)

    def spread(c, rows=nz):
        return jnp.broadcast_to(c[None], (rows // 8, 8, LANES)).reshape(rows, LANES)

    def turn_of(x, h):
        return 2 * x + 2 * nx * h

    def pack(source, skip=1, start=base):
        out = jnp.zeros((half, LANES), F32)
        for x in range(nx):
            for h in range(2):
                v = source[x + skip, pl.ds(start + half * h, half), :]
                out = jnp.where(pair == x + nx * h, pltpu.roll(v, (turn_of(x, h) + 1) % LANES, 1), out)
        return out

    def copies(e):
        xc = pltpu.make_async_remote_copy(
            xsend.at[e], xrecv.at[e],
            face_send.at[e, 0], face_recv.at[e, 0], device_id=(ox, iy, iz), device_id_type=MESH)
        yc, zc = [], []
        for up in range(2):
            yc.append(pltpu.make_async_remote_copy(
                ysend.at[e], yrecv.at[e, 1 - up], face_send.at[e, 1 + up], face_recv.at[e, 2 - up],
                device_id=(ix, jnp.clip(iy + 2 * up - 1, 0, gy - 1), iz), device_id_type=MESH))
            zc.append(pltpu.make_async_remote_copy(
                zsend.at[e, up], zrecv.at[e, 1 - up], face_send.at[e, 3 + up], face_recv.at[e, 4 - up],
                device_id=(ix, iy, jnp.clip(iz + 2 * up - 1, 0, gz - 1)), device_id_type=MESH))
        return xc, yc, zc

    def send_z(e):
        _, _, zc = copies(e)
        pl.when(iz > 0)(zc[0].start)
        pl.when(iz < gz - 1)(zc[1].start)

    def send_xy(e):
        xc, yc, _ = copies(e)
        pl.when(iy > 0)(yc[0].start)
        pl.when(iy < gy - 1)(yc[1].start)
        xc.start()

    def fill_z(source, e):
        zsend[e, 0] = source[pl.ds(1, nx), base, :]
        zsend[e, 1] = source[pl.ds(1, nx), base + nz - 1, :]

    def fill_xy(source, e):
        ysend[e] = pack(source)
        xsend[e] = source[border, inner, :]

    def receive_xy(e):
        xc, yc, _ = copies(e)
        xc.wait()
        pl.when(iy > 0)(lambda: (yc[0].wait_send(), yc[1].wait_recv())[0])
        pl.when(iy < gy - 1)(lambda: (yc[1].wait_send(), yc[0].wait_recv())[0])

    def weights():
        return [
            pltpu.make_async_remote_copy(
                wz.at[up], wzn.at[1 - up], wz_send.at[up], wz_recv.at[1 - up],
                device_id=(ix, iy, jnp.clip(iz + 2 * up - 1, 0, gz - 1)), device_id_type=MESH)
            for up in range(2)
        ]

    def receive_z(e):
        _, _, zc = copies(e)
        pl.when(iz > 0)(lambda: (zc[0].wait_send(), zc[1].wait_recv())[0])
        pl.when(iz < gz - 1)(lambda: (zc[1].wait_send(), zc[0].wait_recv())[0])

    gxy = ix * gy + iy
    first = (part1, [(px, py, iz) for px, py in group], gxy, sum1_send, sum1_recv, [px * gy + py for px, py in group])
    second = (part2, [(ix, iy, pz) for pz in line], iz, sum2_send, sum2_recv, line)

    def spread_out(stage, which):
        part, peers, mine, send_sem, recv_sem, _ = stage
        for i, peer in enumerate(peers):
            pltpu.make_async_remote_copy(
                part.at[which, mine], part.at[which, mine], send_sem.at[which, i], recv_sem.at[which, mine],
                device_id=peer, device_id_type=MESH).start()

    def arrivals(stage, which):
        part, peers, _, send_sem, recv_sem, slots = stage
        return [
            pltpu.make_async_remote_copy(
                part.at[which, slot], part.at[which, slot], send_sem.at[which, i], recv_sem.at[which, slot],
                device_id=peers[i], device_id_type=MESH)
            for i, slot in enumerate(slots)
        ]

    def gather_in(stage, which):
        part = stage[0]
        for copy in arrivals(stage, which):
            copy.wait_recv()
        pairs = [(part[which, i], None) for i in range(part.shape[1])]
        while len(pairs) > 1:
            pairs = [joined_sum(*pairs[i:i + 2]) for i in range(0, len(pairs), 2)]
        return pairs[0]

    def sum_begin(which, row):
        part1[which, gxy] = row
        spread_out(first, which)

    def sum_middle(which):
        high, low = renew(*gather_in(first, which))
        part2[which, iz, pl.ds(0, 1), :] = high
        part2[which, iz, pl.ds(1, 1), :] = low
        spread_out(second, which)

    def sum_end(which):
        total, error = gather_in(second, which)
        return renew(total[0:1], error[0:1] + total[1:2])

    def all_lanes(row, m):
        return jnp.broadcast_to(jnp.sum(jnp.where(row_lane == m, row, 0.0), axis=1, keepdims=True), (8, LANES))

    def one_row(values):
        row = jnp.zeros((1, LANES), F32)
        for m, v in enumerate(values):
            row = jnp.where(row_lane == m, jnp.sum(jnp.sum(v, axis=0, keepdims=True), axis=1, keepdims=True), row)
        return row

    wide_lane = lax.broadcasted_iota(jnp.int32, (nz, LANES), 1)
    inside = wide_lane < LANES - 1
    after = wide_lane > 0
    edge = (wide_lane == 0) | (wide_lane == LANES - 1)
    one = jnp.ones((8, LANES), F32)

    face_row = lax.broadcasted_iota(jnp.int32, (nx, LANES), 0)
    face_lane = lax.broadcasted_iota(jnp.int32, (nx, LANES), 1)
    half_row = lax.broadcasted_iota(jnp.int32, (half, LANES), 0)
    slab_row = lax.broadcasted_iota(jnp.int32, (nz, LANES), 0)

    def z_edges(zpart, low_side, high_side, xa):
        faces = []
        for h in range(2):
            at = (half - 1) * h
            face = zpart[h]
            for at_lane, side, shift in ((0, low_side, 0), (LANES - 1, high_side, 1)):
                one_lane = jnp.where(face_lane == 2 * face_row + 2 * nx * h + shift, side[at:at + 1], 0.0)
                face = face + jnp.where(face_lane == at_lane, jnp.sum(one_lane, axis=1, keepdims=True), 0.0)
            at = (nz - 1) * h
            faces.append(face + jnp.where(face_row == border - 1, xa[at:at + 1], 0.0))
        return faces

    def joined(low_side, high_side):
        return jnp.where(even, pltpu.roll(high_side, LANES - 1, 1), pltpu.roll(low_side, 1, 1))

    def xy_faces(xpart, ypart, za, ya, xa):
        yface, xface = ypart + ya, xpart + xa
        xlanes = []
        for h in range(2):
            here = 2 * nx * h + 1
            at = half_row == (half - 1) * h
            moved = jnp.where(face_lane // 2 == face_row + nx * h, pltpu.roll(za[h], here, 1, stride=2, stride_axis=0), 0.0)
            yface = yface + jnp.where(at, jnp.sum(moved, axis=0, keepdims=True), 0.0)
            xa_half = xa[half * h:half * (h + 1)]
            turns = [(2 * (nx - 1) + here) % LANES, here]
            moved = jnp.where(low_x, pltpu.roll(xa_half, turns[0], 1), pltpu.roll(xa_half, turns[1], 1))
            yface = yface + jnp.where(pair == border - 1 + nx * h, moved, 0.0)
            moved = jnp.where(low_x, pltpu.roll(ya, (LANES - turns[0]) % LANES, 1), pltpu.roll(ya, LANES - turns[1], 1))
            xlanes.append(moved)
            z_at = slab_row == (nz - 1) * h
            xface = xface + jnp.where(z_at, jnp.sum(jnp.where(face_row == border - 1, za[h], 0.0), axis=0, keepdims=True), 0.0)
        return xface + jnp.where(edge, jnp.concatenate(xlanes, axis=0), 0.0), yface

    def keep(za, ya, xa):
        yadd[...] = ya
        zadd[0] = za[0]
        zadd[1] = za[1]
        xadd[...] = xa

    def correct(ref, skip=1, start=base):
        ref[pl.ds(skip, nx), start, :] += zadd[0]
        ref[pl.ds(skip, nx), start + nz - 1, :] += zadd[1]
        ref[border - 1 + skip, pl.ds(start, nz), :] += xadd[...]
        terms = yadd[...]
        for x in range(nx):
            for h in range(2):
                turned[x, pl.ds(half * h, half), :] = pltpu.roll(terms, (LANES - turn_of(x, h) - 1) % LANES, 1)

        def add_sides(x, _):
            ref[x + skip, pl.ds(start, nz), :] += jnp.where(edge, turned[x], 0.0)
            return 0

        lax.fori_loop(0, nx, add_sides, 0, unroll=4)

    loads[0].wait()
    loads[2].start()
    pl.semaphore_wait(barrier, len(group) + len(line))
    fill_z(cond, 0)
    send_z(0)
    fill_xy(cond, 0)
    send_xy(0)
    loads[1].wait()

    def means(x, acc):
        return acc[0] + cond[x + 1, inner, :], acc[1] + absorb[x]

    sums = lax.fori_loop(0, nx, means, (zero_slab, zero_slab), unroll=4)
    sum_begin(0, one_row([tile_sum(v) for v in sums]))

    def clear(k, _):
        field[k, 0, inner, :] = zero_slab
        field[k, nx + 1, inner, :] = zero_slab
        field[k, pl.ds(1, nx), base - 1, :] = zero_face
        field[k, pl.ds(1, nx), base + nz, :] = zero_face
        return 0

    lax.fori_loop(0, STEPS, clear, 0)
    table[0, 0] = one
    table[0, 1] = jnp.zeros((8, LANES), F32)
    cond[0, inner, :] = zero_slab
    cond[nx + 1, inner, :] = zero_slab
    cond[pl.ds(1, nx), base - 1, :] = zero_face
    cond[pl.ds(1, nx), base + nz, :] = zero_face
    fx[0] = 0.5 * cond[1, inner, :]

    def coefficients(x, _):
        here = cond[x + 1, inner, :]
        xp = 0.5 * (here + cond[x + 2, inner, :])
        xm = fx[x]
        yp = 0.5 * (here + jnp.where(inside, pltpu.roll(here, LANES - 1, 1), 0.0))
        ym = 0.5 * (here + jnp.where(after, pltpu.roll(here, 1, 1), 0.0))
        zp = 0.5 * (here + cond[x + 1, above, :])
        zm = 0.5 * (here + cond[x + 1, below, :])
        fx[x + 1] = xp
        fy[x] = jnp.where(inside, yp, 0.0)
        fz[x, below, :] = zm
        fz[x, inner, :] = zp
        diag[x] = absorb[x] + xp + xm + yp + ym + zp + zm
        return 0

    lax.fori_loop(0, nx, coefficients, 0, unroll=8)
    loads[2].wait()
    ypart, yright = pack(diag, 0, 0), pack(weight, 0, 0)
    zpart = [diag[pl.ds(0, nx), (nz - 1) * i, :] for i in range(2)]
    zright = [weight[pl.ds(0, nx), (nz - 1) * i, :] for i in range(2)]
    receive_xy(0)
    low_side, high_side = 0.5 * yrecv[0, 0], 0.5 * yrecv[0, 1]
    xa = 0.5 * xrecv[0]
    zpart = z_edges(zpart, low_side, high_side, xa)
    receive_z(0)
    za = [0.5 * zrecv[0, i] for i in range(2)]
    zdiag = [zpart[i] + za[i] for i in range(2)]
    for i in range(2):
        zsend[1, i] = zright[i] / zdiag[i]
    send_z(1)
    ya = joined(low_side, high_side)
    xdiag, ydiag = xy_faces(diag[border - 1], ypart, za, ya, xa)
    xsend[1] = weight[border - 1] / xdiag
    ysend[1] = yright / ydiag
    send_xy(1)
    for i in range(2):
        wz[i] = (0.5 * zsend[0, i] + za[i]) / zdiag[i]
    down, upward = weights()
    pl.when(iz > 0)(down.start)
    pl.when(iz < gz - 1)(upward.start)
    for i in range(2):
        zterm[i] = zero_face
        zown[0, i] = zsend[1, i]
    wx[...] = (0.5 * xsend[0] + xa) / xdiag
    sides = (0.5 * ysend[0] + ya) / ydiag
    wy[0] = jnp.where(even, pltpu.roll(sides, LANES - 1, 1), 0.0)
    wy[1] = jnp.where(even, 0.0, pltpu.roll(sides, 1, 1))
    dy[...] = ydiag
    sum_middle(0)
    keep(za, ya, xa)
    correct(diag, 0, 0)

    def begin(x, _):
        inverse = 1.0 / diag[x]
        field[0, x + 1, inner, :] = weight[x] * inverse
        weight[x] = inverse
        return 0

    lax.fori_loop(0, nx, begin, 0, unroll=4)
    keep([zero_face, zero_face], jnp.zeros((half, LANES), F32), zero_slab)

    def step(k, _):
        src, dst, old = k, k + 1, jnp.maximum(k - 1, 0)
        e = k + 1

        @pl.when(k == 1)
        def _():
            high, _ = sum_end(0)
            six = 6.0 * all_lanes(high, 0)
            rho = 0.97 * six / (six + all_lanes(high, 1))
            kappa = jnp.floor(64.0 * (2.0 / rho)) * (1.0 / 64.0)
            half_kappa = 0.5 * kappa
            table[1, 0] = kappa * half_kappa
            table[1, 1] = one
            table[2, 0] = kappa
            table[2, 1] = half_kappa
            for j in range(3, STEPS):
                table[j, 0] = kappa
                table[j, 1] = one

        @pl.when(k == 1)
        def _():
            down, upward = weights()
            pl.when(iz > 0)(lambda: (down.wait_send(), upward.wait_recv())[0])
            pl.when(iz < gz - 1)(lambda: (upward.wait_send(), down.wait_recv())[0])

        @pl.when(k > 0)
        def _():
            before = spread(table[k - 1, 0], half)
            for i in range(2):
                zterm[i] = before * wzn[i] * zown[k - 1, i]

        correct(field.at[k])
        a = table[k, 0]
        a_all, b_all = spread(a), spread(table[k, 1])

        def row(x, acc):
            same, older, ahead = acc
            v = field[src, x + 1, inner, :]
            y = fy[x]
            o = field[old, x + 1, inner, :]
            s = fx[x + 1] * field[src, x + 2, inner, :] + fx[x] * field[src, x, inner, :]
            s = s + fz[x, inner, :] * field[src, x + 1, above, :] + fz[x, below, :] * field[src, x + 1, below, :]
            s = s + y * pltpu.roll(v, LANES - 1, 1) + pltpu.roll(y * v, 1, 1)
            new = a_all * (weight[x] * s) - b_all * o
            field[dst, x + 1, inner, :] = new
            w = diag[x] * v
            return same + w * v, older + w * o, ahead + w * new

        same, older, ahead = lax.fori_loop(0, nx, row, (zero_slab, zero_slab, zero_slab), unroll=4)
        dots[2 * k] = tile_sum(same)
        dots[2 * k + 1] = tile_sum(older)
        dots[2 * STEPS] = tile_sum(ahead)

        @pl.when(k == STEPS - 1)
        def _():
            sum_begin(1, one_row([dots[m if m % 2 == 0 else m + 2] for m in range(2 * STEPS - 1)]))


        ypart = pack(field.at[dst])
        zpart = [field[dst, pl.ds(1, nx), base + row_, :] for row_ in (0, nz - 1)]
        xpart = field[dst, border, inner, :]

        a_half = spread(a, half)
        receive_xy(e)
        low_side = a_half * wy[0] * yrecv[e, 0]
        high_side = a_half * wy[1] * yrecv[e, 1]
        xa = a_all * wx[...] * xrecv[e]
        zpart = z_edges(zpart, low_side, high_side, xa)

        @pl.when(k < STEPS - 1)
        def _():
            for i in range(2):
                zsend[e + 1, i] = zpart[i]
            send_z(e + 1)

        zscale = [a_half * wz[i] for i in range(2)]
        receive_z(e)
        za = [zscale[i] * (zrecv[e, i] + zterm[i]) for i in range(2)]
        for i in range(2):
            zown[k + 1, i] = zpart[i] + za[i]
        ya = joined(low_side, high_side)
        keep(za, ya, xa)

        @pl.when(k < STEPS - 1)
        def _():
            xsend[e + 1], ysend[e + 1] = xy_faces(xpart, ypart, za, ya, xa)
            send_xy(e + 1)

        return 0

    lax.fori_loop(0, STEPS, step, 0)
    last = dots[2 * STEPS] + tile_sum(xadd[...] * diag[border - 1] * xsend[STEPS])
    faces = yadd[...] * dy[...] * ysend[STEPS]
    for i in range(2):
        faces = faces + zadd[i] * diag[pl.ds(0, nx), (nz - 1) * i, :] * zown[STEPS - 1, i]
    sum_begin(2, one_row([last + jnp.sum(faces.reshape(half // 8, 8, LANES), axis=0)]))
    correct(field.at[STEPS])
    sum_middle(1)
    sum_middle(2)
    high, low = sum_end(1)
    kappa = table[2, 0]
    half_kappa = table[2, 1]
    raw = [(all_lanes(high, m), all_lanes(low, m)) for m in range(2 * STEPS - 1)]
    exact = (half_kappa, jnp.zeros((8, LANES), F32))
    raw[1] = dmul(raw[1], exact)
    raw[2] = dmul(dmul(raw[2], exact), exact)
    raw[3] = dmul(raw[3], exact)
    mu = raw[:2]
    for m in range(2, 2 * STEPS - 1):
        mu.append(dadd(dtimes(raw[m], 2.0), dneg(mu[m % 2])))
    alpha, beta, end, pivot, ratio = jacobi_matrix(mu)
    u, v, xu, xv, at_u, at_v = solution_polynomials(alpha, beta, kappa, one)
    for p in (u, v, xu, xv):
        p[1] = p[1] * half_kappa
    end = dadd(end, dtimes(mu[1], -(2.0 ** (2 - 2 * STEPS))))
    high, low = sum_end(2)
    end = dadd(end, dtimes((all_lanes(high, 0), all_lanes(low, 0)), 2.0 ** (3 - 2 * STEPS)))
    end = dadd(ddiv(end, pivot), dneg(ratio))[0]
    scale = one / (at_u - end * at_v)
    xs = [scale * (p - end * q) for p, q in zip(xu, xv)]
    rs = [scale * (p - end * q) for p, q in zip(u, v)]
    for k, v in enumerate(xs):
        coef[k] = v
    for k, v in enumerate(rs):
        coef[16 + k] = v
    for which in range(3):
        for stage in (first, second):
            for copy in arrivals(stage, which):
                copy.wait_send()


def finish(nx, nz, groups, field, diag, coef, x_hbm, r_hbm, xs, rs, sems):
    inner = pl.ds(BASE, nz)
    size = nx // groups

    def spread(c):
        return jnp.broadcast_to(c[None], (nz // 8, 8, LANES)).reshape(nz, LANES)

    def slab(x, _):
        v = field[0, x + 1, inner, :]
        sx = spread(coef[0]) * v
        sr = spread(coef[16]) * v
        for k in range(1, STEPS + 1):
            v = field[k, x + 1, inner, :]
            if k < STEPS:
                sx = sx + spread(coef[k]) * v
            sr = sr + spread(coef[16 + k]) * v
        xs[x] = sx
        rs[x] = diag[x] * sr
        return 0

    copies = []
    for g in range(groups):
        lax.fori_loop(g * size, (g + 1) * size, slab, 0, unroll=4)
        part = pl.ds(g * size, size)
        for n, (src, dst) in enumerate(((xs, x_hbm), (rs, r_hbm))):
            copy = pltpu.make_async_copy(src.at[part], dst.at[part], sems.at[n, g])
            copy.start()
            copies.append(copy)
    for copy in copies:
        copy.wait()


def solution(mesh):
    gx, gy, gz = mesh.shape["gx"], mesh.shape["gy"], mesh.shape["gz"]

    def on_device(right_side, conductivity, absorption):
        nx, ny, nz = right_side.shape
        assert ny == LANES and nx * 2 * 2 == LANES and gx == 2
        args = [jnp.transpose(v, (0, 2, 1)) for v in (right_side, conductivity, absorption)]
        block = (nx, nz, LANES)
        exchanges = STEPS + 1
        dma = pltpu.SemaphoreType.DMA
        tall = nz + 16
        field = (STEPS + 1, nx + 2, tall, LANES)
        vmem = pl.BlockSpec(memory_space=pltpu.VMEM)
        kept = pl.pallas_call(
            functools.partial(kernel, nx, nz, (gx, gy, gz)),
            out_shape=[pltpu.VMEM(field, F32), pltpu.VMEM(block, F32), pltpu.VMEM((32, 8, LANES), F32)],
            in_specs=[pl.BlockSpec(memory_space=pl.ANY)] * 3,
            out_specs=[vmem] * 3,
            scratch_shapes=[
                pltpu.VMEM((nx + 2, tall, LANES), F32),
                pltpu.VMEM(block, F32),
                pltpu.VMEM(block, F32),
                pltpu.VMEM((nx + 1, nz, LANES), F32),
                pltpu.VMEM(block, F32),
                pltpu.VMEM((nx, tall, LANES), F32),
                pltpu.VMEM(block, F32),
                pltpu.VMEM((nz, LANES), F32),
                pltpu.VMEM((2, nz // 2, LANES), F32),
                pltpu.VMEM((nz // 2, LANES), F32),
                pltpu.VMEM((2, nx, LANES), F32),
                pltpu.VMEM((2, nx, LANES), F32),
                pltpu.VMEM((2, nx, LANES), F32),
                pltpu.VMEM((STEPS + 1, 2, nx, LANES), F32),
                pltpu.VMEM((nz, LANES), F32),
                pltpu.VMEM((nz // 2, LANES), F32),
                pltpu.VMEM((2, nx, LANES), F32),
                pltpu.VMEM((exchanges, nz, LANES), F32),
                pltpu.VMEM((exchanges, 2, nx, LANES), F32),
                pltpu.VMEM((exchanges, 2, nx, LANES), F32),
                pltpu.VMEM((exchanges, nz // 2, LANES), F32),
                pltpu.VMEM((exchanges, 2, nz // 2, LANES), F32),
                pltpu.VMEM((exchanges, nz, LANES), F32),
                pltpu.VMEM((3, gx * gy, 1, LANES), F32),
                pltpu.VMEM((3, gz, 2, LANES), F32),
                pltpu.VMEM((2 * STEPS + 2, 8, LANES), F32),
                pltpu.VMEM((STEPS, 2, 8, LANES), F32),
                dma((3,)),
                dma((exchanges, 5)),
                dma((exchanges, 5)),
                dma((2,)),
                dma((2,)),
                dma((3, gx * gy)),
                dma((3, gx * gy)),
                dma((3, gz)),
                dma((3, gz)),
            ],
            compiler_params=pltpu.CompilerParams(
                collective_id=0, has_side_effects=True, vmem_limit_bytes=40 * 1024 * 1024
            ),
        )(*[pltpu.with_memory_space_constraint(v, pltpu.HBM) for v in args])
        groups = 4
        out = pl.pallas_call(
            functools.partial(finish, nx, nz, groups),
            out_shape=[jax.ShapeDtypeStruct(block, F32)] * 2,
            in_specs=[vmem] * 3,
            out_specs=[pl.BlockSpec(memory_space=pltpu.HBM)] * 2,
            scratch_shapes=[pltpu.VMEM(block, F32), pltpu.VMEM(block, F32), dma((2, groups))],
            compiler_params=pltpu.CompilerParams(vmem_limit_bytes=20 * 1024 * 1024),
        )(*kept)
        return tuple(jnp.transpose(v, (0, 2, 1)) for v in out)

    spec = P("gx", "gy", "gz")
    return jax.shard_map(on_device, mesh=mesh, in_specs=(spec,) * 3, out_specs=(spec,) * 2, check_vma=False)
```

```python
import functools

import jax
import jax.numpy as jnp
from jax import lax
from jax.experimental import pallas as pl
from jax.experimental.pallas import tpu as pltpu
from jax.sharding import PartitionSpec as P

F32 = jnp.float32
MESH = pl.DeviceIdType.MESH
STEPS = 10
LANES = 128
BASE = 8


def two_sum(a, b):
    s = a + b
    t = s - a
    return s, (a - (s - t)) + (b - t)


def joined_sum(a, b):
    s, e = two_sum(a[0], b[0])
    return s, e if a[1] is None else e + (a[1] + b[1])


def renew(a, b):
    s = a + b
    return s, b - (s - a)


def halves(a):
    t = 4097.0 * a
    high = t - (t - a)
    return high, a - high


def two_product(a, b):
    p = a * b
    ah, al = halves(a)
    bh, bl = halves(b)
    return p, ((ah * bh - p) + ah * bl + al * bh) + al * bl


def dadd(a, b):
    s, e = two_sum(a[0], b[0])
    return renew(s, e + (a[1] + b[1]))


def dneg(a):
    return -a[0], -a[1]


def dmul(a, b):
    p, e = two_product(a[0], b[0])
    return renew(p, e + (a[0] * b[1] + a[1] * b[0]))


def dtimes(a, power):
    return power * a[0], power * a[1]


def ddiv(a, b):
    q = a[0] / b[0]
    p, e = two_product(q, b[0])
    rest = ((a[0] - p) - e) + (a[1] - q * b[1])
    return renew(q, rest / b[0])


def jacobi_matrix(mu):
    n = (len(mu) + 1) // 2
    zero = (0.0 * mu[0][0], 0.0 * mu[0][0])
    cur = [mu[0]] + [dtimes(mu[k], 2.0 ** (1 - k)) for k in range(1, 2 * n - 1)] + [zero]
    prev = None
    ratio = ddiv(cur[1], cur[0])
    alpha, beta = [ratio], [None]
    for k in range(1, n):
        new = [None] * (2 * n)
        minus_alpha = dneg(alpha[-1])
        minus_beta = None if k == 1 else dneg(beta[-1])
        for l in range(k, 2 * n - k):
            v = dadd(cur[l + 1], dmul(minus_alpha, cur[l]))
            if prev is not None:
                v = dadd(v, dmul(minus_beta, prev[l]))
            new[l] = dadd(v, dtimes(cur[l - 1], 0.5 if l == 1 else 0.25))
        beta.append(ddiv(new[k], cur[k - 1]))
        prev, cur = cur, new
        if k < n - 1:
            later = ddiv(new[k + 1], new[k])
            alpha.append(dadd(later, dneg(ratio)))
            ratio = later
    high = [a[0] for a in alpha], [None if b is None else b[0] for b in beta]
    return high[0], high[1], cur[n], cur[n - 1], ratio


def without_pole(p, kappa):
    n = len(p) - 1
    q = [None] * (n + 2)
    q[n] = q[n + 1] = 0.0 * kappa
    for k in range(n, 1, -1):
        q[k - 1] = (q[k] + p[k]) * kappa - q[k + 1]
    q[0] = (q[1] + p[1]) * (0.5 * kappa) - 0.5 * q[2]
    return q[:n]


def solution_polynomials(alpha, beta, kappa, one):
    n = len(beta)
    tau = 0.5 * kappa
    at = [one, tau - alpha[0]]
    for k in range(1, n - 1):
        at.append((tau - alpha[k]) * at[-1] - beta[k] * at[-2])
    before, p = None, [one]
    for k in range(n):
        new = [None] * (k + 2)

        def put(i, v):
            new[i] = v if new[i] is None else new[i] + v

        for i, v in enumerate(p):
            half = 0.5 * v
            put(i + 1, half)
            put(abs(i - 1), half)
        if k < n - 1:
            for i, v in enumerate(p):
                put(i, -(alpha[k] * v))
        if before is not None:
            for i, v in enumerate(before):
                put(i, -(beta[k] * v))
        before, p = p, new
    v = before + [0.0 * one]
    at_u = tau * at[-1] - beta[n - 1] * at[-2]
    return p, v, without_pole(p, kappa), without_pole(v, kappa), at_u, at[-1]


def kernel(nx, nz, sizes, r_hbm, c_hbm, a_hbm, field, diag, coef,
           cond, absorb, weight, fx, fy, fz, turned, wx, wy, dy, wz, wzn, zterm, zown, xadd, yadd, zadd, xsend, zsend, zrecv, ysend, yrecv, xrecv,
           part1, part2, dots, table,
           load_sem, face_send, face_recv, wz_send, wz_recv, sum1_send, sum1_recv, sum2_send, sum2_recv):
    gx, gy, gz = sizes
    ix, iy, iz = lax.axis_index("gx"), lax.axis_index("gy"), lax.axis_index("gz")
    ox = 1 - ix
    base = BASE
    inner = pl.ds(base, nz)
    above = pl.ds(base + 1, nz)
    below = pl.ds(base - 1, nz)
    half = nz // 2
    tiles = nz // 8
    low_x = ix == 0
    border = jnp.where(low_x, nx, 1)

    loads = [
        pltpu.make_async_copy(c_hbm, cond.at[pl.ds(1, nx), inner, :], load_sem.at[0]),
        pltpu.make_async_copy(a_hbm, absorb, load_sem.at[1]),
        pltpu.make_async_copy(r_hbm, weight, load_sem.at[2]),
    ]
    loads[0].start()
    loads[1].start()

    zero_face = jnp.zeros((nx, LANES), F32)
    zero_slab = jnp.zeros((nz, LANES), F32)

    barrier = pltpu.get_barrier_semaphore()
    group = [((ix + dx) % gx, (iy + dy) % gy) for dx in range(gx) for dy in range(gy) if (dx, dy) != (0, 0)]
    line = [(iz + d) % gz for d in range(1, gz)]
    for px, py in group:
        pl.semaphore_signal(barrier, inc=1, device_id=(px, py, iz), device_id_type=MESH)
    for pz in line:
        pl.semaphore_signal(barrier, inc=1, device_id=(ix, iy, pz), device_id_type=MESH)

    for ref, side, alone in ((zrecv, 0, iz == 0), (zrecv, 1, iz == gz - 1), (yrecv, 0, iy == 0), (yrecv, 1, iy == gy - 1)):

        @pl.when(alone)
        def _(ref=ref, side=side):
            def clear_faces(k, _):
                ref[k, side] = zero_face
                return 0

            lax.fori_loop(0, STEPS + 1, clear_faces, 0)
            if ref is zrecv:
                wzn[side] = zero_face

    lane = lax.broadcasted_iota(jnp.int32, (half, LANES), 1)
    pair = lane // 2
    even = (lane % 2) == 0
    row_lane = lax.broadcasted_iota(jnp.int32, (1, LANES), 1)

    def tile_sum(v):
        return jnp.sum(v.reshape(tiles, 8, LANES), axis=0)

    def spread(c, rows=nz):
        return jnp.broadcast_to(c[None], (rows // 8, 8, LANES)).reshape(rows, LANES)

    def turn_of(x, h):
        return 2 * x + 2 * nx * h

    def pack(source, skip=1, start=base):
        out = jnp.zeros((half, LANES), F32)
        for x in range(nx):
            for h in range(2):
                v = source[x + skip, pl.ds(start + half * h, half), :]
                out = jnp.where(pair == x + nx * h, pltpu.roll(v, (turn_of(x, h) + 1) % LANES, 1), out)
        return out

    def copies(e):
        xc = pltpu.make_async_remote_copy(
            xsend.at[e], xrecv.at[e],
            face_send.at[e, 0], face_recv.at[e, 0], device_id=(ox, iy, iz), device_id_type=MESH)
        yc, zc = [], []
        for up in range(2):
            yc.append(pltpu.make_async_remote_copy(
                ysend.at[e], yrecv.at[e, 1 - up], face_send.at[e, 1 + up], face_recv.at[e, 2 - up],
                device_id=(ix, jnp.clip(iy + 2 * up - 1, 0, gy - 1), iz), device_id_type=MESH))
            zc.append(pltpu.make_async_remote_copy(
                zsend.at[e, up], zrecv.at[e, 1 - up], face_send.at[e, 3 + up], face_recv.at[e, 4 - up],
                device_id=(ix, iy, jnp.clip(iz + 2 * up - 1, 0, gz - 1)), device_id_type=MESH))
        return xc, yc, zc

    def send_z(e):
        _, _, zc = copies(e)
        pl.when(iz > 0)(zc[0].start)
        pl.when(iz < gz - 1)(zc[1].start)

    def send_xy(e):
        xc, yc, _ = copies(e)
        pl.when(iy > 0)(yc[0].start)
        pl.when(iy < gy - 1)(yc[1].start)
        xc.start()

    def fill_z(source, e):
        zsend[e, 0] = source[pl.ds(1, nx), base, :]
        zsend[e, 1] = source[pl.ds(1, nx), base + nz - 1, :]

    def fill_xy(source, e):
        ysend[e] = pack(source)
        xsend[e] = source[border, inner, :]

    def receive_xy(e):
        xc, yc, _ = copies(e)
        xc.wait()
        pl.when(iy > 0)(lambda: (yc[0].wait_send(), yc[1].wait_recv())[0])
        pl.when(iy < gy - 1)(lambda: (yc[1].wait_send(), yc[0].wait_recv())[0])

    def weights():
        return [
            pltpu.make_async_remote_copy(
                wz.at[up], wzn.at[1 - up], wz_send.at[up], wz_recv.at[1 - up],
                device_id=(ix, iy, jnp.clip(iz + 2 * up - 1, 0, gz - 1)), device_id_type=MESH)
            for up in range(2)
        ]

    def receive_z(e):
        _, _, zc = copies(e)
        pl.when(iz > 0)(lambda: (zc[0].wait_send(), zc[1].wait_recv())[0])
        pl.when(iz < gz - 1)(lambda: (zc[1].wait_send(), zc[0].wait_recv())[0])

    gxy = ix * gy + iy
    first = (part1, [(px, py, iz) for px, py in group], gxy, sum1_send, sum1_recv, [px * gy + py for px, py in group])
    second = (part2, [(ix, iy, pz) for pz in line], iz, sum2_send, sum2_recv, line)

    def spread_out(stage, which):
        part, peers, mine, send_sem, recv_sem, _ = stage
        for i, peer in enumerate(peers):
            pltpu.make_async_remote_copy(
                part.at[which, mine], part.at[which, mine], send_sem.at[which, i], recv_sem.at[which, mine],
                device_id=peer, device_id_type=MESH).start()

    def arrivals(stage, which):
        part, peers, _, send_sem, recv_sem, slots = stage
        return [
            pltpu.make_async_remote_copy(
                part.at[which, slot], part.at[which, slot], send_sem.at[which, i], recv_sem.at[which, slot],
                device_id=peers[i], device_id_type=MESH)
            for i, slot in enumerate(slots)
        ]

    def gather_in(stage, which):
        part = stage[0]
        for copy in arrivals(stage, which):
            copy.wait_recv()
        pairs = [(part[which, i], None) for i in range(part.shape[1])]
        while len(pairs) > 1:
            pairs = [joined_sum(*pairs[i:i + 2]) for i in range(0, len(pairs), 2)]
        return pairs[0]

    def sum_begin(which, row):
        part1[which, gxy] = row
        spread_out(first, which)

    def sum_middle(which):
        high, low = renew(*gather_in(first, which))
        part2[which, iz, pl.ds(0, 1), :] = high
        part2[which, iz, pl.ds(1, 1), :] = low
        spread_out(second, which)

    def sum_end(which):
        total, error = gather_in(second, which)
        return renew(total[0:1], error[0:1] + total[1:2])

    def all_lanes(row, m):
        return jnp.broadcast_to(jnp.sum(jnp.where(row_lane == m, row, 0.0), axis=1, keepdims=True), (8, LANES))

    def one_row(values):
        row = jnp.zeros((1, LANES), F32)
        for m, v in enumerate(values):
            row = jnp.where(row_lane == m, jnp.sum(jnp.sum(v, axis=0, keepdims=True), axis=1, keepdims=True), row)
        return row

    wide_lane = lax.broadcasted_iota(jnp.int32, (nz, LANES), 1)
    inside = wide_lane < LANES - 1
    after = wide_lane > 0
    edge = (wide_lane == 0) | (wide_lane == LANES - 1)
    one = jnp.ones((8, LANES), F32)

    face_row = lax.broadcasted_iota(jnp.int32, (nx, LANES), 0)
    face_lane = lax.broadcasted_iota(jnp.int32, (nx, LANES), 1)
    half_row = lax.broadcasted_iota(jnp.int32, (half, LANES), 0)
    slab_row = lax.broadcasted_iota(jnp.int32, (nz, LANES), 0)

    def z_edges(zpart, low_side, high_side, xa):
        faces = []
        for h in range(2):
            at = (half - 1) * h
            face = zpart[h]
            for at_lane, side, shift in ((0, low_side, 0), (LANES - 1, high_side, 1)):
                one_lane = jnp.where(face_lane == 2 * face_row + 2 * nx * h + shift, side[at:at + 1], 0.0)
                face = face + jnp.where(face_lane == at_lane, jnp.sum(one_lane, axis=1, keepdims=True), 0.0)
            at = (nz - 1) * h
            faces.append(face + jnp.where(face_row == border - 1, xa[at:at + 1], 0.0))
        return faces

    def joined(low_side, high_side):
        return jnp.where(even, pltpu.roll(high_side, LANES - 1, 1), pltpu.roll(low_side, 1, 1))

    def xy_faces(xpart, ypart, za, ya, xa):
        yface, xface = ypart + ya, xpart + xa
        xlanes = []
        for h in range(2):
            here = 2 * nx * h + 1
            at = half_row == (half - 1) * h
            moved = jnp.where(face_lane // 2 == face_row + nx * h, pltpu.roll(za[h], here, 1, stride=2, stride_axis=0), 0.0)
            yface = yface + jnp.where(at, jnp.sum(moved, axis=0, keepdims=True), 0.0)
            xa_half = xa[half * h:half * (h + 1)]
            turns = [(2 * (nx - 1) + here) % LANES, here]
            moved = jnp.where(low_x, pltpu.roll(xa_half, turns[0], 1), pltpu.roll(xa_half, turns[1], 1))
            yface = yface + jnp.where(pair == border - 1 + nx * h, moved, 0.0)
            moved = jnp.where(low_x, pltpu.roll(ya, (LANES - turns[0]) % LANES, 1), pltpu.roll(ya, LANES - turns[1], 1))
            xlanes.append(moved)
            z_at = slab_row == (nz - 1) * h
            xface = xface + jnp.where(z_at, jnp.sum(jnp.where(face_row == border - 1, za[h], 0.0), axis=0, keepdims=True), 0.0)
        return xface + jnp.where(edge, jnp.concatenate(xlanes, axis=0), 0.0), yface

    def keep(za, ya, xa):
        yadd[...] = ya
        zadd[0] = za[0]
        zadd[1] = za[1]
        xadd[...] = xa

    def correct(ref, skip=1, start=base):
        ref[pl.ds(skip, nx), start, :] += zadd[0]
        ref[pl.ds(skip, nx), start + nz - 1, :] += zadd[1]
        ref[border - 1 + skip, pl.ds(start, nz), :] += xadd[...]
        terms = yadd[...]
        for x in range(nx):
            for h in range(2):
                turned[x, pl.ds(half * h, half), :] = pltpu.roll(terms, (LANES - turn_of(x, h) - 1) % LANES, 1)

        def add_sides(x, _):
            ref[x + skip, pl.ds(start, nz), :] += jnp.where(edge, turned[x], 0.0)
            return 0

        lax.fori_loop(0, nx, add_sides, 0, unroll=4)

    loads[0].wait()
    loads[2].start()
    pl.semaphore_wait(barrier, len(group) + len(line))
    fill_z(cond, 0)
    send_z(0)
    fill_xy(cond, 0)
    send_xy(0)
    loads[1].wait()

    def means(x, acc):
        return acc[0] + cond[x + 1, inner, :], acc[1] + absorb[x]

    sums = lax.fori_loop(0, nx, means, (zero_slab, zero_slab), unroll=4)
    sum_begin(0, one_row([tile_sum(v) for v in sums]))

    def clear(k, _):
        field[k, 0, inner, :] = zero_slab
        field[k, nx + 1, inner, :] = zero_slab
        field[k, pl.ds(1, nx), base - 1, :] = zero_face
        field[k, pl.ds(1, nx), base + nz, :] = zero_face
        return 0

    lax.fori_loop(0, STEPS, clear, 0)
    table[0, 0] = one
    table[0, 1] = jnp.zeros((8, LANES), F32)
    cond[0, inner, :] = zero_slab
    cond[nx + 1, inner, :] = zero_slab
    cond[pl.ds(1, nx), base - 1, :] = zero_face
    cond[pl.ds(1, nx), base + nz, :] = zero_face
    fx[0] = 0.5 * cond[1, inner, :]

    def coefficients(x, _):
        here = cond[x + 1, inner, :]
        xp = 0.5 * (here + cond[x + 2, inner, :])
        xm = fx[x]
        yp = 0.5 * (here + jnp.where(inside, pltpu.roll(here, LANES - 1, 1), 0.0))
        ym = 0.5 * (here + jnp.where(after, pltpu.roll(here, 1, 1), 0.0))
        zp = 0.5 * (here + cond[x + 1, above, :])
        zm = 0.5 * (here + cond[x + 1, below, :])
        fx[x + 1] = xp
        fy[x] = jnp.where(inside, yp, 0.0)
        fz[x, below, :] = zm
        fz[x, inner, :] = zp
        diag[x] = absorb[x] + xp + xm + yp + ym + zp + zm
        return 0

    lax.fori_loop(0, nx, coefficients, 0, unroll=8)
    loads[2].wait()
    ypart, yright = pack(diag, 0, 0), pack(weight, 0, 0)
    zpart = [diag[pl.ds(0, nx), (nz - 1) * i, :] for i in range(2)]
    zright = [weight[pl.ds(0, nx), (nz - 1) * i, :] for i in range(2)]
    receive_xy(0)
    low_side, high_side = 0.5 * yrecv[0, 0], 0.5 * yrecv[0, 1]
    xa = 0.5 * xrecv[0]
    zpart = z_edges(zpart, low_side, high_side, xa)
    receive_z(0)
    za = [0.5 * zrecv[0, i] for i in range(2)]
    zdiag = [zpart[i] + za[i] for i in range(2)]
    for i in range(2):
        zsend[1, i] = zright[i] / zdiag[i]
    send_z(1)
    ya = joined(low_side, high_side)
    xdiag, ydiag = xy_faces(diag[border - 1], ypart, za, ya, xa)
    xsend[1] = weight[border - 1] / xdiag
    ysend[1] = yright / ydiag
    send_xy(1)
    sum_middle(0)
    for i in range(2):
        wz[i] = (0.5 * zsend[0, i] + za[i]) / zdiag[i]
    down, upward = weights()
    pl.when(iz > 0)(down.start)
    pl.when(iz < gz - 1)(upward.start)
    for i in range(2):
        zterm[i] = zero_face
        zown[0, i] = zsend[1, i]
    wx[...] = (0.5 * xsend[0] + xa) / xdiag
    sides = (0.5 * ysend[0] + ya) / ydiag
    wy[0] = jnp.where(even, pltpu.roll(sides, LANES - 1, 1), 0.0)
    wy[1] = jnp.where(even, 0.0, pltpu.roll(sides, 1, 1))
    dy[...] = ydiag
    keep(za, ya, xa)
    correct(diag, 0, 0)

    def begin(x, _):
        inverse = 1.0 / diag[x]
        field[0, x + 1, inner, :] = weight[x] * inverse
        weight[x] = inverse
        return 0

    lax.fori_loop(0, nx, begin, 0, unroll=8)
    keep([zero_face, zero_face], jnp.zeros((half, LANES), F32), zero_slab)

    def step(k, _):
        src, dst, old = k, k + 1, jnp.maximum(k - 1, 0)
        e = k + 1

        @pl.when(k == 1)
        def _():
            high, _ = sum_end(0)
            six = 6.0 * all_lanes(high, 0)
            rho = 0.97 * six / (six + all_lanes(high, 1))
            kappa = jnp.floor(64.0 * (2.0 / rho)) * (1.0 / 64.0)
            half_kappa = 0.5 * kappa
            table[1, 0] = kappa * half_kappa
            table[1, 1] = one
            table[2, 0] = kappa
            table[2, 1] = half_kappa
            for j in range(3, STEPS):
                table[j, 0] = kappa
                table[j, 1] = one

        @pl.when(k == 1)
        def _():
            down, upward = weights()
            pl.when(iz > 0)(lambda: (down.wait_send(), upward.wait_recv())[0])
            pl.when(iz < gz - 1)(lambda: (upward.wait_send(), down.wait_recv())[0])

        @pl.when(k > 0)
        def _():
            before = spread(table[k - 1, 0], half)
            for i in range(2):
                zterm[i] = before * wzn[i] * zown[k - 1, i]

        pl.when(k > 0)(lambda: correct(field.at[k]))
        a = table[k, 0]
        a_all, b_all = spread(a), spread(table[k, 1])

        def row(x, acc):
            same, older, ahead = acc
            v = field[src, x + 1, inner, :]
            y = fy[x]
            o = field[old, x + 1, inner, :]
            s = fx[x + 1] * field[src, x + 2, inner, :] + fx[x] * field[src, x, inner, :]
            s = s + fz[x, inner, :] * field[src, x + 1, above, :] + fz[x, below, :] * field[src, x + 1, below, :]
            s = s + y * pltpu.roll(v, LANES - 1, 1) + pltpu.roll(y * v, 1, 1)
            new = a_all * (weight[x] * s) - b_all * o
            field[dst, x + 1, inner, :] = new
            w = diag[x] * v
            return same + w * v, older + w * o, ahead + w * new

        same, older, ahead = lax.fori_loop(0, nx, row, (zero_slab, zero_slab, zero_slab), unroll=8)
        dots[2 * k] = tile_sum(same)
        dots[2 * k + 1] = tile_sum(older)
        dots[2 * STEPS] = tile_sum(ahead)

        @pl.when(k == STEPS - 1)
        def _():
            sum_begin(1, one_row([dots[m if m % 2 == 0 else m + 2] for m in range(2 * STEPS - 1)]))


        ypart = pack(field.at[dst])
        zpart = [field[dst, pl.ds(1, nx), base + row_, :] for row_ in (0, nz - 1)]
        xpart = field[dst, border, inner, :]

        a_half = spread(a, half)
        receive_xy(e)
        low_side = a_half * wy[0] * yrecv[e, 0]
        high_side = a_half * wy[1] * yrecv[e, 1]
        xa = a_all * wx[...] * xrecv[e]
        zpart = z_edges(zpart, low_side, high_side, xa)

        @pl.when(k < STEPS - 1)
        def _():
            for i in range(2):
                zsend[e + 1, i] = zpart[i]
            send_z(e + 1)

        zscale = [a_half * wz[i] for i in range(2)]
        receive_z(e)
        za = [zscale[i] * (zrecv[e, i] + zterm[i]) for i in range(2)]
        for i in range(2):
            zown[k + 1, i] = zpart[i] + za[i]
        ya = joined(low_side, high_side)
        keep(za, ya, xa)

        @pl.when(k < STEPS - 1)
        def _():
            xsend[e + 1], ysend[e + 1] = xy_faces(xpart, ypart, za, ya, xa)
            send_xy(e + 1)

        return 0

    lax.fori_loop(0, STEPS, step, 0)
    last = dots[2 * STEPS] + tile_sum(xadd[...] * diag[border - 1] * xsend[STEPS])
    faces = yadd[...] * dy[...] * ysend[STEPS]
    for i in range(2):
        faces = faces + zadd[i] * diag[pl.ds(0, nx), (nz - 1) * i, :] * zown[STEPS - 1, i]
    sum_begin(2, one_row([last + jnp.sum(faces.reshape(half // 8, 8, LANES), axis=0)]))
    correct(field.at[STEPS])
    sum_middle(1)
    sum_middle(2)
    high, low = sum_end(1)
    kappa = table[2, 0]
    half_kappa = table[2, 1]
    raw = [(all_lanes(high, m), all_lanes(low, m)) for m in range(2 * STEPS - 1)]
    exact = (half_kappa, jnp.zeros((8, LANES), F32))
    raw[1] = dmul(raw[1], exact)
    raw[2] = dmul(dmul(raw[2], exact), exact)
    raw[3] = dmul(raw[3], exact)
    mu = raw[:2]
    for m in range(2, 2 * STEPS - 1):
        mu.append(dadd(dtimes(raw[m], 2.0), dneg(mu[m % 2])))
    alpha, beta, end, pivot, ratio = jacobi_matrix(mu)
    u, v, xu, xv, at_u, at_v = solution_polynomials(alpha, beta, kappa, one)
    for p in (u, v, xu, xv):
        p[1] = p[1] * half_kappa
    end = dadd(end, dtimes(mu[1], -(2.0 ** (2 - 2 * STEPS))))
    high, low = sum_end(2)
    end = dadd(end, dtimes((all_lanes(high, 0), all_lanes(low, 0)), 2.0 ** (3 - 2 * STEPS)))
    end = dadd(ddiv(end, pivot), dneg(ratio))[0]
    scale = one / (at_u - end * at_v)
    xs = [scale * (p - end * q) for p, q in zip(xu, xv)]
    rs = [scale * (p - end * q) for p, q in zip(u, v)]
    for k, v in enumerate(xs):
        coef[k] = v
    for k, v in enumerate(rs):
        coef[16 + k] = v
    for which in range(3):
        for stage in (first, second):
            for copy in arrivals(stage, which):
                copy.wait_send()


def finish(nx, nz, groups, field, diag, coef, x_hbm, r_hbm, xs, rs, sems):
    inner = pl.ds(BASE, nz)
    size = nx // groups

    def spread(c):
        return jnp.broadcast_to(c[None], (nz // 8, 8, LANES)).reshape(nz, LANES)

    def slab(x, _):
        v = field[0, x + 1, inner, :]
        sx = spread(coef[0]) * v
        sr = spread(coef[16]) * v
        for k in range(1, STEPS + 1):
            v = field[k, x + 1, inner, :]
            if k < STEPS:
                sx = sx + spread(coef[k]) * v
            sr = sr + spread(coef[16 + k]) * v
        xs[x] = sx
        rs[x] = diag[x] * sr
        return 0

    copies = []
    for g in range(groups):
        lax.fori_loop(g * size, (g + 1) * size, slab, 0, unroll=4)
        part = pl.ds(g * size, size)
        for n, (src, dst) in enumerate(((xs, x_hbm), (rs, r_hbm))):
            copy = pltpu.make_async_copy(src.at[part], dst.at[part], sems.at[n, g])
            copy.start()
            copies.append(copy)
    for copy in copies:
        copy.wait()


def solution(mesh):
    gx, gy, gz = mesh.shape["gx"], mesh.shape["gy"], mesh.shape["gz"]

    def on_device(right_side, conductivity, absorption):
        nx, ny, nz = right_side.shape
        assert ny == LANES and nx * 2 * 2 == LANES and gx == 2
        args = [jnp.transpose(v, (0, 2, 1)) for v in (right_side, conductivity, absorption)]
        block = (nx, nz, LANES)
        exchanges = STEPS + 1
        dma = pltpu.SemaphoreType.DMA
        tall = nz + 16
        field = (STEPS + 1, nx + 2, tall, LANES)
        vmem = pl.BlockSpec(memory_space=pltpu.VMEM)
        kept = pl.pallas_call(
            functools.partial(kernel, nx, nz, (gx, gy, gz)),
            out_shape=[pltpu.VMEM(field, F32), pltpu.VMEM(block, F32), pltpu.VMEM((32, 8, LANES), F32)],
            in_specs=[pl.BlockSpec(memory_space=pl.ANY)] * 3,
            out_specs=[vmem] * 3,
            scratch_shapes=[
                pltpu.VMEM((nx + 2, tall, LANES), F32),
                pltpu.VMEM(block, F32),
                pltpu.VMEM(block, F32),
                pltpu.VMEM((nx + 1, nz, LANES), F32),
                pltpu.VMEM(block, F32),
                pltpu.VMEM((nx, tall, LANES), F32),
                pltpu.VMEM(block, F32),
                pltpu.VMEM((nz, LANES), F32),
                pltpu.VMEM((2, nz // 2, LANES), F32),
                pltpu.VMEM((nz // 2, LANES), F32),
                pltpu.VMEM((2, nx, LANES), F32),
                pltpu.VMEM((2, nx, LANES), F32),
                pltpu.VMEM((2, nx, LANES), F32),
                pltpu.VMEM((STEPS + 1, 2, nx, LANES), F32),
                pltpu.VMEM((nz, LANES), F32),
                pltpu.VMEM((nz // 2, LANES), F32),
                pltpu.VMEM((2, nx, LANES), F32),
                pltpu.VMEM((exchanges, nz, LANES), F32),
                pltpu.VMEM((exchanges, 2, nx, LANES), F32),
                pltpu.VMEM((exchanges, 2, nx, LANES), F32),
                pltpu.VMEM((exchanges, nz // 2, LANES), F32),
                pltpu.VMEM((exchanges, 2, nz // 2, LANES), F32),
                pltpu.VMEM((exchanges, nz, LANES), F32),
                pltpu.VMEM((3, gx * gy, 1, LANES), F32),
                pltpu.VMEM((3, gz, 2, LANES), F32),
                pltpu.VMEM((2 * STEPS + 2, 8, LANES), F32),
                pltpu.VMEM((STEPS, 2, 8, LANES), F32),
                dma((3,)),
                dma((exchanges, 5)),
                dma((exchanges, 5)),
                dma((2,)),
                dma((2,)),
                dma((3, gx * gy)),
                dma((3, gx * gy)),
                dma((3, gz)),
                dma((3, gz)),
            ],
            compiler_params=pltpu.CompilerParams(
                collective_id=0, has_side_effects=True, vmem_limit_bytes=40 * 1024 * 1024
            ),
        )(*[pltpu.with_memory_space_constraint(v, pltpu.HBM) for v in args])
        groups = 4
        out = pl.pallas_call(
            functools.partial(finish, nx, nz, groups),
            out_shape=[jax.ShapeDtypeStruct(block, F32)] * 2,
            in_specs=[vmem] * 3,
            out_specs=[pl.BlockSpec(memory_space=pltpu.HBM)] * 2,
            scratch_shapes=[pltpu.VMEM(block, F32), pltpu.VMEM(block, F32), dma((2, groups))],
            compiler_params=pltpu.CompilerParams(vmem_limit_bytes=20 * 1024 * 1024),
        )(*kept)
        return tuple(jnp.transpose(v, (0, 2, 1)) for v in out)

    spec = P("gx", "gy", "gz")
    return jax.shard_map(on_device, mesh=mesh, in_specs=(spec,) * 3, out_specs=(spec,) * 2, check_vma=False)
```

```python
import functools

import jax
import jax.numpy as jnp
from jax import lax
from jax.experimental import pallas as pl
from jax.experimental.pallas import tpu as pltpu
from jax.sharding import PartitionSpec as P

F32 = jnp.float32
MESH = pl.DeviceIdType.MESH
STEPS = 10
LANES = 128
BASE = 8


def two_sum(a, b):
    s = a + b
    t = s - a
    return s, (a - (s - t)) + (b - t)


def joined_sum(a, b):
    s, e = two_sum(a[0], b[0])
    return s, e if a[1] is None else e + (a[1] + b[1])


def renew(a, b):
    s = a + b
    return s, b - (s - a)


def halves(a):
    t = 4097.0 * a
    high = t - (t - a)
    return high, a - high


def two_product(a, b):
    p = a * b
    ah, al = halves(a)
    bh, bl = halves(b)
    return p, ((ah * bh - p) + ah * bl + al * bh) + al * bl


def dadd(a, b):
    s, e = two_sum(a[0], b[0])
    return renew(s, e + (a[1] + b[1]))


def dneg(a):
    return -a[0], -a[1]


def dmul(a, b):
    p, e = two_product(a[0], b[0])
    return renew(p, e + (a[0] * b[1] + a[1] * b[0]))


def dtimes(a, power):
    return power * a[0], power * a[1]


def ddiv(a, b):
    q = a[0] / b[0]
    p, e = two_product(q, b[0])
    rest = ((a[0] - p) - e) + (a[1] - q * b[1])
    return renew(q, rest / b[0])


def jacobi_matrix(mu):
    n = (len(mu) + 1) // 2
    zero = (0.0 * mu[0][0], 0.0 * mu[0][0])
    cur = [mu[0]] + [dtimes(mu[k], 2.0 ** (1 - k)) for k in range(1, 2 * n - 1)] + [zero]
    prev = None
    ratio = ddiv(cur[1], cur[0])
    alpha, beta = [ratio], [None]
    for k in range(1, n):
        new = [None] * (2 * n)
        minus_alpha = dneg(alpha[-1])
        minus_beta = None if k == 1 else dneg(beta[-1])
        for l in range(k, 2 * n - k):
            v = dadd(cur[l + 1], dmul(minus_alpha, cur[l]))
            if prev is not None:
                v = dadd(v, dmul(minus_beta, prev[l]))
            new[l] = dadd(v, dtimes(cur[l - 1], 0.5 if l == 1 else 0.25))
        beta.append(ddiv(new[k], cur[k - 1]))
        prev, cur = cur, new
        if k < n - 1:
            later = ddiv(new[k + 1], new[k])
            alpha.append(dadd(later, dneg(ratio)))
            ratio = later
    high = [a[0] for a in alpha], [None if b is None else b[0] for b in beta]
    return high[0], high[1], cur[n], cur[n - 1], ratio


def without_pole(p, kappa):
    n = len(p) - 1
    q = [None] * (n + 2)
    q[n] = q[n + 1] = 0.0 * kappa
    for k in range(n, 1, -1):
        q[k - 1] = (q[k] + p[k]) * kappa - q[k + 1]
    q[0] = (q[1] + p[1]) * (0.5 * kappa) - 0.5 * q[2]
    return q[:n]


def solution_polynomials(alpha, beta, kappa, one):
    n = len(beta)
    tau = 0.5 * kappa
    at = [one, tau - alpha[0]]
    for k in range(1, n - 1):
        at.append((tau - alpha[k]) * at[-1] - beta[k] * at[-2])
    before, p = None, [one]
    for k in range(n):
        new = [None] * (k + 2)

        def put(i, v):
            new[i] = v if new[i] is None else new[i] + v

        for i, v in enumerate(p):
            half = 0.5 * v
            put(i + 1, half)
            put(abs(i - 1), half)
        if k < n - 1:
            for i, v in enumerate(p):
                put(i, -(alpha[k] * v))
        if before is not None:
            for i, v in enumerate(before):
                put(i, -(beta[k] * v))
        before, p = p, new
    v = before + [0.0 * one]
    at_u = tau * at[-1] - beta[n - 1] * at[-2]
    return p, v, without_pole(p, kappa), without_pole(v, kappa), at_u, at[-1]


def kernel(nx, nz, sizes, r_hbm, c_hbm, a_hbm, field, diag, coef,
           cond, absorb, weight, fx, fy, fz, turned, wx, wy, dy, wz, wzn, zterm, zown, xadd, yadd, zadd, xsend, zsend, zrecv, ysend, yrecv, xrecv,
           part1, part2, dots, table,
           load_sem, face_send, face_recv, wz_send, wz_recv, sum1_send, sum1_recv, sum2_send, sum2_recv):
    gx, gy, gz = sizes
    ix, iy, iz = lax.axis_index("gx"), lax.axis_index("gy"), lax.axis_index("gz")
    ox = 1 - ix
    base = BASE
    inner = pl.ds(base, nz)
    above = pl.ds(base + 1, nz)
    below = pl.ds(base - 1, nz)
    half = nz // 2
    tiles = nz // 8
    low_x = ix == 0
    border = jnp.where(low_x, nx, 1)

    loads = [
        pltpu.make_async_copy(c_hbm, cond.at[pl.ds(1, nx), inner, :], load_sem.at[0]),
        pltpu.make_async_copy(a_hbm, absorb, load_sem.at[1]),
        pltpu.make_async_copy(r_hbm, weight, load_sem.at[2]),
    ]
    loads[0].start()
    loads[1].start()

    zero_face = jnp.zeros((nx, LANES), F32)
    zero_slab = jnp.zeros((nz, LANES), F32)

    barrier = pltpu.get_barrier_semaphore()
    group = [((ix + dx) % gx, (iy + dy) % gy) for dx in range(gx) for dy in range(gy) if (dx, dy) != (0, 0)]
    line = [(iz + d) % gz for d in range(1, gz)]
    for px, py in group:
        pl.semaphore_signal(barrier, inc=1, device_id=(px, py, iz), device_id_type=MESH)
    for pz in line:
        pl.semaphore_signal(barrier, inc=1, device_id=(ix, iy, pz), device_id_type=MESH)

    for ref, side, alone in ((zrecv, 0, iz == 0), (zrecv, 1, iz == gz - 1), (yrecv, 0, iy == 0), (yrecv, 1, iy == gy - 1)):

        @pl.when(alone)
        def _(ref=ref, side=side):
            def clear_faces(k, _):
                ref[k, side] = zero_face
                return 0

            lax.fori_loop(0, STEPS + 1, clear_faces, 0)
            if ref is zrecv:
                wzn[side] = zero_face

    lane = lax.broadcasted_iota(jnp.int32, (half, LANES), 1)
    pair = lane // 2
    even = (lane % 2) == 0
    row_lane = lax.broadcasted_iota(jnp.int32, (1, LANES), 1)

    def tile_sum(v):
        return jnp.sum(v.reshape(tiles, 8, LANES), axis=0)

    def spread(c, rows=nz):
        return jnp.broadcast_to(c[None], (rows // 8, 8, LANES)).reshape(rows, LANES)

    def turn_of(x, h):
        return 2 * x + 2 * nx * h

    def pack(source, skip=1, start=base):
        out = jnp.zeros((half, LANES), F32)
        for x in range(nx):
            for h in range(2):
                v = source[x + skip, pl.ds(start + half * h, half), :]
                out = jnp.where(pair == x + nx * h, pltpu.roll(v, (turn_of(x, h) + 1) % LANES, 1), out)
        return out

    def copies(e):
        xc = pltpu.make_async_remote_copy(
            xsend.at[e], xrecv.at[e],
            face_send.at[e, 0], face_recv.at[e, 0], device_id=(ox, iy, iz), device_id_type=MESH)
        yc, zc = [], []
        for up in range(2):
            yc.append(pltpu.make_async_remote_copy(
                ysend.at[e], yrecv.at[e, 1 - up], face_send.at[e, 1 + up], face_recv.at[e, 2 - up],
                device_id=(ix, jnp.clip(iy + 2 * up - 1, 0, gy - 1), iz), device_id_type=MESH))
            zc.append(pltpu.make_async_remote_copy(
                zsend.at[e, up], zrecv.at[e, 1 - up], face_send.at[e, 3 + up], face_recv.at[e, 4 - up],
                device_id=(ix, iy, jnp.clip(iz + 2 * up - 1, 0, gz - 1)), device_id_type=MESH))
        return xc, yc, zc

    def send_z(e):
        _, _, zc = copies(e)
        pl.when(iz > 0)(zc[0].start)
        pl.when(iz < gz - 1)(zc[1].start)

    def send_xy(e):
        xc, yc, _ = copies(e)
        pl.when(iy > 0)(yc[0].start)
        pl.when(iy < gy - 1)(yc[1].start)
        xc.start()

    def fill_z(source, e):
        zsend[e, 0] = source[pl.ds(1, nx), base, :]
        zsend[e, 1] = source[pl.ds(1, nx), base + nz - 1, :]

    def fill_xy(source, e):
        ysend[e] = pack(source)
        xsend[e] = source[border, inner, :]

    def receive_xy(e):
        xc, yc, _ = copies(e)
        xc.wait()
        pl.when(iy > 0)(lambda: (yc[0].wait_send(), yc[1].wait_recv())[0])
        pl.when(iy < gy - 1)(lambda: (yc[1].wait_send(), yc[0].wait_recv())[0])

    def weights():
        return [
            pltpu.make_async_remote_copy(
                wz.at[up], wzn.at[1 - up], wz_send.at[up], wz_recv.at[1 - up],
                device_id=(ix, iy, jnp.clip(iz + 2 * up - 1, 0, gz - 1)), device_id_type=MESH)
            for up in range(2)
        ]

    def receive_z(e):
        _, _, zc = copies(e)
        pl.when(iz > 0)(lambda: (zc[0].wait_send(), zc[1].wait_recv())[0])
        pl.when(iz < gz - 1)(lambda: (zc[1].wait_send(), zc[0].wait_recv())[0])

    gxy = ix * gy + iy
    first = (part1, [(px, py, iz) for px, py in group], gxy, sum1_send, sum1_recv, [px * gy + py for px, py in group])
    second = (part2, [(ix, iy, pz) for pz in line], iz, sum2_send, sum2_recv, line)

    def spread_out(stage, which):
        part, peers, mine, send_sem, recv_sem, _ = stage
        for i, peer in enumerate(peers):
            pltpu.make_async_remote_copy(
                part.at[which, mine], part.at[which, mine], send_sem.at[which, i], recv_sem.at[which, mine],
                device_id=peer, device_id_type=MESH).start()

    def arrivals(stage, which):
        part, peers, _, send_sem, recv_sem, slots = stage
        return [
            pltpu.make_async_remote_copy(
                part.at[which, slot], part.at[which, slot], send_sem.at[which, i], recv_sem.at[which, slot],
                device_id=peers[i], device_id_type=MESH)
            for i, slot in enumerate(slots)
        ]

    def gather_in(stage, which):
        part = stage[0]
        for copy in arrivals(stage, which):
            copy.wait_recv()
        pairs = [(part[which, i], None) for i in range(part.shape[1])]
        while len(pairs) > 1:
            pairs = [joined_sum(*pairs[i:i + 2]) for i in range(0, len(pairs), 2)]
        return pairs[0]

    def sum_begin(which, row):
        part1[which, gxy] = row
        spread_out(first, which)

    def sum_middle(which):
        high, low = renew(*gather_in(first, which))
        part2[which, iz, pl.ds(0, 1), :] = high
        part2[which, iz, pl.ds(1, 1), :] = low
        spread_out(second, which)

    def sum_end(which):
        total, error = gather_in(second, which)
        return renew(total[0:1], error[0:1] + total[1:2])

    def all_lanes(row, m):
        return jnp.broadcast_to(jnp.sum(jnp.where(row_lane == m, row, 0.0), axis=1, keepdims=True), (8, LANES))

    def one_row(values):
        row = jnp.zeros((1, LANES), F32)
        for m, v in enumerate(values):
            row = jnp.where(row_lane == m, jnp.sum(jnp.sum(v, axis=0, keepdims=True), axis=1, keepdims=True), row)
        return row

    wide_lane = lax.broadcasted_iota(jnp.int32, (nz, LANES), 1)
    inside = wide_lane < LANES - 1
    after = wide_lane > 0
    edge = (wide_lane == 0) | (wide_lane == LANES - 1)
    one = jnp.ones((8, LANES), F32)

    face_row = lax.broadcasted_iota(jnp.int32, (nx, LANES), 0)
    face_lane = lax.broadcasted_iota(jnp.int32, (nx, LANES), 1)
    half_row = lax.broadcasted_iota(jnp.int32, (half, LANES), 0)
    slab_row = lax.broadcasted_iota(jnp.int32, (nz, LANES), 0)

    def z_edges(zpart, low_side, high_side, xa):
        faces = []
        for h in range(2):
            at = (half - 1) * h
            face = zpart[h]
            for at_lane, side, shift in ((0, low_side, 0), (LANES - 1, high_side, 1)):
                one_lane = jnp.where(face_lane == 2 * face_row + 2 * nx * h + shift, side[at:at + 1], 0.0)
                face = face + jnp.where(face_lane == at_lane, jnp.sum(one_lane, axis=1, keepdims=True), 0.0)
            at = (nz - 1) * h
            faces.append(face + jnp.where(face_row == border - 1, xa[at:at + 1], 0.0))
        return faces

    def joined(low_side, high_side):
        return jnp.where(even, pltpu.roll(high_side, LANES - 1, 1), pltpu.roll(low_side, 1, 1))

    def xy_begun(xpart, ypart, ya, xa):
        yface, xlanes = ypart + ya, []
        for h in range(2):
            here = 2 * nx * h + 1
            xa_half = xa[half * h:half * (h + 1)]
            turns = [(2 * (nx - 1) + here) % LANES, here]
            moved = jnp.where(low_x, pltpu.roll(xa_half, turns[0], 1), pltpu.roll(xa_half, turns[1], 1))
            yface = yface + jnp.where(pair == border - 1 + nx * h, moved, 0.0)
            moved = jnp.where(low_x, pltpu.roll(ya, (LANES - turns[0]) % LANES, 1), pltpu.roll(ya, LANES - turns[1], 1))
            xlanes.append(moved)
        return xpart + xa + jnp.where(edge, jnp.concatenate(xlanes, axis=0), 0.0), yface

    def xy_ended(xface, yface, za):
        for h in range(2):
            at = half_row == (half - 1) * h
            moved = jnp.where(face_lane // 2 == face_row + nx * h, pltpu.roll(za[h], 2 * nx * h + 1, 1, stride=2, stride_axis=0), 0.0)
            yface = yface + jnp.where(at, jnp.sum(moved, axis=0, keepdims=True), 0.0)
            z_at = slab_row == (nz - 1) * h
            xface = xface + jnp.where(z_at, jnp.sum(jnp.where(face_row == border - 1, za[h], 0.0), axis=0, keepdims=True), 0.0)
        return xface, yface

    def keep(za, ya, xa):
        yadd[...] = ya
        zadd[0] = za[0]
        zadd[1] = za[1]
        xadd[...] = xa

    def correct(ref, skip=1, start=base):
        ref[pl.ds(skip, nx), start, :] += zadd[0]
        ref[pl.ds(skip, nx), start + nz - 1, :] += zadd[1]
        ref[border - 1 + skip, pl.ds(start, nz), :] += xadd[...]
        terms = yadd[...]
        for x in range(nx):
            for h in range(2):
                turned[x, pl.ds(half * h, half), :] = pltpu.roll(terms, (LANES - turn_of(x, h) - 1) % LANES, 1)

        def add_sides(x, _):
            ref[x + skip, pl.ds(start, nz), :] += jnp.where(edge, turned[x], 0.0)
            return 0

        lax.fori_loop(0, nx, add_sides, 0, unroll=4)

    loads[0].wait()
    loads[2].start()
    pl.semaphore_wait(barrier, len(group) + len(line))
    fill_z(cond, 0)
    send_z(0)
    fill_xy(cond, 0)
    send_xy(0)
    loads[1].wait()

    def means(x, acc):
        return acc[0] + cond[x + 1, inner, :], acc[1] + absorb[x]

    sums = lax.fori_loop(0, nx, means, (zero_slab, zero_slab), unroll=4)
    sum_begin(0, one_row([tile_sum(v) for v in sums]))

    def clear(k, _):
        field[k, 0, inner, :] = zero_slab
        field[k, nx + 1, inner, :] = zero_slab
        field[k, pl.ds(1, nx), base - 1, :] = zero_face
        field[k, pl.ds(1, nx), base + nz, :] = zero_face
        return 0

    lax.fori_loop(0, STEPS, clear, 0)
    table[0, 0] = one
    table[0, 1] = jnp.zeros((8, LANES), F32)
    cond[0, inner, :] = zero_slab
    cond[nx + 1, inner, :] = zero_slab
    cond[pl.ds(1, nx), base - 1, :] = zero_face
    cond[pl.ds(1, nx), base + nz, :] = zero_face
    fx[0] = 0.5 * cond[1, inner, :]

    def coefficients(x, _):
        here = cond[x + 1, inner, :]
        xp = 0.5 * (here + cond[x + 2, inner, :])
        xm = fx[x]
        yp = 0.5 * (here + jnp.where(inside, pltpu.roll(here, LANES - 1, 1), 0.0))
        ym = 0.5 * (here + jnp.where(after, pltpu.roll(here, 1, 1), 0.0))
        zp = 0.5 * (here + cond[x + 1, above, :])
        zm = 0.5 * (here + cond[x + 1, below, :])
        fx[x + 1] = xp
        fy[x] = jnp.where(inside, yp, 0.0)
        fz[x, below, :] = zm
        fz[x, inner, :] = zp
        diag[x] = absorb[x] + xp + xm + yp + ym + zp + zm
        return 0

    lax.fori_loop(0, nx, coefficients, 0, unroll=8)
    loads[2].wait()
    ypart, yright = pack(diag, 0, 0), pack(weight, 0, 0)
    zpart = [diag[pl.ds(0, nx), (nz - 1) * i, :] for i in range(2)]
    zright = [weight[pl.ds(0, nx), (nz - 1) * i, :] for i in range(2)]
    receive_xy(0)
    low_side, high_side = 0.5 * yrecv[0, 0], 0.5 * yrecv[0, 1]
    xa = 0.5 * xrecv[0]
    zpart = z_edges(zpart, low_side, high_side, xa)
    receive_z(0)
    za = [0.5 * zrecv[0, i] for i in range(2)]
    zdiag = [zpart[i] + za[i] for i in range(2)]
    for i in range(2):
        zsend[1, i] = zright[i] / zdiag[i]
    send_z(1)
    ya = joined(low_side, high_side)
    xdiag, ydiag = xy_ended(*xy_begun(diag[border - 1], ypart, ya, xa), za)
    xsend[1] = weight[border - 1] / xdiag
    ysend[1] = yright / ydiag
    send_xy(1)
    sum_middle(0)
    for i in range(2):
        wz[i] = (0.5 * zsend[0, i] + za[i]) / zdiag[i]
    down, upward = weights()
    pl.when(iz > 0)(down.start)
    pl.when(iz < gz - 1)(upward.start)
    for i in range(2):
        zterm[i] = zero_face
        zown[0, i] = zsend[1, i]
    wx[...] = (0.5 * xsend[0] + xa) / xdiag
    sides = (0.5 * ysend[0] + ya) / ydiag
    wy[0] = jnp.where(even, pltpu.roll(sides, LANES - 1, 1), 0.0)
    wy[1] = jnp.where(even, 0.0, pltpu.roll(sides, 1, 1))
    dy[...] = ydiag
    keep(za, ya, xa)
    correct(diag, 0, 0)

    def begin(x, _):
        inverse = 1.0 / diag[x]
        field[0, x + 1, inner, :] = weight[x] * inverse
        weight[x] = inverse
        return 0

    lax.fori_loop(0, nx, begin, 0, unroll=8)
    keep([zero_face, zero_face], jnp.zeros((half, LANES), F32), zero_slab)

    def step(k, _):
        src, dst, old = k, k + 1, jnp.maximum(k - 1, 0)
        e = k + 1

        @pl.when(k == 1)
        def _():
            high, _ = sum_end(0)
            six = 6.0 * all_lanes(high, 0)
            rho = 0.97 * six / (six + all_lanes(high, 1))
            kappa = jnp.floor(64.0 * (2.0 / rho)) * (1.0 / 64.0)
            half_kappa = 0.5 * kappa
            table[1, 0] = kappa * half_kappa
            table[1, 1] = one
            table[2, 0] = kappa
            table[2, 1] = half_kappa
            for j in range(3, STEPS):
                table[j, 0] = kappa
                table[j, 1] = one

        @pl.when(k == 1)
        def _():
            down, upward = weights()
            pl.when(iz > 0)(lambda: (down.wait_send(), upward.wait_recv())[0])
            pl.when(iz < gz - 1)(lambda: (upward.wait_send(), down.wait_recv())[0])

        @pl.when(k > 0)
        def _():
            before = spread(table[k - 1, 0], half)
            for i in range(2):
                zterm[i] = before * wzn[i] * zown[k - 1, i]

        pl.when(k > 0)(lambda: correct(field.at[k]))
        a = table[k, 0]
        a_all, b_all = spread(a), spread(table[k, 1])

        def row(x, acc):
            same, older, ahead = acc
            v = field[src, x + 1, inner, :]
            y = fy[x]
            o = field[old, x + 1, inner, :]
            s = fx[x + 1] * field[src, x + 2, inner, :] + fx[x] * field[src, x, inner, :]
            s = s + fz[x, inner, :] * field[src, x + 1, above, :] + fz[x, below, :] * field[src, x + 1, below, :]
            s = s + y * pltpu.roll(v, LANES - 1, 1) + pltpu.roll(y * v, 1, 1)
            new = a_all * (weight[x] * s) - b_all * o
            field[dst, x + 1, inner, :] = new
            w = diag[x] * v
            return same + w * v, older + w * o, ahead + w * new

        same, older, ahead = lax.fori_loop(0, nx, row, (zero_slab, zero_slab, zero_slab), unroll=8)
        dots[2 * k] = tile_sum(same)
        dots[2 * k + 1] = tile_sum(older)
        dots[2 * STEPS] = tile_sum(ahead)

        @pl.when(k == STEPS - 1)
        def _():
            sum_begin(1, one_row([dots[m if m % 2 == 0 else m + 2] for m in range(2 * STEPS - 1)]))


        ypart = pack(field.at[dst])
        zpart = [field[dst, pl.ds(1, nx), base + row_, :] for row_ in (0, nz - 1)]
        xpart = field[dst, border, inner, :]

        a_half = spread(a, half)
        receive_xy(e)
        low_side = a_half * wy[0] * yrecv[e, 0]
        high_side = a_half * wy[1] * yrecv[e, 1]
        xa = a_all * wx[...] * xrecv[e]
        zpart = z_edges(zpart, low_side, high_side, xa)

        @pl.when(k < STEPS - 1)
        def _():
            for i in range(2):
                zsend[e + 1, i] = zpart[i]
            send_z(e + 1)

        ya = joined(low_side, high_side)
        xface, yface = xy_begun(xpart, ypart, ya, xa)
        zscale = [a_half * wz[i] for i in range(2)]
        receive_z(e)
        za = [zscale[i] * (zrecv[e, i] + zterm[i]) for i in range(2)]

        @pl.when(k < STEPS - 1)
        def _():
            xsend[e + 1], ysend[e + 1] = xy_ended(xface, yface, za)
            send_xy(e + 1)

        for i in range(2):
            zown[k + 1, i] = zpart[i] + za[i]
        keep(za, ya, xa)
        return 0

    lax.fori_loop(0, STEPS, step, 0)
    last = dots[2 * STEPS] + tile_sum(xadd[...] * diag[border - 1] * xsend[STEPS])
    faces = yadd[...] * dy[...] * ysend[STEPS]
    for i in range(2):
        faces = faces + zadd[i] * diag[pl.ds(0, nx), (nz - 1) * i, :] * zown[STEPS - 1, i]
    sum_begin(2, one_row([last + jnp.sum(faces.reshape(half // 8, 8, LANES), axis=0)]))
    correct(field.at[STEPS])
    sum_middle(1)
    sum_middle(2)
    high, low = sum_end(1)
    kappa = table[2, 0]
    half_kappa = table[2, 1]
    raw = [(all_lanes(high, m), all_lanes(low, m)) for m in range(2 * STEPS - 1)]
    exact = (half_kappa, jnp.zeros((8, LANES), F32))
    raw[1] = dmul(raw[1], exact)
    raw[2] = dmul(dmul(raw[2], exact), exact)
    raw[3] = dmul(raw[3], exact)
    mu = raw[:2]
    for m in range(2, 2 * STEPS - 1):
        mu.append(dadd(dtimes(raw[m], 2.0), dneg(mu[m % 2])))
    alpha, beta, end, pivot, ratio = jacobi_matrix(mu)
    u, v, xu, xv, at_u, at_v = solution_polynomials(alpha, beta, kappa, one)
    for p in (u, v, xu, xv):
        p[1] = p[1] * half_kappa
    end = dadd(end, dtimes(mu[1], -(2.0 ** (2 - 2 * STEPS))))
    high, low = sum_end(2)
    end = dadd(end, dtimes((all_lanes(high, 0), all_lanes(low, 0)), 2.0 ** (3 - 2 * STEPS)))
    end = dadd(ddiv(end, pivot), dneg(ratio))[0]
    scale = one / (at_u - end * at_v)
    xs = [scale * (p - end * q) for p, q in zip(xu, xv)]
    rs = [scale * (p - end * q) for p, q in zip(u, v)]
    for k, v in enumerate(xs):
        coef[k] = v
    for k, v in enumerate(rs):
        coef[16 + k] = v
    for which in range(3):
        for stage in (first, second):
            for copy in arrivals(stage, which):
                copy.wait_send()


def finish(nx, nz, groups, field, diag, coef, x_hbm, r_hbm, xs, rs, sems):
    inner = pl.ds(BASE, nz)
    size = nx // groups

    def spread(c):
        return jnp.broadcast_to(c[None], (nz // 8, 8, LANES)).reshape(nz, LANES)

    def slab(x, _):
        v = field[0, x + 1, inner, :]
        sx = spread(coef[0]) * v
        sr = spread(coef[16]) * v
        for k in range(1, STEPS + 1):
            v = field[k, x + 1, inner, :]
            if k < STEPS:
                sx = sx + spread(coef[k]) * v
            sr = sr + spread(coef[16 + k]) * v
        xs[x] = sx
        rs[x] = diag[x] * sr
        return 0

    copies = []
    for g in range(groups):
        lax.fori_loop(g * size, (g + 1) * size, slab, 0, unroll=4)
        part = pl.ds(g * size, size)
        for n, (src, dst) in enumerate(((xs, x_hbm), (rs, r_hbm))):
            copy = pltpu.make_async_copy(src.at[part], dst.at[part], sems.at[n, g])
            copy.start()
            copies.append(copy)
    for copy in copies:
        copy.wait()


def solution(mesh):
    gx, gy, gz = mesh.shape["gx"], mesh.shape["gy"], mesh.shape["gz"]

    def on_device(right_side, conductivity, absorption):
        nx, ny, nz = right_side.shape
        assert ny == LANES and nx * 2 * 2 == LANES and gx == 2
        args = [jnp.transpose(v, (0, 2, 1)) for v in (right_side, conductivity, absorption)]
        block = (nx, nz, LANES)
        exchanges = STEPS + 1
        dma = pltpu.SemaphoreType.DMA
        tall = nz + 16
        field = (STEPS + 1, nx + 2, tall, LANES)
        vmem = pl.BlockSpec(memory_space=pltpu.VMEM)
        kept = pl.pallas_call(
            functools.partial(kernel, nx, nz, (gx, gy, gz)),
            out_shape=[pltpu.VMEM(field, F32), pltpu.VMEM(block, F32), pltpu.VMEM((32, 8, LANES), F32)],
            in_specs=[pl.BlockSpec(memory_space=pl.ANY)] * 3,
            out_specs=[vmem] * 3,
            scratch_shapes=[
                pltpu.VMEM((nx + 2, tall, LANES), F32),
                pltpu.VMEM(block, F32),
                pltpu.VMEM(block, F32),
                pltpu.VMEM((nx + 1, nz, LANES), F32),
                pltpu.VMEM(block, F32),
                pltpu.VMEM((nx, tall, LANES), F32),
                pltpu.VMEM(block, F32),
                pltpu.VMEM((nz, LANES), F32),
                pltpu.VMEM((2, nz // 2, LANES), F32),
                pltpu.VMEM((nz // 2, LANES), F32),
                pltpu.VMEM((2, nx, LANES), F32),
                pltpu.VMEM((2, nx, LANES), F32),
                pltpu.VMEM((2, nx, LANES), F32),
                pltpu.VMEM((STEPS + 1, 2, nx, LANES), F32),
                pltpu.VMEM((nz, LANES), F32),
                pltpu.VMEM((nz // 2, LANES), F32),
                pltpu.VMEM((2, nx, LANES), F32),
                pltpu.VMEM((exchanges, nz, LANES), F32),
                pltpu.VMEM((exchanges, 2, nx, LANES), F32),
                pltpu.VMEM((exchanges, 2, nx, LANES), F32),
                pltpu.VMEM((exchanges, nz // 2, LANES), F32),
                pltpu.VMEM((exchanges, 2, nz // 2, LANES), F32),
                pltpu.VMEM((exchanges, nz, LANES), F32),
                pltpu.VMEM((3, gx * gy, 1, LANES), F32),
                pltpu.VMEM((3, gz, 2, LANES), F32),
                pltpu.VMEM((2 * STEPS + 2, 8, LANES), F32),
                pltpu.VMEM((STEPS, 2, 8, LANES), F32),
                dma((3,)),
                dma((exchanges, 5)),
                dma((exchanges, 5)),
                dma((2,)),
                dma((2,)),
                dma((3, gx * gy)),
                dma((3, gx * gy)),
                dma((3, gz)),
                dma((3, gz)),
            ],
            compiler_params=pltpu.CompilerParams(
                collective_id=0, has_side_effects=True, vmem_limit_bytes=40 * 1024 * 1024
            ),
        )(*[pltpu.with_memory_space_constraint(v, pltpu.HBM) for v in args])
        groups = 4
        out = pl.pallas_call(
            functools.partial(finish, nx, nz, groups),
            out_shape=[jax.ShapeDtypeStruct(block, F32)] * 2,
            in_specs=[vmem] * 3,
            out_specs=[pl.BlockSpec(memory_space=pltpu.HBM)] * 2,
            scratch_shapes=[pltpu.VMEM(block, F32), pltpu.VMEM(block, F32), dma((2, groups))],
            compiler_params=pltpu.CompilerParams(vmem_limit_bytes=20 * 1024 * 1024),
        )(*kept)
        return tuple(jnp.transpose(v, (0, 2, 1)) for v in out)

    spec = P("gx", "gy", "gz")
    return jax.shard_map(on_device, mesh=mesh, in_specs=(spec,) * 3, out_specs=(spec,) * 2, check_vma=False)
```

```python
import functools

import jax
import jax.numpy as jnp
from jax import lax
from jax.experimental import pallas as pl
from jax.experimental.pallas import tpu as pltpu
from jax.sharding import PartitionSpec as P

F32 = jnp.float32
MESH = pl.DeviceIdType.MESH
STEPS = 10
LANES = 128
BASE = 8


def two_sum(a, b):
    s = a + b
    t = s - a
    return s, (a - (s - t)) + (b - t)


def joined_sum(a, b):
    s, e = two_sum(a[0], b[0])
    return s, e if a[1] is None else e + (a[1] + b[1])


def renew(a, b):
    s = a + b
    return s, b - (s - a)


def halves(a):
    t = 4097.0 * a
    high = t - (t - a)
    return high, a - high


def two_product(a, b):
    p = a * b
    ah, al = halves(a)
    bh, bl = halves(b)
    return p, ((ah * bh - p) + ah * bl + al * bh) + al * bl


def dadd(a, b):
    s, e = two_sum(a[0], b[0])
    return renew(s, e + (a[1] + b[1]))


def dneg(a):
    return -a[0], -a[1]


def dmul(a, b):
    p, e = two_product(a[0], b[0])
    return renew(p, e + (a[0] * b[1] + a[1] * b[0]))


def dtimes(a, power):
    return power * a[0], power * a[1]


def ddiv(a, b):
    q = a[0] / b[0]
    p, e = two_product(q, b[0])
    rest = ((a[0] - p) - e) + (a[1] - q * b[1])
    return renew(q, rest / b[0])


def jacobi_matrix(mu):
    n = (len(mu) + 1) // 2
    zero = (0.0 * mu[0][0], 0.0 * mu[0][0])
    cur = [mu[0]] + [dtimes(mu[k], 2.0 ** (1 - k)) for k in range(1, 2 * n - 1)] + [zero]
    prev = None
    ratio = ddiv(cur[1], cur[0])
    alpha, beta = [ratio], [None]
    for k in range(1, n):
        new = [None] * (2 * n)
        minus_alpha = dneg(alpha[-1])
        minus_beta = None if k == 1 else dneg(beta[-1])
        for l in range(k, 2 * n - k):
            v = dadd(cur[l + 1], dmul(minus_alpha, cur[l]))
            if prev is not None:
                v = dadd(v, dmul(minus_beta, prev[l]))
            new[l] = dadd(v, dtimes(cur[l - 1], 0.5 if l == 1 else 0.25))
        beta.append(ddiv(new[k], cur[k - 1]))
        prev, cur = cur, new
        if k < n - 1:
            later = ddiv(new[k + 1], new[k])
            alpha.append(dadd(later, dneg(ratio)))
            ratio = later
    high = [a[0] for a in alpha], [None if b is None else b[0] for b in beta]
    return high[0], high[1], cur[n], cur[n - 1], ratio


def without_pole(p, kappa):
    n = len(p) - 1
    q = [None] * (n + 2)
    q[n] = q[n + 1] = 0.0 * kappa
    for k in range(n, 1, -1):
        q[k - 1] = (q[k] + p[k]) * kappa - q[k + 1]
    q[0] = (q[1] + p[1]) * (0.5 * kappa) - 0.5 * q[2]
    return q[:n]


def solution_polynomials(alpha, beta, kappa, one):
    n = len(beta)
    tau = 0.5 * kappa
    at = [one, tau - alpha[0]]
    for k in range(1, n - 1):
        at.append((tau - alpha[k]) * at[-1] - beta[k] * at[-2])
    before, p = None, [one]
    for k in range(n):
        new = [None] * (k + 2)

        def put(i, v):
            new[i] = v if new[i] is None else new[i] + v

        for i, v in enumerate(p):
            half = 0.5 * v
            put(i + 1, half)
            put(abs(i - 1), half)
        if k < n - 1:
            for i, v in enumerate(p):
                put(i, -(alpha[k] * v))
        if before is not None:
            for i, v in enumerate(before):
                put(i, -(beta[k] * v))
        before, p = p, new
    v = before + [0.0 * one]
    at_u = tau * at[-1] - beta[n - 1] * at[-2]
    return p, v, without_pole(p, kappa), without_pole(v, kappa), at_u, at[-1]


def kernel(nx, nz, sizes, r_hbm, c_hbm, a_hbm, field, diag, coef,
           cond, absorb, weight, fx, fy, fz, turned, wx, wy, dy, wz, wzn, zterm, zown, xadd, yadd, zadd, xsend, zsend, zrecv, ysend, yrecv, xrecv,
           part1, part2, dots, table,
           load_sem, face_send, face_recv, wz_send, wz_recv, sum1_send, sum1_recv, sum2_send, sum2_recv):
    gx, gy, gz = sizes
    ix, iy, iz = lax.axis_index("gx"), lax.axis_index("gy"), lax.axis_index("gz")
    ox = 1 - ix
    base = BASE
    inner = pl.ds(base, nz)
    above = pl.ds(base + 1, nz)
    below = pl.ds(base - 1, nz)
    half = nz // 2
    tiles = nz // 8
    low_x = ix == 0
    border = jnp.where(low_x, nx, 1)

    loads = [
        pltpu.make_async_copy(c_hbm, cond.at[pl.ds(1, nx), inner, :], load_sem.at[0]),
        pltpu.make_async_copy(a_hbm, absorb, load_sem.at[1]),
        pltpu.make_async_copy(r_hbm, weight, load_sem.at[2]),
    ]
    loads[0].start()
    loads[1].start()

    zero_face = jnp.zeros((nx, LANES), F32)
    zero_slab = jnp.zeros((nz, LANES), F32)

    barrier = pltpu.get_barrier_semaphore()
    group = [((ix + dx) % gx, (iy + dy) % gy) for dx in range(gx) for dy in range(gy) if (dx, dy) != (0, 0)]
    line = [(iz + d) % gz for d in range(1, gz)]
    for px, py in group:
        pl.semaphore_signal(barrier, inc=1, device_id=(px, py, iz), device_id_type=MESH)
    for pz in line:
        pl.semaphore_signal(barrier, inc=1, device_id=(ix, iy, pz), device_id_type=MESH)

    for ref, side, alone in ((zrecv, 0, iz == 0), (zrecv, 1, iz == gz - 1), (yrecv, 0, iy == 0), (yrecv, 1, iy == gy - 1)):

        @pl.when(alone)
        def _(ref=ref, side=side):
            def clear_faces(k, _):
                ref[k, side] = zero_face
                return 0

            lax.fori_loop(0, STEPS + 1, clear_faces, 0)
            if ref is zrecv:
                wzn[side] = zero_face

    lane = lax.broadcasted_iota(jnp.int32, (half, LANES), 1)
    pair = lane // 2
    even = (lane % 2) == 0
    row_lane = lax.broadcasted_iota(jnp.int32, (1, LANES), 1)

    def tile_sum(v):
        return jnp.sum(v.reshape(tiles, 8, LANES), axis=0)

    def spread(c, rows=nz):
        return jnp.broadcast_to(c[None], (rows // 8, 8, LANES)).reshape(rows, LANES)

    def turn_of(x, h):
        return 2 * x + 2 * nx * h

    def pack(source, skip=1, start=base):
        out = jnp.zeros((half, LANES), F32)
        for x in range(nx):
            for h in range(2):
                v = source[x + skip, pl.ds(start + half * h, half), :]
                out = jnp.where(pair == x + nx * h, pltpu.roll(v, (turn_of(x, h) + 1) % LANES, 1), out)
        return out

    def copies(e):
        xc = pltpu.make_async_remote_copy(
            xsend.at[e], xrecv.at[e],
            face_send.at[e, 0], face_recv.at[e, 0], device_id=(ox, iy, iz), device_id_type=MESH)
        yc, zc = [], []
        for up in range(2):
            yc.append(pltpu.make_async_remote_copy(
                ysend.at[e], yrecv.at[e, 1 - up], face_send.at[e, 1 + up], face_recv.at[e, 2 - up],
                device_id=(ix, jnp.clip(iy + 2 * up - 1, 0, gy - 1), iz), device_id_type=MESH))
            zc.append(pltpu.make_async_remote_copy(
                zsend.at[e, up], zrecv.at[e, 1 - up], face_send.at[e, 3 + up], face_recv.at[e, 4 - up],
                device_id=(ix, iy, jnp.clip(iz + 2 * up - 1, 0, gz - 1)), device_id_type=MESH))
        return xc, yc, zc

    def send_z(e):
        _, _, zc = copies(e)
        pl.when(iz > 0)(zc[0].start)
        pl.when(iz < gz - 1)(zc[1].start)

    def send_xy(e):
        xc, yc, _ = copies(e)
        pl.when(iy > 0)(yc[0].start)
        pl.when(iy < gy - 1)(yc[1].start)
        xc.start()

    def fill_z(source, e):
        zsend[e, 0] = source[pl.ds(1, nx), base, :]
        zsend[e, 1] = source[pl.ds(1, nx), base + nz - 1, :]

    def fill_xy(source, e):
        ysend[e] = pack(source)
        xsend[e] = source[border, inner, :]

    def receive_xy(e):
        xc, yc, _ = copies(e)
        xc.wait()
        pl.when(iy > 0)(lambda: (yc[0].wait_send(), yc[1].wait_recv())[0])
        pl.when(iy < gy - 1)(lambda: (yc[1].wait_send(), yc[0].wait_recv())[0])

    def weights():
        return [
            pltpu.make_async_remote_copy(
                wz.at[up], wzn.at[1 - up], wz_send.at[up], wz_recv.at[1 - up],
                device_id=(ix, iy, jnp.clip(iz + 2 * up - 1, 0, gz - 1)), device_id_type=MESH)
            for up in range(2)
        ]

    def receive_z(e):
        _, _, zc = copies(e)
        pl.when(iz > 0)(lambda: (zc[0].wait_send(), zc[1].wait_recv())[0])
        pl.when(iz < gz - 1)(lambda: (zc[1].wait_send(), zc[0].wait_recv())[0])

    gxy = ix * gy + iy
    first = (part1, [(px, py, iz) for px, py in group], gxy, sum1_send, sum1_recv, [px * gy + py for px, py in group])
    second = (part2, [(ix, iy, pz) for pz in line], iz, sum2_send, sum2_recv, line)

    def spread_out(stage, which):
        part, peers, mine, send_sem, recv_sem, _ = stage
        for i, peer in enumerate(peers):
            pltpu.make_async_remote_copy(
                part.at[which, mine], part.at[which, mine], send_sem.at[which, i], recv_sem.at[which, mine],
                device_id=peer, device_id_type=MESH).start()

    def arrivals(stage, which):
        part, peers, _, send_sem, recv_sem, slots = stage
        return [
            pltpu.make_async_remote_copy(
                part.at[which, slot], part.at[which, slot], send_sem.at[which, i], recv_sem.at[which, slot],
                device_id=peers[i], device_id_type=MESH)
            for i, slot in enumerate(slots)
        ]

    def gather_in(stage, which):
        part = stage[0]
        for copy in arrivals(stage, which):
            copy.wait_recv()
        pairs = [(part[which, i], None) for i in range(part.shape[1])]
        while len(pairs) > 1:
            pairs = [joined_sum(*pairs[i:i + 2]) for i in range(0, len(pairs), 2)]
        return pairs[0]

    def sum_begin(which, row):
        part1[which, gxy] = row
        spread_out(first, which)

    def sum_middle(which):
        high, low = renew(*gather_in(first, which))
        part2[which, iz, pl.ds(0, 1), :] = high
        part2[which, iz, pl.ds(1, 1), :] = low
        spread_out(second, which)

    def sum_end(which):
        total, error = gather_in(second, which)
        return renew(total[0:1], error[0:1] + total[1:2])

    def all_lanes(row, m):
        return jnp.broadcast_to(jnp.sum(jnp.where(row_lane == m, row, 0.0), axis=1, keepdims=True), (8, LANES))

    def one_row(values):
        row = jnp.zeros((1, LANES), F32)
        for m, v in enumerate(values):
            row = jnp.where(row_lane == m, jnp.sum(jnp.sum(v, axis=0, keepdims=True), axis=1, keepdims=True), row)
        return row

    wide_lane = lax.broadcasted_iota(jnp.int32, (nz, LANES), 1)
    inside = wide_lane < LANES - 1
    after = wide_lane > 0
    edge = (wide_lane == 0) | (wide_lane == LANES - 1)
    one = jnp.ones((8, LANES), F32)

    face_row = lax.broadcasted_iota(jnp.int32, (nx, LANES), 0)
    face_lane = lax.broadcasted_iota(jnp.int32, (nx, LANES), 1)
    half_row = lax.broadcasted_iota(jnp.int32, (half, LANES), 0)
    slab_row = lax.broadcasted_iota(jnp.int32, (nz, LANES), 0)

    def z_edges(zpart, low_side, high_side, xa):
        faces = []
        for h in range(2):
            at = (half - 1) * h
            face = zpart[h]
            for at_lane, side, shift in ((0, low_side, 0), (LANES - 1, high_side, 1)):
                one_lane = jnp.where(face_lane == 2 * face_row + 2 * nx * h + shift, side[at:at + 1], 0.0)
                face = face + jnp.where(face_lane == at_lane, jnp.sum(one_lane, axis=1, keepdims=True), 0.0)
            at = (nz - 1) * h
            faces.append(face + jnp.where(face_row == border - 1, xa[at:at + 1], 0.0))
        return faces

    def joined(low_side, high_side):
        return jnp.where(even, pltpu.roll(high_side, LANES - 1, 1), pltpu.roll(low_side, 1, 1))

    def xy_begun(xpart, ypart, ya, xa):
        yface, xlanes = ypart + ya, []
        for h in range(2):
            here = 2 * nx * h + 1
            xa_half = xa[half * h:half * (h + 1)]
            turns = [(2 * (nx - 1) + here) % LANES, here]
            moved = jnp.where(low_x, pltpu.roll(xa_half, turns[0], 1), pltpu.roll(xa_half, turns[1], 1))
            yface = yface + jnp.where(pair == border - 1 + nx * h, moved, 0.0)
            moved = jnp.where(low_x, pltpu.roll(ya, (LANES - turns[0]) % LANES, 1), pltpu.roll(ya, LANES - turns[1], 1))
            xlanes.append(moved)
        return xpart + xa + jnp.where(edge, jnp.concatenate(xlanes, axis=0), 0.0), yface

    def xy_ended(xface, yface, za):
        for h in range(2):
            at = half_row == (half - 1) * h
            moved = jnp.where(face_lane // 2 == face_row + nx * h, pltpu.roll(za[h], 2 * nx * h + 1, 1, stride=2, stride_axis=0), 0.0)
            yface = yface + jnp.where(at, jnp.sum(moved, axis=0, keepdims=True), 0.0)
            z_at = slab_row == (nz - 1) * h
            xface = xface + jnp.where(z_at, jnp.sum(jnp.where(face_row == border - 1, za[h], 0.0), axis=0, keepdims=True), 0.0)
        return xface, yface

    def keep(za, ya, xa):
        yadd[...] = ya
        zadd[0] = za[0]
        zadd[1] = za[1]
        xadd[...] = xa

    def correct(ref, skip=1, start=base):
        ref[pl.ds(skip, nx), start, :] += zadd[0]
        ref[pl.ds(skip, nx), start + nz - 1, :] += zadd[1]
        ref[border - 1 + skip, pl.ds(start, nz), :] += xadd[...]
        terms = yadd[...]
        for x in range(nx):
            for h in range(2):
                turned[x, pl.ds(half * h, half), :] = pltpu.roll(terms, (LANES - turn_of(x, h) - 1) % LANES, 1)

        def add_sides(x, _):
            ref[x + skip, pl.ds(start, nz), :] += jnp.where(edge, turned[x], 0.0)
            return 0

        lax.fori_loop(0, nx, add_sides, 0, unroll=4)

    loads[0].wait()
    loads[2].start()
    pl.semaphore_wait(barrier, len(group) + len(line))
    fill_z(cond, 0)
    send_z(0)
    fill_xy(cond, 0)
    send_xy(0)
    loads[1].wait()

    def means(x, acc):
        return acc[0] + cond[x + 1, inner, :], acc[1] + absorb[x]

    sums = lax.fori_loop(0, nx, means, (zero_slab, zero_slab), unroll=4)
    sum_begin(0, one_row([tile_sum(v) for v in sums]))

    def clear(k, _):
        field[k, 0, inner, :] = zero_slab
        field[k, nx + 1, inner, :] = zero_slab
        field[k, pl.ds(1, nx), base - 1, :] = zero_face
        field[k, pl.ds(1, nx), base + nz, :] = zero_face
        return 0

    lax.fori_loop(0, STEPS, clear, 0)
    table[0, 0] = one
    table[0, 1] = jnp.zeros((8, LANES), F32)
    cond[0, inner, :] = zero_slab
    cond[nx + 1, inner, :] = zero_slab
    cond[pl.ds(1, nx), base - 1, :] = zero_face
    cond[pl.ds(1, nx), base + nz, :] = zero_face
    fx[0] = 0.5 * cond[1, inner, :]

    def coefficients(x, _):
        here = cond[x + 1, inner, :]
        xp = 0.5 * (here + cond[x + 2, inner, :])
        xm = fx[x]
        yp = 0.5 * (here + jnp.where(inside, pltpu.roll(here, LANES - 1, 1), 0.0))
        ym = 0.5 * (here + jnp.where(after, pltpu.roll(here, 1, 1), 0.0))
        zp = 0.5 * (here + cond[x + 1, above, :])
        zm = 0.5 * (here + cond[x + 1, below, :])
        fx[x + 1] = xp
        fy[x] = jnp.where(inside, yp, 0.0)
        fz[x, below, :] = zm
        fz[x, inner, :] = zp
        diag[x] = absorb[x] + xp + xm + yp + ym + zp + zm
        return 0

    lax.fori_loop(0, nx, coefficients, 0, unroll=8)
    loads[2].wait()
    ypart, yright = pack(diag, 0, 0), pack(weight, 0, 0)
    zpart = [diag[pl.ds(0, nx), (nz - 1) * i, :] for i in range(2)]
    zright = [weight[pl.ds(0, nx), (nz - 1) * i, :] for i in range(2)]
    receive_xy(0)
    low_side, high_side = 0.5 * yrecv[0, 0], 0.5 * yrecv[0, 1]
    xa = 0.5 * xrecv[0]
    zpart = z_edges(zpart, low_side, high_side, xa)
    receive_z(0)
    za = [0.5 * zrecv[0, i] for i in range(2)]
    zdiag = [zpart[i] + za[i] for i in range(2)]
    for i in range(2):
        zsend[1, i] = zright[i] / zdiag[i]
    send_z(1)
    ya = joined(low_side, high_side)
    xdiag, ydiag = xy_ended(*xy_begun(diag[border - 1], ypart, ya, xa), za)
    xsend[1] = weight[border - 1] / xdiag
    ysend[1] = yright / ydiag
    send_xy(1)
    sum_middle(0)
    for i in range(2):
        wz[i] = (0.5 * zsend[0, i] + za[i]) / zdiag[i]
    down, upward = weights()
    pl.when(iz > 0)(down.start)
    pl.when(iz < gz - 1)(upward.start)
    for i in range(2):
        zterm[i] = zero_face
        zown[0, i] = zsend[1, i]
    wx[...] = (0.5 * xsend[0] + xa) / xdiag
    sides = (0.5 * ysend[0] + ya) / ydiag
    wy[0] = jnp.where(even, pltpu.roll(sides, LANES - 1, 1), 0.0)
    wy[1] = jnp.where(even, 0.0, pltpu.roll(sides, 1, 1))
    dy[...] = ydiag
    keep(za, ya, xa)
    correct(diag, 0, 0)

    def begin(x, _):
        inverse = 1.0 / diag[x]
        field[0, x + 1, inner, :] = weight[x] * inverse
        weight[x] = inverse
        return 0

    lax.fori_loop(0, nx, begin, 0, unroll=8)
    keep([zero_face, zero_face], jnp.zeros((half, LANES), F32), zero_slab)

    def step(k, _):
        src, dst, old = k, k + 1, jnp.maximum(k - 1, 0)
        e = k + 1

        @pl.when(k == 1)
        def _():
            high, _ = sum_end(0)
            six = 6.0 * all_lanes(high, 0)
            rho = 0.97 * six / (six + all_lanes(high, 1))
            kappa = jnp.floor(64.0 * (2.0 / rho)) * (1.0 / 64.0)
            half_kappa = 0.5 * kappa
            table[1, 0] = kappa * half_kappa
            table[1, 1] = one
            table[2, 0] = kappa
            table[2, 1] = half_kappa
            for j in range(3, STEPS):
                table[j, 0] = kappa
                table[j, 1] = one

        @pl.when(k == 1)
        def _():
            down, upward = weights()
            pl.when(iz > 0)(lambda: (down.wait_send(), upward.wait_recv())[0])
            pl.when(iz < gz - 1)(lambda: (upward.wait_send(), down.wait_recv())[0])

        @pl.when(k > 0)
        def _():
            before = spread(table[k - 1, 0], half)
            for i in range(2):
                zterm[i] = before * wzn[i] * zown[k - 1, i]

        pl.when(k > 0)(lambda: correct(field.at[k]))
        a = table[k, 0]
        a_all, b_all = spread(a), spread(table[k, 1])

        def row(x, acc):
            same, older, ahead = acc
            v = field[src, x + 1, inner, :]
            y = fy[x]
            o = field[old, x + 1, inner, :]
            s = fx[x + 1] * field[src, x + 2, inner, :] + fx[x] * field[src, x, inner, :]
            s = s + fz[x, inner, :] * field[src, x + 1, above, :] + fz[x, below, :] * field[src, x + 1, below, :]
            s = s + y * pltpu.roll(v, LANES - 1, 1) + pltpu.roll(y * v, 1, 1)
            new = a_all * (weight[x] * s) - b_all * o
            field[dst, x + 1, inner, :] = new
            w = diag[x] * v
            return same + w * v, older + w * o, ahead + w * new

        same, older, ahead = lax.fori_loop(0, nx, row, (zero_slab, zero_slab, zero_slab), unroll=8)
        dots[2 * k] = tile_sum(same)
        dots[2 * k + 1] = tile_sum(older)
        dots[2 * STEPS] = tile_sum(ahead)

        @pl.when(k == STEPS - 1)
        def _():
            sum_begin(1, one_row([dots[m if m % 2 == 0 else m + 2] for m in range(2 * STEPS - 1)]))


        ypart = pack(field.at[dst])
        zpart = [field[dst, pl.ds(1, nx), base + row_, :] for row_ in (0, nz - 1)]
        xpart = field[dst, border, inner, :]

        a_half = spread(a, half)
        receive_xy(e)
        low_side = a_half * wy[0] * yrecv[e, 0]
        high_side = a_half * wy[1] * yrecv[e, 1]
        xa = a_all * wx[...] * xrecv[e]
        zpart = z_edges(zpart, low_side, high_side, xa)

        @pl.when(k < STEPS - 1)
        def _():
            for i in range(2):
                zsend[e + 1, i] = zpart[i]
            send_z(e + 1)

        ya = joined(low_side, high_side)
        xface, yface = xy_begun(xpart, ypart, ya, xa)
        zscale = [a_half * wz[i] for i in range(2)]
        receive_z(e)
        za = [zscale[i] * (zrecv[e, i] + zterm[i]) for i in range(2)]

        @pl.when(k < STEPS - 1)
        def _():
            xsend[e + 1], ysend[e + 1] = xy_ended(xface, yface, za)
            send_xy(e + 1)

        for i in range(2):
            zown[k + 1, i] = zpart[i] + za[i]
        keep(za, ya, xa)
        return 0

    lax.fori_loop(0, STEPS, step, 0)
    last = dots[2 * STEPS] + tile_sum(xadd[...] * diag[border - 1] * xsend[STEPS])
    faces = yadd[...] * dy[...] * ysend[STEPS]
    for i in range(2):
        faces = faces + zadd[i] * diag[pl.ds(0, nx), (nz - 1) * i, :] * zown[STEPS - 1, i]
    sum_begin(2, one_row([last + jnp.sum(faces.reshape(half // 8, 8, LANES), axis=0)]))
    correct(field.at[STEPS])
    sum_middle(1)
    sum_middle(2)
    high, low = sum_end(1)
    kappa = table[2, 0]
    half_kappa = table[2, 1]
    raw = [(all_lanes(high, m), all_lanes(low, m)) for m in range(2 * STEPS - 1)]
    exact = (half_kappa, jnp.zeros((8, LANES), F32))
    raw[1] = dmul(raw[1], exact)
    raw[2] = dmul(dmul(raw[2], exact), exact)
    raw[3] = dmul(raw[3], exact)
    mu = raw[:2]
    for m in range(2, 2 * STEPS - 1):
        mu.append(dadd(dtimes(raw[m], 2.0), dneg(mu[m % 2])))
    alpha, beta, end, pivot, ratio = jacobi_matrix(mu)
    u, v, xu, xv, at_u, at_v = solution_polynomials(alpha, beta, kappa, one)
    for p in (u, v, xu, xv):
        p[1] = p[1] * half_kappa
    end = dadd(end, dtimes(mu[1], -(2.0 ** (2 - 2 * STEPS))))
    high, low = sum_end(2)
    end = dadd(end, dtimes((all_lanes(high, 0), all_lanes(low, 0)), 2.0 ** (3 - 2 * STEPS)))
    end = dadd(ddiv(end, pivot), dneg(ratio))[0]
    scale = one / (at_u - end * at_v)
    xs = [scale * (p - end * q) for p, q in zip(xu, xv)]
    rs = [scale * (p - end * q) for p, q in zip(u, v)]
    for k, v in enumerate(xs):
        coef[k] = v
    for k, v in enumerate(rs):
        coef[16 + k] = v
    for which in range(3):
        for stage in (first, second):
            for copy in arrivals(stage, which):
                copy.wait_send()


def finish(nx, nz, groups, field, diag, coef, x_hbm, r_hbm, xs, rs, sems):
    inner = pl.ds(BASE, nz)
    size = nx // groups

    def spread(c):
        return jnp.broadcast_to(c[None], (nz // 8, 8, LANES)).reshape(nz, LANES)

    def slab(x, _):
        v = field[0, x + 1, inner, :]
        sx = spread(coef[0]) * v
        sr = spread(coef[16]) * v
        for k in range(1, STEPS + 1):
            v = field[k, x + 1, inner, :]
            if k < STEPS:
                sx = sx + spread(coef[k]) * v
            sr = sr + spread(coef[16 + k]) * v
        xs[x] = sx
        rs[x] = diag[x] * sr
        return 0

    copies = []
    for g in range(groups):
        lax.fori_loop(g * size, (g + 1) * size, slab, 0, unroll=4)
        part = pl.ds(g * size, size)
        for n, (src, dst) in enumerate(((xs, x_hbm), (rs, r_hbm))):
            copy = pltpu.make_async_copy(src.at[part], dst.at[part], sems.at[n, g])
            copy.start()
            copies.append(copy)
    for copy in copies:
        copy.wait()


def solution(mesh):
    gx, gy, gz = mesh.shape["gx"], mesh.shape["gy"], mesh.shape["gz"]

    def on_device(right_side, conductivity, absorption):
        nx, ny, nz = right_side.shape
        assert ny == LANES and nx * 2 * 2 == LANES and gx == 2
        args = [jnp.transpose(v, (0, 2, 1)) for v in (right_side, conductivity, absorption)]
        block = (nx, nz, LANES)
        exchanges = STEPS + 1
        dma = pltpu.SemaphoreType.DMA
        tall = nz + 16
        field = (STEPS + 1, nx + 2, tall, LANES)
        vmem = pl.BlockSpec(memory_space=pltpu.VMEM)
        kept = pl.pallas_call(
            functools.partial(kernel, nx, nz, (gx, gy, gz)),
            out_shape=[pltpu.VMEM(field, F32), pltpu.VMEM(block, F32), pltpu.VMEM((32, 8, LANES), F32)],
            in_specs=[pl.BlockSpec(memory_space=pl.ANY)] * 3,
            out_specs=[vmem] * 3,
            scratch_shapes=[
                pltpu.VMEM((nx + 2, tall, LANES), F32),
                pltpu.VMEM(block, F32),
                pltpu.VMEM(block, F32),
                pltpu.VMEM((nx + 1, nz, LANES), F32),
                pltpu.VMEM(block, F32),
                pltpu.VMEM((nx, tall, LANES), F32),
                pltpu.VMEM(block, F32),
                pltpu.VMEM((nz, LANES), F32),
                pltpu.VMEM((2, nz // 2, LANES), F32),
                pltpu.VMEM((nz // 2, LANES), F32),
                pltpu.VMEM((2, nx, LANES), F32),
                pltpu.VMEM((2, nx, LANES), F32),
                pltpu.VMEM((2, nx, LANES), F32),
                pltpu.VMEM((STEPS + 1, 2, nx, LANES), F32),
                pltpu.VMEM((nz, LANES), F32),
                pltpu.VMEM((nz // 2, LANES), F32),
                pltpu.VMEM((2, nx, LANES), F32),
                pltpu.VMEM((exchanges, nz, LANES), F32),
                pltpu.VMEM((exchanges, 2, nx, LANES), F32),
                pltpu.VMEM((exchanges, 2, nx, LANES), F32),
                pltpu.VMEM((exchanges, nz // 2, LANES), F32),
                pltpu.VMEM((exchanges, 2, nz // 2, LANES), F32),
                pltpu.VMEM((exchanges, nz, LANES), F32),
                pltpu.VMEM((3, gx * gy, 1, LANES), F32),
                pltpu.VMEM((3, gz, 2, LANES), F32),
                pltpu.VMEM((2 * STEPS + 2, 8, LANES), F32),
                pltpu.VMEM((STEPS, 2, 8, LANES), F32),
                dma((3,)),
                dma((exchanges, 5)),
                dma((exchanges, 5)),
                dma((2,)),
                dma((2,)),
                dma((3, gx * gy)),
                dma((3, gx * gy)),
                dma((3, gz)),
                dma((3, gz)),
            ],
            compiler_params=pltpu.CompilerParams(
                collective_id=0, has_side_effects=True, vmem_limit_bytes=40 * 1024 * 1024
            ),
        )(*[pltpu.with_memory_space_constraint(v, pltpu.HBM) for v in args])
        groups = 8
        out = pl.pallas_call(
            functools.partial(finish, nx, nz, groups),
            out_shape=[jax.ShapeDtypeStruct(block, F32)] * 2,
            in_specs=[vmem] * 3,
            out_specs=[pl.BlockSpec(memory_space=pltpu.HBM)] * 2,
            scratch_shapes=[pltpu.VMEM(block, F32), pltpu.VMEM(block, F32), dma((2, groups))],
            compiler_params=pltpu.CompilerParams(vmem_limit_bytes=20 * 1024 * 1024),
        )(*kept)
        return tuple(jnp.transpose(v, (0, 2, 1)) for v in out)

    spec = P("gx", "gy", "gz")
    return jax.shard_map(on_device, mesh=mesh, in_specs=(spec,) * 3, out_specs=(spec,) * 2, check_vma=False)
```
